256 devices in a mesh: gx: 16 (over y_lo, z), gy: 16 (over x, y_hi, core).
Axes of the slice: x: 4, y: 4 (y_hi: 2, y_lo: 2; y = y_hi * 2 + y_lo), z: 8, core: 2. Of those that a mesh axis runs over, the one named last changes fastest.
Arguments:
- modes: float32 [2, 3, 192, 256, 128], P(None, None, 'gx', 'gy'), may hold values from -6 to 6
- moduli: float32 [192, 256, 128], P('gx', 'gy'), may hold values from 0.5 to 2
- pinned: int32 [192, 256, 128], P('gx', 'gy'), may hold values 0 or 1
- spectrum: float32 [3, 2], replicated, may hold values from 0.175 to 5, as said below
Outputs:
- correction: float32 [2, 3, 192, 256, 128], P(None, None, 'gx', 'gy')
The draws below stay inside these ranges and needn't reach their ends.
Inputs may be any that keep to these rules, and one draw needn't show every extreme that they name: spectrum[l] = (lower, upper) with upper from 3.5 to 5 and lower 0.05 to 0.15 times upper.
All inputs are finite; a program needn't handle non-finite values. No bound on the sum of `pinned` on one device may be relied on, other than what follows from the above.
Results may differ from the reference program's by a relative error of at most 0.0003.
Values sent between devices are 32-bit elements; how exact they have to be, the bound alone decides.
No kernel may reach another device: no remote copies, remote signals or barrier semaphores. Data moves between devices by JAX's collectives and lax.ppermute only.
A program may use at most 128 MiB of HBM per device.

```python
import math
import jax
import jax.numpy as jnp
import numpy as np
from jax import lax

VECS = 2
DEG = 3
COARSE_DEG = 4
X = 192
Y = 256
Z = 128


def draw_spectrum(key, part):
    upper_key = jax.random.fold_in(key, 11)
    ratio_key = jax.random.fold_in(key, 23)
    top_end = jax.random.uniform(upper_key, (3,), jnp.float32, 3.5, 5.0)
    fraction = jax.random.uniform(ratio_key, (3,), jnp.float32, 0.05, 0.15)
    return jnp.stack([top_end * fraction, top_end], 1)


def place_ends(values, key, low, top_value):
    longest = values.shape.index(max(values.shape))
    spots = []
    for shift in (0, 1):
        where = [jax.random.randint(jax.random.fold_in(key, axis), (), 0, length) for axis, length in enumerate(values.shape)]
        where[longest] = (where[longest] + shift) % values.shape[longest]
        spots.append(tuple(where))
    return values.at[spots[0]].set(low).at[spots[1]].set(top_value)


def steps_of(stream_key, extent, cuts, least, high):
    def one(axis_at, parts):
        heights = jax.random.uniform(jax.random.fold_in(jax.random.fold_in(stream_key, 6), axis_at), (parts,), jnp.float32, least / len(cuts), high / len(cuts))
        return jnp.repeat(jnp.exp(heights), extent[axis_at] // parts).reshape((-1,) + (1,) * (len(extent) - axis_at - 1))

    factor_of = one(*cuts[0])
    for cut in cuts[1:]:
        factor_of = factor_of * one(*cut)
    return factor_of


def scatter_about(own_key, extent, spread, limit, split=(), kind=jnp.bfloat16):
    entries = spread * jax.random.normal(own_key, extent, jnp.float32)
    if split:
        entries = entries * steps_of(own_key, extent, split, -0.22, 0.18)
    return jnp.clip(entries, -limit, limit).astype(kind)


def setup_inputs(seed: int = 0) -> dict:
    streams_of = jax.random.split(jax.random.key(seed), 5)
    modes = scatter_about(streams_of[0], (VECS, 3, X, Y, Z), 1.0, 6.0, ((2, 16), (3, 16)), jnp.float32)
    moduli = jnp.clip(jnp.exp(math.log(2.0) - 1.3862944 * jax.random.uniform(streams_of[1], (X, Y, Z), jnp.float32) ** steps_of(streams_of[1], (X, Y, Z), ((0, 16), (1, 16)), -0.2, 0.2)), 0.5, 2.0)
    pinned = place_ends((jax.random.randint(streams_of[2], (X, Y, Z), 0, 8) < 1).astype(jnp.int32), jax.random.fold_in(streams_of[2], 1), 0, 1)
    spectrum = draw_spectrum(jax.random.fold_in(streams_of[4], 71), 0)
    return {"modes": modes, "moduli": moduli, "pinned": pinned, "spectrum": spectrum}


MU_SHEAR = 1.0
LAMBDA_BULK = 1.5
PROLONG_TABLES = {4: np.array([[1.0, 0.0, 0.0], [0.375, 0.75, -0.125], [0.0, 1.0, 0.0], [-0.125, 0.75, 0.375]], dtype=np.float32), 2: np.array([[1.0, 0.0], [0.5, 0.5]], dtype=np.float32)}
GAUSS_POINTS = [-0.9602898564975363, -0.7966664774136267, -0.5255324099163290, -0.1834346424956498, 0.1834346424956498, 0.5255324099163290, 0.7966664774136267, 0.9602898564975363]
GAUSS_WEIGHTS = [0.1012285362903763, 0.2223810344533745, 0.3137066458778873, 0.3626837833783620, 0.3626837833783620, 0.3137066458778873, 0.2223810344533745, 0.1012285362903763]


def assemble(element, degree):
    coef_table = np.zeros((degree, 2 * degree + 1))
    for residue in range(degree):
        for offset in range(-degree, degree + 1):
            target = residue + offset
            if 0 <= target <= degree:
                coef_table[residue, offset + degree] += element[residue, target]
            if residue == 0 and offset <= 0:
                coef_table[residue, offset + degree] += element[degree, degree + offset]
    return coef_table.astype(np.float32)


def basis_tables(degree):
    nodes = [float(place) / degree for place in range(degree + 1)]
    points = 0.5 * (np.array(GAUSS_POINTS) + 1.0)
    weights = 0.5 * np.array(GAUSS_WEIGHTS)
    values = np.zeros((degree + 1, points.size))
    slopes = np.zeros((degree + 1, points.size))
    for column in range(degree + 1):
        product = np.ones(points.size)
        for other in range(degree + 1):
            if other != column:
                product = product * (points - nodes[other]) / (nodes[column] - nodes[other])
        values[column] = product
        slope_sum = np.zeros(points.size)
        for skipped in range(degree + 1):
            if skipped != column:
                partial_prod = np.ones(points.size) / (nodes[column] - nodes[skipped])
                for other in range(degree + 1):
                    if other != column and other != skipped:
                        partial_prod = partial_prod * (points - nodes[other]) / (nodes[column] - nodes[other])
                slope_sum = slope_sum + partial_prod
        slopes[column] = slope_sum
    mass_el = (values * weights) @ values.T
    stiff_el = (slopes * weights) @ slopes.T
    mixed_el = (slopes * weights) @ values.T
    return [assemble(mass_el, degree), assemble(stiff_el, degree), assemble(mixed_el, degree), assemble(mixed_el.T, degree)]


def coupling():
    return MU_SHEAR + (LAMBDA_BULK + MU_SHEAR) * np.eye(3, dtype=np.float32)


def line_apply(field, along, coef_table, margin):
    degree = coef_table.shape[0]
    length = field.shape[along] - 2 * degree
    residue = (np.arange(length) + degree - margin) % degree
    coef_rows = coef_table[residue]
    shape_out = [1] * field.ndim
    shape_out[along] = length
    summed = None
    for offset in range(2 * degree + 1):
        window = lax.slice_in_dim(field, offset, offset + length, 1, along)
        weighted = window * jnp.asarray(coef_rows[:, offset].reshape(shape_out))
        summed = weighted if summed is None else summed + weighted
    return summed


def z_line(field, coef_table):
    degree = coef_table.shape[0]
    widths = [(0, 0)] * (field.ndim - 1) + [(degree, degree)]
    return line_apply(jnp.pad(field, widths), field.ndim - 1, coef_table, degree)


def elastic(padded, tables, margin):
    mass_tab, stiff_tab, mixed_tab, trans_tab = tables
    weights = coupling()
    z_mass = z_line(padded, mass_tab)
    z_stiff = z_line(padded, stiff_tab)
    along_x = line_apply(line_apply(z_mass, 3, mass_tab, margin), 2, stiff_tab, margin)
    along_y = line_apply(line_apply(z_mass, 3, stiff_tab, margin), 2, mass_tab, margin)
    along_z = line_apply(line_apply(z_stiff, 3, mass_tab, margin), 2, mass_tab, margin)
    outputs = []
    for target in range(3):
        result = weights[target, 0] * along_x[:, target] + weights[target, 1] * along_y[:, target] + weights[target, 2] * along_z[:, target]
        for source in range(3):
            if source != target:
                chosen = [mass_tab, mass_tab, mass_tab]
                chosen[target] = mixed_tab
                chosen[source] = trans_tab
                coupled = z_line(padded[:, source], chosen[2])
                coupled = line_apply(coupled, 2, chosen[1], margin)
                coupled = line_apply(coupled, 1, chosen[0], margin)
                result = result + (LAMBDA_BULK + MU_SHEAR) * coupled
        outputs.append(result)
    return jnp.stack(outputs, 1)


def level_fields(moduli, pinned, stride):
    sampled = moduli[::stride, ::stride, ::stride]
    pinned_f = pinned[::stride, ::stride, ::stride].astype(jnp.float32)
    return sampled * (1.0 - pinned_f), pinned_f


def inverse_diag(scaling, pinned_f, tables):
    mass_tab, stiff_tab = tables[0], tables[1]
    degree = mass_tab.shape[0]
    weights = coupling()
    centers = []
    for along in range(3):
        residue = np.arange(scaling.shape[along]) % degree
        shape_out = [1, 1, 1]
        shape_out[along] = scaling.shape[along]
        centers.append((mass_tab[residue, degree].reshape(shape_out), stiff_tab[residue, degree].reshape(shape_out)))
    rows_out = []
    for target in range(3):
        diagonal = weights[target, 0] * centers[0][1] * centers[1][0] * centers[2][0]
        diagonal = diagonal + weights[target, 1] * centers[0][0] * centers[1][1] * centers[2][0]
        diagonal = diagonal + weights[target, 2] * centers[0][0] * centers[1][0] * centers[2][1]
        rows_out.append(scaling * scaling * jnp.asarray(diagonal) + pinned_f)
    return 1.0 / jnp.stack(rows_out, 0)


def operate(field, scaling, pinned_f, tables, padder):
    degree = tables[0].shape[0]
    padded = padder(scaling * field, degree)
    return scaling * elastic(padded, tables, degree) + pinned_f * field


def chebyshev(source, initial, n_steps, bounds, inverse, apply_op):
    low_end = bounds[0]
    top_end = bounds[1]
    center = 0.5 * (top_end + low_end)
    radius = 0.5 * (top_end - low_end)
    ratio_cs = center / radius
    rho_now = 1.0 / ratio_cs
    residual = source if initial is None else source - apply_op(initial)
    update = inverse * residual / center
    solution = update if initial is None else initial + update
    for sweep_at in range(n_steps - 1):
        residual = residual - apply_op(update)
        rho_next = 1.0 / (2.0 * ratio_cs - rho_now)
        update = rho_next * rho_now * update + (2.0 * rho_next / radius) * inverse * residual
        solution = solution + update
        rho_now = rho_next
    return solution


def alternate(pieces, along):
    stacked = jnp.stack(pieces, along + 1)
    dims_now = list(stacked.shape)
    merged = dims_now[:along] + [dims_now[along] * dims_now[along + 1]] + dims_now[along + 2:]
    return stacked.reshape(merged)


def restrict_line(field, along, table, margin):
    period, tap_count = table.shape
    half_per = period // 2
    owned_n = field.shape[along] - 2 * margin
    if margin < period:
        widths = [(0, 0)] * field.ndim
        widths[along] = (period - margin, 0)
        field = jnp.pad(field, widths)
        start_at = 0
    else:
        start_at = margin - period
    blocks = lax.slice_in_dim(field, start_at, start_at + owned_n + period, 1, along)
    dims_now = list(blocks.shape)
    elems = owned_n // period
    blocks = blocks.reshape(dims_now[:along] + [elems + 1, period] + dims_now[along + 1:])
    tap_sums = []
    for tap_at in range(tap_count):
        running = None
        for residue in range(period):
            if table[residue, tap_at] != 0.0:
                portion = float(table[residue, tap_at]) * lax.index_in_dim(blocks, residue, along + 1, False)
                running = portion if running is None else running + portion
        tap_sums.append(running)
    leading = lax.slice_in_dim(tap_sums[0], 1, elems + 1, 1, along) + lax.slice_in_dim(tap_sums[half_per], 0, elems, 1, along)
    pieces = [leading] + [lax.slice_in_dim(tap_sums[tap_at], 1, elems + 1, 1, along) for tap_at in range(1, half_per)]
    return alternate(pieces, along)


def restrict_all(field, margin, degree):
    table = PROLONG_TABLES[degree]
    coarse = restrict_line(field, 2, table, margin)
    coarse = restrict_line(coarse, 3, table, margin)
    return restrict_line(coarse, 4, table, 0)


def prolong_line(field, along, table, margin):
    period, tap_count = table.shape
    half_per = period // 2
    elems = (field.shape[along] - 2 * margin) // half_per
    columns = [lax.slice_in_dim(field, margin + tap_at, margin + tap_at + half_per * (elems - 1) + 1, half_per, along) for tap_at in range(tap_count)]
    pieces = []
    for residue in range(period):
        running = None
        for tap_at in range(tap_count):
            if table[residue, tap_at] != 0.0:
                portion = float(table[residue, tap_at]) * columns[tap_at]
                running = portion if running is None else running + portion
        pieces.append(running)
    return alternate(pieces, along)


def prolong_all(field, degree):
    table = PROLONG_TABLES[degree]
    fine = prolong_line(field, 2, table, 1)
    fine = prolong_line(fine, 3, table, 1)
    fine = jnp.pad(fine, [(0, 0)] * 4 + [(1, 1)])
    return prolong_line(fine, 4, table, 1)


def zero_pad(field, width):
    widths = [(0, 0)] * field.ndim
    widths[-3] = (width, width)
    widths[-2] = (width, width)
    return jnp.pad(field, widths)


def reference(modes, moduli, pinned, spectrum):
    degrees = [4, 2, 1]
    tables = [basis_tables(degree) for degree in degrees]
    fields = [level_fields(moduli, pinned, stride) for stride in (1, 2, 4)]

    def v_cycle(level_at, source):
        scaling, pinned_f = fields[level_at]
        inverse = inverse_diag(scaling, pinned_f, tables[level_at])[None]

        def apply_op(field):
            return operate(field, scaling, pinned_f, tables[level_at], zero_pad)

        if level_at == 2:
            return chebyshev(source, None, COARSE_DEG, spectrum[2], inverse, apply_op)
        degree = degrees[level_at]
        solution = chebyshev(source, None, DEG, spectrum[level_at], inverse, apply_op)
        residual = (1.0 - pinned_f) * source - scaling * elastic(zero_pad(scaling * solution, degree), tables[level_at], degree)
        coarse_fixed = fields[level_at + 1][1]
        coarse_src = (1.0 - coarse_fixed) * restrict_all(zero_pad(residual, degree - 1), degree - 1, degree)
        lifted = v_cycle(level_at + 1, coarse_src)
        solution = solution + (1.0 - pinned_f) * prolong_all(zero_pad(lifted, 1), degree)
        return chebyshev(source, solution, DEG, spectrum[level_at], inverse, apply_op)

    return v_cycle(0, modes)
```

```python
import functools

import jax
import jax.numpy as jnp
import ml_dtypes
import numpy as np
from jax import lax
from jax.experimental import pallas as pl
from jax.experimental.pallas import tpu as pltpu
from jax.sharding import PartitionSpec as P

F32 = jnp.float32
BF16 = jnp.bfloat16
COUPLE = 2.5
NX, NY, NZ = 12, 16, 128
EX, EY = 3, 4
GX, GY = 16, 16

PROLONG = {
    4: np.array([[1.0, 0.0, 0.0], [0.375, 0.75, -0.125], [0.0, 1.0, 0.0], [-0.125, 0.75, 0.375]]),
    2: np.array([[1.0, 0.0], [0.5, 0.5]]),
}


def element_matrices(degree):
    points, weights = np.polynomial.legendre.leggauss(8)
    points, weights = 0.5 * (points + 1.0), 0.5 * weights
    nodes = np.arange(degree + 1) / degree
    values = np.zeros((degree + 1, points.size))
    slopes = np.zeros((degree + 1, points.size))
    for i in range(degree + 1):
        others = [j for j in range(degree + 1) if j != i]
        values[i] = np.prod([(points - nodes[j]) / (nodes[i] - nodes[j]) for j in others], axis=0)
        for k in others:
            rest = [(points - nodes[j]) / (nodes[i] - nodes[j]) for j in others if j != k]
            slopes[i] += np.prod(rest, axis=0) / (nodes[i] - nodes[k]) if rest else 1.0 / (nodes[i] - nodes[k])
    mass = (values * weights) @ values.T
    stiff = (slopes * weights) @ slopes.T
    mixed = (slopes * weights) @ values.T
    return [mass, stiff, mixed, mixed.T]


ELEMENTS = {p: element_matrices(p) for p in (4, 2, 1)}


def line_matrix(element, count):
    degree = element.shape[0] - 1
    full = np.zeros((degree * count + 1, degree * count + 1))
    for e in range(count):
        full[degree * e : degree * e + degree + 1, degree * e : degree * e + degree + 1] += element
    return full


def z_matrices(degree, copies):
    count = NZ // 4
    length = count * degree
    out = np.zeros((4, 128, 128))
    for k, element in enumerate(ELEMENTS[degree]):
        full = line_matrix(element, count)[:length, :length].copy()
        full[0, 0] += element[degree, degree]
        for v in range(copies):
            out[k, v * length : (v + 1) * length, v * length : (v + 1) * length] = full.T
    return out


def hi_lo(array):
    array = array.astype(np.float32)
    hi = array.astype(ml_dtypes.bfloat16)
    lo = (array - hi.astype(np.float32)).astype(ml_dtypes.bfloat16)
    return hi, lo


def prolong_line(degree, count):
    table = PROLONG[degree]
    half = degree // 2
    full = np.zeros((degree * count + 1, half * count + 1))
    for e in range(count):
        for a in range(degree):
            for t in range(table.shape[1]):
                full[degree * e + a, half * e + t] += table[a, t]
    full[-1, -1] = 1.0
    return full


def natural(degree, halo):
    return [
        (i, j)
        for i in range(-degree * halo, degree * (EX + halo) + 1)
        for j in range(-degree * halo, degree * (EY + halo) + 1)
    ]


def pad_to(n, m):
    return -(-n // m) * m


NODES4 = (
    [(i, j) for i in range(NX) for j in range(NY)]
    + [(NX, j) for j in range(NY)]
    + [(i, NY) for i in range(NX)]
    + [(NX, NY)]
)
NODES = {
    "4": NODES4,
    "2o": natural(2, 0),
    "2e": natural(2, 2),
    "1o": natural(1, 0),
    "1e": natural(1, 2),
}
ROWS = {"4": 224, "2o": 64, "2e": 256, "1o": 32, "1e": 80}
COLS = {"4": 256, "2e": 256, "1e": 80}


def one_hot(rows, cols, pairs):
    out = np.zeros((rows, cols), np.float32)
    for r, c in pairs:
        out[r, c] = 1.0
    return out.astype(ml_dtypes.bfloat16)


def exchange_tables(degree, halo, own, ext, rows_own, rows_ext):
    bx, by = degree * EX, degree * EY
    layers = degree * halo + 1
    own_at = {node: r for r, node in enumerate(own)}
    xlo = [(i, j) for i in range(layers) for j in range(by + 1)]
    xhi = [(bx - layers + 1 + i, j) for i in range(layers) for j in range(by + 1)]
    nx = pad_to(len(xlo), 16)
    sources = [(node, r) for node, r in own_at.items()]
    sources += [((i - bx, j), rows_own + r) for r, (i, j) in enumerate(xhi)]
    sources += [((i + bx, j), rows_own + nx + r) for r, (i, j) in enumerate(xlo)]
    span = range(-degree * halo, bx + degree * halo + 1)
    ylo = [(i, j) for i in span for j in range(layers)]
    yhi = [(i, by - layers + 1 + j) for i in span for j in range(layers)]
    ny = pad_to(len(ylo), 16)
    xs = [one_hot(nx, rows_own, [(r, own_at[n]) for r, n in enumerate(face)]) for face in (xlo, xhi)]
    width = rows_own + 2 * nx
    ys = [
        one_hot(ny, width, [(r, c) for r, n in enumerate(face) for node, c in sources if node == n])
        for face in (ylo, yhi)
    ]
    sources2 = list(sources)
    sources2 += [((i, j - by), width + r) for r, (i, j) in enumerate(yhi)]
    sources2 += [((i, j + by), width + ny + r) for r, (i, j) in enumerate(ylo)]
    ext_at = {node: r for r, node in enumerate(ext)}
    total = one_hot(rows_ext, width + 2 * ny, [(ext_at[n], c) for n, c in sources2 if n in ext_at])
    return {
        "nx": nx,
        "ny": ny,
        "xs": np.concatenate(xs, 0),
        "ys": np.concatenate(ys, 0),
        "sum": total,
    }


EXCH = {
    "2": exchange_tables(2, 2, NODES["2o"], NODES["2e"], 64, 256),
    "20": exchange_tables(2, 0, NODES["2o"], NODES["2o"], 64, 64),
    "1": exchange_tables(1, 2, NODES["1o"], NODES["1e"], 32, 80),
}


def side_by_side(a, own_a, b, own_b):
    own, nx, ny = own_a + own_b, a["nx"] + b["nx"], a["ny"] + b["ny"]
    out = {"nx": nx, "ny": ny}
    spread = lambda t, o, first: np.concatenate(
        [
            np.arange(o) + (0 if first else own_a),
            *(own + k * nx + (0 if first else a["nx"]) + np.arange(t["nx"]) for k in range(2)),
            *(own + 2 * nx + k * ny + (0 if first else a["ny"]) + np.arange(t["ny"]) for k in range(2)),
        ]
    )
    for key, width, step in (("xs", own, "nx"), ("ys", own + 2 * nx, "ny"), ("sum", own + 2 * nx + 2 * ny, None)):
        blocks = []
        for k in range(1 if step is None else 2):
            for t, o, first in ((a, own_a, True), (b, own_b, False)):
                rows = t[key] if step is None else t[key][k * t[step] : (k + 1) * t[step]]
                block = np.zeros((rows.shape[0], width), ml_dtypes.bfloat16)
                block[:, spread(t, o, first)[: rows.shape[1]]] = rows
                blocks.append(block)
        out[key] = np.concatenate(blocks, 0)
    return out


EXCH["21"] = side_by_side(EXCH["2"], 64, EXCH["1"], 32)


def placement(nodes, rows, degree, halo, axis, match):
    out = np.zeros((rows, 32), np.float32)
    for r, node in enumerate(nodes):
        if match is None or node in match:
            out[r, node[axis] + degree * halo] = 1.0
    return out


def kd_tables(nodes, rows, degree):
    m = lambda a: ELEMENTS[degree][0][a % degree, a % degree] + (ELEMENTS[degree][0][degree, degree] if a % degree == 0 else 0.0)
    k = lambda a: ELEMENTS[degree][1][a % degree, a % degree] + (ELEMENTS[degree][1][degree, degree] if a % degree == 0 else 0.0)
    out = np.zeros((rows, 8), np.float32)
    for r, (i, j) in enumerate(nodes):
        for c in range(3):
            co = [1.0 + COUPLE * (c == e) for e in range(3)]
            out[r, c] = co[0] * k(i) * m(j) + co[1] * m(i) * k(j)
            out[r, 3 + c] = co[2] * m(i) * m(j)
    copies = {4: 1, 2: 2, 1: 2}[degree]
    length = NZ // 4 * degree
    lanes = np.zeros((8, 128), np.float32)
    for z in range(length):
        for v in range(copies):
            lanes[0, v * length + z] = m(z)
            lanes[1, v * length + z] = k(z)
    return out, lanes


def dot(a, b):
    return jnp.dot(a, b, preferred_element_type=F32)


def split(v):
    hi = v.astype(BF16)
    return hi, (v - hi.astype(F32)).astype(BF16)


def sel(exact, v):
    hi, lo = split(v)
    return dot(exact, hi) + dot(exact, lo)


def sel3(exact, v):
    hi = v.astype(BF16)
    rest = v - hi.astype(F32)
    mid = rest.astype(BF16)
    lo = (rest - mid.astype(F32)).astype(BF16)
    return dot(exact, hi) + dot(exact, mid) + dot(exact, lo)


def rsel(v, exact):
    hi, lo = split(v)
    return dot(hi, exact) + dot(lo, exact)


def rsel3(v, exact):
    hi = v.astype(BF16)
    rest = v - hi.astype(F32)
    mid = rest.astype(BF16)
    lo = (rest - mid.astype(F32)).astype(BF16)
    return dot(hi, exact) + dot(mid, exact) + dot(lo, exact)


def place(idx_ref, axis):
    at = idx_ref[0]
    at = (at >> 4) if axis == 0 else (at & 15)
    even = (at & 1) == 0
    return even, (at > 0).astype(F32), (at < (GX, GY)[axis] - 1).astype(F32)


def for_pairs(idx_ref, axis, lo, hi):
    even, _, _ = place(idx_ref, axis)
    return jnp.where(even, hi, lo), jnp.where(even, lo, hi)


def from_pairs(idx_ref, axis, r0, r1):
    even, has_lo, has_hi = place(idx_ref, axis)
    return jnp.where(even, r1, r0) * has_lo, jnp.where(even, r0, r1) * has_hi


def stiffness(fields, ahi, alo, bhi, blo, y_ref, rows):
    cols = ahi.shape[2]
    for s in range(3):
        u = fields[s]
        if cols != u.shape[0]:
            u = jnp.concatenate([u, jnp.zeros((cols - u.shape[0], u.shape[1]), F32)], 0)
        uh, ul = split(u)
        y_ref[s] = dot(ahi[s], uh) + dot(ahi[s], ul) + dot(alo[s], uh)
    part = lambda s, k: y_ref[s, k * rows : (k + 1) * rows, :]
    plans = (
        (lambda: part(0, 0) + part(1, 2), lambda: part(0, 1), lambda: part(2, 2), 3),
        (lambda: part(1, 0) + part(0, 2), lambda: part(1, 1), lambda: part(2, 3), 3),
        (lambda: part(2, 0), lambda: part(2, 1), lambda: part(0, 3) + part(1, 3), 2),
    )
    outs = []
    for first, second, third, mixed in plans:
        mats_h = jnp.concatenate([bhi[0], bhi[1], bhi[mixed]], 0)
        mats_l = jnp.concatenate([blo[0], blo[1], blo[mixed]], 0)
        one, two, three = first(), second(), third()
        halves = []
        for v in range(one.shape[1] // 128):
            cut = lambda t: t[:, 128 * v : 128 * v + 128]
            h, l = split(jnp.concatenate([cut(one), cut(two), cut(three)], 1))
            halves.append(dot(h, mats_h) + dot(l, mats_h) + dot(h, mats_l))
        outs.append(halves[0] if len(halves) == 1 else jnp.concatenate(halves, 1))
    return outs


def wide(v):
    return jnp.concatenate([v, v], 1)


VMEM = pl.BlockSpec(memory_space=pltpu.VMEM)
SMEM = pl.BlockSpec(memory_space=pltpu.SMEM)


def call(body, name, smem, args, outs, scratch=(), flops=1000000, limit=40):
    return pl.pallas_call(
        body,
        name=name,
        out_shape=[jax.ShapeDtypeStruct(shape, dtype) for shape, dtype in outs],
        in_specs=[SMEM] * len(smem) + [VMEM] * len(args),
        out_specs=[VMEM] * len(outs),
        scratch_shapes=list(scratch),
        compiler_params=pltpu.CompilerParams(vmem_limit_bytes=limit * 2**20),
        cost_estimate=pl.CostEstimate(flops=flops, bytes_accessed=100000, transcendentals=0),
    )(*smem, *args)


def setup_body(corr, idx_ref, x1_ref, y1_ref, ox_ref, oxt_ref, oy_ref, oyt_ref, ahi_ref, alo_ref, xe_ref, ye_ref):
    rows = ox_ref.shape[0]
    at = idx_ref[0]
    hdot = functools.partial(jnp.dot, preferred_element_type=F32, precision=lax.Precision.HIGHEST)
    corner = (lax.broadcasted_iota(jnp.int32, (32, 32), 0) + lax.broadcasted_iota(jnp.int32, (32, 32), 1)) == 0
    for k in range(4):
        x1, y1 = x1_ref[k], y1_ref[k]
        if corr is not None:
            x1 = x1 + jnp.where(corner, corr[k], 0.0) * ((at >> 4) == 0).astype(F32)
            y1 = y1 + jnp.where(corner, corr[k], 0.0) * ((at & 15) == 0).astype(F32)
        xe_ref[k] = hdot(hdot(ox_ref[...], x1), oxt_ref[...])
        ye_ref[k] = hdot(hdot(oy_ref[...], y1), oyt_ref[...])
    m, k, g, t = range(4)
    strong = 1.0 + COUPLE
    xy = lambda a, b: xe_ref[a] * ye_ref[b]
    plans = (
        (lambda: strong * xy(k, m) + xy(m, k), lambda: xy(m, m), lambda: COUPLE * xy(t, g), lambda: COUPLE * xy(t, m)),
        (lambda: xy(k, m) + strong * xy(m, k), lambda: xy(m, m), lambda: COUPLE * xy(g, t), lambda: COUPLE * xy(m, t)),
        (lambda: xy(k, m) + xy(m, k), lambda: strong * xy(m, m), lambda: COUPLE * xy(g, m), lambda: COUPLE * xy(m, g)),
    )
    for s in range(3):
        for j in range(4):
            hi, lo = split(plans[s][j]())
            ahi_ref[s, j * rows : (j + 1) * rows, :] = hi
            alo_ref[s, j * rows : (j + 1) * rows, :] = lo


def plane_matrices(idx, degree, out_key, in_key):
    halo = 0 if in_key == "4" else 2
    rows, cols = ROWS[out_key], COLS[in_key]
    own = out_key in ("4", "2o", "1o")
    match = set(NODES["4" if in_key == "4" else out_key]) if own else None
    x1, y1 = np.zeros((4, 32, 32), np.float32), np.zeros((4, 32, 32), np.float32)
    start = degree * halo if own else 0
    ex, ey = (EX, EY) if own else (EX + 2 * halo, EY + 2 * halo)
    for k, element in enumerate(ELEMENTS[degree]):
        for out, count in ((x1, ex), (y1, ey)):
            n = degree * count + 1
            out[k, :n, :n] = line_matrix(element, count)
    places = []
    shift = 0 if own else halo
    for axis in (0, 1):
        places.append(placement(NODES[out_key], rows, degree, shift, axis, match))
        places.append(placement(NODES[in_key], cols, degree, shift, axis, match).T.copy() if not own else
                      np.ascontiguousarray(placement([n if n in match else (0, 0) for n in NODES[in_key]], cols, degree, 0, axis, None).T
                                           * np.array([1.0 if r < len(NODES[in_key]) and NODES[in_key][r] in match else 0.0 for r in range(cols)], np.float32)))
    corr = [float(np.float32(e[degree, degree])) for e in ELEMENTS[degree]] if own else None
    shape = (3, 4 * rows, cols)
    return call(
        functools.partial(setup_body, corr),
        "setup_" + out_key,
        [idx],
        [x1, y1, places[0], places[1], places[2], places[3]],
        [(shape, BF16), (shape, BF16)],
        [pltpu.VMEM((4, rows, cols), F32), pltpu.VMEM((4, rows, cols), F32)],
    )


def pack_x_body(idx_ref, modes_ref, w_ref, pin_ref, pick_ref, zw_ref, zm_ref, xs_ref, own_ref, s0_ref, s1_ref):
    w = w_ref[...]
    m = 1.0 - pin_ref[...].astype(F32)
    own = rsel3(sel3(pick_ref[...], w), zw_ref[...]) + rsel(sel(pick_ref[...], m), zm_ref[...])
    own_ref[...] = own
    nx = xs_ref.shape[0] // 2
    faces = sel3(xs_ref[...], own)
    a, b = for_pairs(idx_ref, 0, faces[:nx], faces[nx:])
    for ref, face in ((s0_ref, a), (s1_ref, b)):
        for v in range(2):
            for c in range(3):
                ref[16 * (3 * v + c) : 16 * (3 * v + c) + 16, :] = modes_ref[v, c, 0:16, :]
        ref[96:112, :] = w[0:16]
        ref[112:128, :] = m[0:16]
        ref[128 : 128 + nx, :] = face


def pack_y_body(idx_ref, modes_ref, w_ref, pin_ref, own_ref, r0_ref, r1_ref, ys_ref, s0_ref, s1_ref, m_ref):
    m_ref[...] = 1.0 - pin_ref[...].astype(F32)
    lo, hi = from_pairs(idx_ref, 0, r0_ref[...], r1_ref[...])
    ny = ys_ref.shape[0] // 2
    stack = jnp.concatenate([own_ref[...], lo[128:], hi[128:]], 0)
    faces = sel3(ys_ref[...], stack)
    a, b = for_pairs(idx_ref, 1, faces[:ny], faces[ny:])
    for ref, face in ((s0_ref, a), (s1_ref, b)):
        ref[0:128, :] = jnp.zeros((128, 128), F32)
        for k in range(8):
            if k < 6:
                line = modes_ref[k // 3, k % 3, pl.ds(0, NX, stride=NY), :]
            else:
                line = (w_ref if k == 6 else m_ref)[pl.ds(0, NX, stride=NY), :]
            ref[16 * k : 16 * k + NX, :] = line
            ref[16 * k + NX : 16 * k + NX + 1, :] = hi[16 * k : 16 * k + 1]
        ref[128 : 128 + ny, :] = face


def static_of(w, m, kd, lanes):
    s = w * m
    f = 1.0 - m
    s2 = s * s
    inv = [1.0 / (s2 * (kd[:, c : c + 1] * lanes[0:1] + kd[:, 3 + c : 4 + c] * lanes[1:2]) + f) for c in range(3)]
    return s, f, inv


def statics_body(
    idx_ref, own_ref, rx0_ref, rx1_ref, ry0_ref, ry1_ref, sum_ref, dw_ref, dm_ref, own2_ref, pick1_ref, d1w_ref, d1m_ref, own1_ref,
    kd2_ref, l2_ref, kd2o_ref, kd1_ref, l1_ref, kd1o_ref,
    e2_ref, o2_ref, e1_ref, o1_ref,
):
    xlo, xhi = from_pairs(idx_ref, 0, rx0_ref[128:, :], rx1_ref[128:, :])
    ylo, yhi = from_pairs(idx_ref, 1, ry0_ref[128:, :], ry1_ref[128:, :])
    ext = sel3(sum_ref[...], jnp.concatenate([own_ref[...], xlo, xhi, ylo, yhi], 0))

    def put(ref, w, m, kd, lanes):
        s, f, inv = static_of(w, m, kd, lanes)
        ref[0], ref[1] = s, f
        for c in range(3):
            ref[2 + c] = inv[c]

    w2, m2 = rsel3(ext, dw_ref[...]), rsel(ext, dm_ref[...])
    put(e2_ref, w2, m2, kd2_ref[...], l2_ref[...])
    put(o2_ref, sel3(own2_ref[...], w2), sel(own2_ref[...], m2), kd2o_ref[...], l2_ref[...])
    coarse = sel3(pick1_ref[...], ext)
    w1, m1 = rsel3(coarse, d1w_ref[...]), rsel(coarse, d1m_ref[...])
    put(e1_ref, w1, m1, kd1_ref[...], l1_ref[...])
    put(o1_ref, sel3(own1_ref[...], w1), sel(own1_ref[...], m1), kd1o_ref[...], l1_ref[...])


X4, Y4 = 24, 16


def faces_x4(idx_ref, outs, s0_ref, s1_ref):
    even, _, _ = place(idx_ref, 0)
    for c in range(3):
        w = outs[c]
        lo = jnp.concatenate([w[0:16], w[208:216]], 0)
        hi = jnp.concatenate([w[192:208], w[216:224]], 0)
        s0_ref[c] = jnp.where(even, hi, lo)
        s1_ref[c] = jnp.where(even, lo, hi)


LO16, HI16 = 16, 20


def faces_y4_body(idx_ref, w_ref, r0_ref, r1_ref, s0_ref, s1_ref):
    even, _, _ = place(idx_ref, 1)
    for c in range(3):
        xlo, xhi = from_pairs(idx_ref, 0, r0_ref[c], r1_ref[c])
        row = lax.broadcasted_iota(jnp.int32, (Y4, 256), 0)
        lo = jnp.concatenate([w_ref[2 * c + v, pl.ds(0, NX, stride=NY), :] for v in range(2)], 1)
        lo = jnp.concatenate([lo, jnp.concatenate([w_ref[2 * c + v, 192:196, :] for v in range(2)], 1)], 0)
        hi = jnp.concatenate([w_ref[2 * c + v, 208:224, :] for v in range(2)], 1)
        lo = lo + jnp.where(row == 0, xlo[0:1], 0.0) + jnp.where(row == NX, xhi[0:1], 0.0)
        hi = hi + jnp.where(row == 0, xlo[HI16 : HI16 + 1], 0.0) + jnp.where(row == NX, xhi[LO16 : LO16 + 1], 0.0)
        s0_ref[c] = jnp.where(even, hi, lo)
        s1_ref[c] = jnp.where(even, lo, hi)


def summed4(idx_ref, w_ref, rx0, rx1, ry0, ry1, full_ref):
    row = lax.broadcasted_iota(jnp.int32, (Y4, 256), 0)
    for c in range(3):
        xlo, xhi = from_pairs(idx_ref, 0, rx0[c], rx1[c])
        ylo, yhi = from_pairs(idx_ref, 1, ry0[c], ry1[c])
        yhi = jnp.where(row <= NX, yhi, 0.0)
        yhi = yhi + jnp.where(row == 0, xlo[HI16 : HI16 + 1], 0.0) + jnp.where(row == NX, xhi[LO16 : LO16 + 1], 0.0)
        end = xhi[0:16] + jnp.where(row == 0, ylo[NX : NX + 1], 0.0)
        for v in range(2):
            k, cut = 2 * c + v, slice(128 * v, 128 * v + 128)
            full_ref[k] = w_ref[k]
            full_ref[k, 0:16, :] += xlo[0:16, cut]
            full_ref[k, 192:208, :] += end[:, cut]
            full_ref[k, 208:224, :] += yhi[:, cut]
            full_ref[k, pl.ds(0, NX, stride=NY), :] += ylo[:NX, cut]


def put4(ref, outs):
    for c in range(3):
        for v in range(2):
            ref[2 * c + v] = outs[c][:, 128 * v : 128 * v + 128]


def first4_body(
    idx_ref, coef_ref, modes_ref, w_ref, pin_ref, rx0_ref, rx1_ref, ry0_ref, ry1_ref, kd_ref, lanes_ref, ahi, alo, bhi, blo,
    b_ref, st_ref, d_ref, out_ref, s0_ref, s1_ref, y_ref,
):
    _, xhi = from_pairs(idx_ref, 0, rx0_ref[0:128, :], rx1_ref[0:128, :])
    _, yhi = from_pairs(idx_ref, 1, ry0_ref[0:128, :], ry1_ref[0:128, :])

    def gathered(own, k):
        return jnp.concatenate([own, xhi[16 * k : 16 * k + 16], yhi[16 * k : 16 * k + 16]], 0)

    w = gathered(w_ref[...], 6)
    m = gathered(1.0 - pin_ref[...].astype(F32), 7)
    s, f, inv = static_of(w, m, kd_ref[...], lanes_ref[...])
    st_ref[0], st_ref[1] = s, f
    for c in range(3):
        st_ref[2 + c] = inv[c]
    fields = []
    for c in range(3):
        b = jnp.concatenate([gathered(modes_ref[v, c], 3 * v + c) for v in range(2)], 1)
        b_ref[c] = b
        d = wide(inv[c]) * b * coef_ref[0, 0]
        d_ref[c] = d
        fields.append(wide(s) * d)
    outs = stiffness(fields, ahi, alo, bhi, blo, y_ref, 224)
    put4(out_ref, outs)
    faces_x4(idx_ref, outs, s0_ref, s1_ref)


def both4(ref, c):
    return jnp.concatenate([ref[2 * c], ref[2 * c + 1]], 1)


def update4(idx_ref, coef_ref, step, w_ref, recv, st_ref, r_ref, d_ref, full_ref, c):
    s, f, inv = wide(st_ref[0]), wide(st_ref[1]), wide(st_ref[2 + c])
    r = r_ref[c] - (s * both4(full_ref, c) + f * d_ref[c])
    if step == 0:
        d = coef_ref[0, 0] * inv * r
    else:
        d = coef_ref[0, 2 * step - 1] * d_ref[c] + coef_ref[0, 2 * step] * inv * r
    return s, f, r, d


def mid4_body(
    step, idx_ref, coef_ref, w_ref, rx0, rx1, ry0, ry1, st_ref, r_ref, d_ref, x_ref, ahi, alo, bhi, blo,
    r_out, d_out, x_out, out_ref, s0_ref, s1_ref, y_ref, full_ref,
):
    summed4(idx_ref, w_ref, rx0, rx1, ry0, ry1, full_ref)
    fields = []
    for c in range(3):
        s, f, r, d = update4(idx_ref, coef_ref, step, w_ref, None, st_ref, r_ref, d_ref, full_ref, c)
        r_out[c], d_out[c] = r, d
        x_out[c] = x_ref[c] + d
        fields.append(s * d)
    outs = stiffness(fields, ahi, alo, bhi, blo, y_ref, 224)
    put4(out_ref, outs)
    faces_x4(idx_ref, outs, s0_ref, s1_ref)


def resid4_body(
    idx_ref, coef_ref, w_ref, rx0, rx1, ry0, ry1, st_ref, r_ref, d_ref, x_ref, ahi, alo, bhi, blo, rxy_ref, rz_ref, xs_ref,
    x_out, p_ref, s0_ref, s1_ref, y_ref, full_ref, keep_ref,
):
    summed4(idx_ref, w_ref, rx0, rx1, ry0, ry1, full_ref)
    fields = []
    owned = lax.broadcasted_iota(jnp.int32, (224, 256), 0) < NX * NY
    for c in range(3):
        s, f, r, d = update4(idx_ref, coef_ref, 2, w_ref, None, st_ref, r_ref, d_ref, full_ref, c)
        x_out[c] = x_ref[c] + d
        keep_ref[c] = jnp.where(owned, (1.0 - f) * r, 0.0)
        fields.append(s * d)
    outs = stiffness(fields, ahi, alo, bhi, blo, y_ref, 224)
    nx = xs_ref.shape[0] // 2
    for c in range(3):
        left = sel(rxy_ref[...], keep_ref[c] - wide(st_ref[0]) * outs[c])
        part = rsel(left[:, :128], rz_ref[0]) + rsel(left[:, 128:], rz_ref[1])
        p_ref[c] = part
        faces = sel(xs_ref[...], part)
        s0_ref[c], s1_ref[c] = for_pairs(idx_ref, 0, faces[:nx], faces[nx:])


def rise4_body(
    idx_ref, p_ref, rx0, rx1, ry0, ry1, sum_ref, pxy_ref, pz_ref, st_ref, x_ref, ahi, alo, bhi, blo,
    x_out, out_ref, s0_ref, s1_ref, y_ref,
):
    fields = []
    s, m = wide(st_ref[0]), 1.0 - wide(st_ref[1])
    for c in range(3):
        e = gather_sum(idx_ref, sum_ref, p_ref[c], rx0[c], rx1[c], ry0[c], ry1[c])
        e = sel(pxy_ref[...], e)
        x = x_ref[c] + m * jnp.concatenate([rsel(e, pz_ref[0]), rsel(e, pz_ref[1])], 1)
        x_out[c] = x
        fields.append(s * x)
    outs = stiffness(fields, ahi, alo, bhi, blo, y_ref, 224)
    put4(out_ref, outs)
    faces_x4(idx_ref, outs, s0_ref, s1_ref)


def last4_body(idx_ref, coef_ref, w_ref, rx0, rx1, ry0, ry1, st_ref, r_ref, d_ref, x_ref, out_ref, full_ref):
    summed4(idx_ref, w_ref, rx0, rx1, ry0, ry1, full_ref)
    for c in range(3):
        _, _, _, d = update4(idx_ref, coef_ref, 2, w_ref, None, st_ref, r_ref, d_ref, full_ref, c)
        x = x_ref[c] + d
        for v in range(2):
            out_ref[v, c] = x[: NX * NY, 128 * v : 128 * v + 128]


def gather_sum(idx_ref, sum_ref, own, rx0, rx1, ry0, ry1):
    xlo, xhi = from_pairs(idx_ref, 0, rx0, rx1)
    ylo, yhi = from_pairs(idx_ref, 1, ry0, ry1)
    return sel(sum_ref[...], jnp.concatenate([own, xlo, xhi, ylo, yhi], 0))


def faces_y_body(idx_ref, p_ref, r0_ref, r1_ref, ys_ref, s0_ref, s1_ref):
    ny = ys_ref.shape[0] // 2
    for c in range(3):
        lo, hi = from_pairs(idx_ref, 0, r0_ref[c], r1_ref[c])
        faces = sel(ys_ref[...], jnp.concatenate([p_ref[c], lo, hi], 0))
        s0_ref[c], s1_ref[c] = for_pairs(idx_ref, 1, faces[:ny], faces[ny:])


def smooth(level, coef_ref, st_ref, b, x, steps, mats, y_ref, rows):
    s, f = st_ref[0], st_ref[1]
    inv = [st_ref[2 + c] for c in range(3)]
    apply = lambda v: [s * w + f * t for w, t in zip(stiffness([s * t for t in v], *mats, y_ref, rows), v)]
    r = b
    if x is not None:
        r = [a - t for a, t in zip(r, apply(x))]
    d = [inv[c] * r[c] * coef_ref[level, 0] for c in range(3)]
    x = d if x is None else [a + t for a, t in zip(x, d)]
    for step in range(1, steps):
        r = [a - t for a, t in zip(r, apply(d))]
        d = [coef_ref[level, 2 * step - 1] * d[c] + coef_ref[level, 2 * step] * inv[c] * r[c] for c in range(3)]
        x = [a + t for a, t in zip(x, d)]
    return s, f, inv, r, d, x


def down2_body(
    idx_ref, coef_ref, p_ref, rx0, rx1, ry0, ry1, sum_ref, st_ref, sto_ref, own_ref, rxy_ref, rz_ref, xs_ref,
    ahi, alo, ohi, olo, bhi, blo, owner_ref,
    b_out, x_out, p_out, s0_ref, s1_ref, y_ref, yo_ref,
):
    m = 1.0 - st_ref[1]
    b = []
    for c in range(3):
        b.append(m * gather_sum(idx_ref, sum_ref, p_ref[c], rx0[c], rx1[c], ry0[c], ry1[c]))
        b_out[c] = b[c]
    s, f, inv, r, d, x = smooth(1, coef_ref, st_ref, b, None, 3, (ahi, alo, bhi, blo), y_ref, 256)
    outs = stiffness([s * t for t in d], ohi, olo, bhi, blo, yo_ref, 64)
    nx = xs_ref.shape[0] // 2
    for c in range(3):
        x_out[c] = sel(own_ref[...], x[c])
        left = owner_ref[...] * sel(own_ref[...], m * r[c]) - sto_ref[0] * outs[c]
        part = rsel(sel(rxy_ref[...], left), rz_ref[...])
        p_out[c] = part
        faces = sel(xs_ref[...], part)
        s0_ref[c], s1_ref[c] = for_pairs(idx_ref, 0, faces[:nx], faces[nx:])


def tail(level, last, coef_ref, own_ref, owner_ref, sto_ref, f, inv, r, d, x, outs, c):
    base = x[c] + coef_ref[level, 2 * last - 1] * d[c] + coef_ref[level, 2 * last] * inv[c] * (r[c] - f * d[c])
    return owner_ref[...] * sel(own_ref[...], base) - coef_ref[level, 2 * last] * sto_ref[2 + c] * sto_ref[0] * outs[c]


def bottom_body(
    idx_ref, coef_ref, p_ref, rx0, rx1, ry0, ry1, sum_ref, st_ref, sto_ref, own_ref, owner_ref, ahi, alo, ohi, olo, bhi, blo,
    x2_ref, owner2_ref, xs_ref,
    p_out, s0_ref, s1_ref, y_ref, yo_ref,
):
    m = 1.0 - st_ref[1]
    b = [m * gather_sum(idx_ref, sum_ref, p_ref[c], rx0[c], rx1[c], ry0[c], ry1[c]) for c in range(3)]
    s, f, inv, r, d, x = smooth(2, coef_ref, st_ref, b, None, 3, (ahi, alo, bhi, blo), y_ref, 80)
    outs = stiffness([s * t for t in d], ohi, olo, bhi, blo, yo_ref, 32)
    nx = xs_ref.shape[0] // 2
    for c in range(3):
        e = tail(2, 3, coef_ref, own_ref, owner_ref, sto_ref, f, inv, r, d, x, outs, c)
        part = jnp.concatenate([owner2_ref[...] * x2_ref[c], e], 0)
        p_out[c] = part
        faces = sel(xs_ref[...], part)
        s0_ref[c], s1_ref[c] = for_pairs(idx_ref, 0, faces[:nx], faces[nx:])


def up2_body(
    idx_ref, coef_ref, p_ref, rx0, rx1, ry0, ry1, sum_ref, b_ref, st_ref, sto_ref, own_ref, owner_ref, ahi, alo, ohi, olo, bhi, blo, xs_ref,
    pxy_ref, pz_ref, p_out, s0_ref, s1_ref, y_ref, yo_ref,
):
    x = []
    for c in range(3):
        both = gather_sum(idx_ref, sum_ref, p_ref[c], rx0[c], rx1[c], ry0[c], ry1[c])
        x.append(both[:256] + (1.0 - st_ref[1]) * rsel(sel(pxy_ref[...], both[256:]), pz_ref[...]))
    b = [b_ref[c] for c in range(3)]
    s, f, inv, r, d, x = smooth(1, coef_ref, st_ref, b, x, 2, (ahi, alo, bhi, blo), y_ref, 256)
    outs = stiffness([s * t for t in d], ohi, olo, bhi, blo, yo_ref, 64)
    nx = xs_ref.shape[0] // 2
    for c in range(3):
        part = tail(1, 2, coef_ref, own_ref, owner_ref, sto_ref, f, inv, r, d, x, outs, c)
        p_out[c] = part
        faces = sel(xs_ref[...], part)
        s0_ref[c], s1_ref[c] = for_pairs(idx_ref, 0, faces[:nx], faces[nx:])


def swap(axis, s0, s1):
    n = GX if axis == "gx" else GY
    even = [(i, i ^ 1) for i in range(n)]
    odd = [(i, (((i - 1) ^ 1) + 1) % n) for i in range(n)]
    return lax.ppermute(s0, axis, even), lax.ppermute(s1, axis, odd)


def chebyshev_table(spectrum):
    low, top = spectrum[:, 0], spectrum[:, 1]
    center, radius = 0.5 * (top + low), 0.5 * (top - low)
    ratio = center / radius
    rho = 1.0 / ratio
    columns = [1.0 / center]
    for _ in range(3):
        after = 1.0 / (2.0 * ratio - rho)
        columns += [after * rho, 2.0 * after / radius]
        rho = after
    return jnp.stack(columns, 1)


def interp_tables():
    plane = {}
    for key, degree, halo, fine, rows, coarse, rows_c in (
        (4, 4, 0, NODES["4"], 224, NODES["2o"], 64),
        (2, 2, 0, NODES["2o"], 64, NODES["1o"], 32),
        ("2e", 2, 2, NODES["2e"], 256, NODES["1e"], 80),
    ):
        px, py = prolong_line(degree, EX + 2 * halo), prolong_line(degree, EY + 2 * halo)
        f0, c0 = degree * halo, degree * halo // 2
        full = np.zeros((rows, rows_c))
        for r, (i, j) in enumerate(fine):
            for q, (a, b) in enumerate(coarse):
                full[r, q] = px[i + f0, a + c0] * py[j + f0, b + c0]
        plane[key] = full.astype(ml_dtypes.bfloat16)
    z4 = prolong_line(4, 32)[:128, :64]
    z2 = prolong_line(2, 32)[:64, :32]
    pz4 = np.zeros((2, 128, 128))
    for v in range(2):
        pz4[v, 64 * v : 64 * v + 64, :] = z4.T
    pz2 = np.zeros((128, 128))
    for v in range(2):
        pz2[32 * v : 32 * v + 32, 64 * v : 64 * v + 64] = z2.T
    cast = lambda t: np.ascontiguousarray(t).astype(ml_dtypes.bfloat16)
    return plane, cast(pz4), cast(pz4.transpose(0, 2, 1)), cast(pz2), cast(pz2.T)


def local(modes, moduli, pinned, spectrum):
    idx = (lax.axis_index("gx") * 16 + lax.axis_index("gy")).astype(jnp.int32).reshape(1)
    coef = chebyshev_table(spectrum)
    modes = modes.reshape(2, 3, NX * NY, NZ)
    moduli = moduli.reshape(NX * NY, NZ)
    pinned = pinned.reshape(NX * NY, NZ)

    zmats = {p: hi_lo(z_matrices(p, 1 if p == 4 else 2)) for p in (4, 2, 1)}
    plane, pz4, rz4, pz2, rz2 = interp_tables()
    bf = lambda t: np.ascontiguousarray(t).astype(ml_dtypes.bfloat16)
    x2, x20, x1, x21 = EXCH["2"], EXCH["20"], EXCH["1"], EXCH["21"]

    at4 = {n: r for r, n in enumerate(NODES["4"])}
    at2e = {n: r for r, n in enumerate(NODES["2e"])}
    at1e = {n: r for r, n in enumerate(NODES["1e"])}
    pick2 = one_hot(64, NX * NY, [(r, at4[(2 * i, 2 * j)]) for r, (i, j) in enumerate(NODES["2o"]) if i < 6 and j < 8])
    zw, zm = np.zeros((128, 128)), np.zeros((128, 128))
    dw, dm, d1w, d1m = (np.zeros((128, 128)) for _ in range(4))
    for k in range(64):
        zw[2 * k, k] = zm[2 * k, 64 + k] = 1.0
        for v in range(2):
            dw[k, 64 * v + k] = dm[64 + k, 64 * v + k] = 1.0
            if k % 2 == 0:
                d1w[k, 32 * v + k // 2] = d1m[64 + k, 32 * v + k // 2] = 1.0
    own2 = one_hot(64, 256, [(r, at2e[n]) for r, n in enumerate(NODES["2o"])])
    own1 = one_hot(32, 80, [(r, at1e[n]) for r, n in enumerate(NODES["1o"])])
    pick1 = one_hot(80, 256, [(r, at2e[(2 * i, 2 * j)]) for r, (i, j) in enumerate(NODES["1e"])])
    owner2, owner1 = np.zeros((64, 128), np.float32), np.zeros((32, 128), np.float32)
    for r, (i, j) in enumerate(NODES["2o"]):
        owner2[r] = float(i < 6 and j < 8)
    for r, (i, j) in enumerate(NODES["1o"]):
        owner1[r] = float(i < 3 and j < 4)
    kd4, l4 = kd_tables(NODES["4"], 224, 4)
    kd2, l2 = kd_tables(NODES["2e"], 256, 2)
    kd2o, _ = kd_tables(NODES["2o"], 64, 2)
    kd1, l1 = kd_tables(NODES["1e"], 80, 1)
    kd1o, _ = kd_tables(NODES["1o"], 32, 1)

    mx = 128 + x2["nx"]
    my = 128 + x2["ny"]
    q2own, sx0, sx1 = call(
        pack_x_body, "pack_x", [idx], [modes, moduli, pinned, pick2, bf(zw), bf(zm), x2["xs"]],
        [((64, 128), F32), ((mx, 128), F32), ((mx, 128), F32)],
    )
    rx0, rx1 = swap("gx", sx0, sx1)
    a4 = plane_matrices(idx, 4, "4", "4")
    sy0, sy1 = call(
        pack_y_body, "pack_y", [idx], [modes, moduli, pinned, q2own, rx0, rx1, x2["ys"]],
        [((my, 128), F32), ((my, 128), F32)], [pltpu.VMEM((NX * NY, NZ), F32)],
    )
    ry0, ry1 = swap("gy", sy0, sy1)
    a2e = plane_matrices(idx, 2, "2e", "2e")
    a2o = plane_matrices(idx, 2, "2o", "2e")
    a1e = plane_matrices(idx, 1, "1e", "1e")
    a1o = plane_matrices(idx, 1, "1o", "1e")

    big = ((3, 224, 256), F32)
    msgx, msgy = ((3, X4, 256), F32), ((3, Y4, 256), F32)
    y4 = pltpu.VMEM((3, 4 * 224, 256), F32)
    full = pltpu.VMEM((6, 224, 128), F32)
    keep = pltpu.VMEM((3, 224, 256), F32)
    halves = ((6, 224, 128), F32)
    mats4 = [*a4, *zmats[4]]

    b, st4, d, w, s0, s1 = call(
        first4_body, "first4", [idx, coef], [modes, moduli, pinned, rx0, rx1, ry0, ry1, kd4, l4, *mats4],
        [big, ((5, 224, 128), F32), big, halves, msgx, msgx], [y4],
    )
    st2, st2o, st1, st1o = call(
        statics_body, "statics", [idx],
        [q2own, rx0, rx1, ry0, ry1, x2["sum"], bf(dw), bf(dm), own2, pick1, bf(d1w), bf(d1m), own1, kd2, l2, kd2o, kd1, l1, kd1o],
        [((5, 256, 128), F32), ((5, 64, 128), F32), ((5, 80, 128), F32), ((5, 32, 128), F32)],
    )

    def trade4(w, s0, s1):
        r0, r1 = swap("gx", s0, s1)
        t0, t1 = call(faces_y4_body, "faces_y4", [idx], [w, r0, r1], [msgy, msgy])
        return [w, r0, r1, *swap("gy", t0, t1)]

    def trade(table, p, s0, s1):
        r0, r1 = swap("gx", s0, s1)
        t0, t1 = call(faces_y_body, "faces_y", [idx], [p, r0, r1, table["ys"]], [((3, table["ny"], 128), F32)] * 2)
        return [p, r0, r1, *swap("gy", t0, t1), table["sum"]]

    got = trade4(w, s0, s1)
    r, d, x, w, s0, s1 = call(
        functools.partial(mid4_body, 1), "mid4", [idx, coef], [*got, st4, b, d, d, *mats4], [big, big, big, halves, msgx, msgx], [y4, full],
    )
    got = trade4(w, s0, s1)
    face2, face20, face1, face21 = (((3, t["nx"], 128), F32) for t in (x2, x20, x1, x21))
    own2f, own1f = ((3, 64, 128), F32), ((3, 32, 128), F32)
    x4, p2, s0, s1 = call(
        resid4_body, "resid4", [idx, coef], [*got, st4, r, d, x, *mats4, bf(plane[4].T), rz4, x2["xs"]],
        [big, own2f, face2, face2], [y4, full, keep],
    )
    y2, y2o = pltpu.VMEM((3, 1024, 128), F32), pltpu.VMEM((3, 256, 128), F32)
    y1, y1o = pltpu.VMEM((3, 320, 128), F32), pltpu.VMEM((3, 128, 128), F32)
    b2, xo2, p1, s0, s1 = call(
        down2_body, "down2", [idx, coef],
        [*trade(x2, p2, s0, s1), st2, st2o, own2, bf(plane[2].T), rz2, x1["xs"], *a2e, *a2o, *zmats[2], owner2],
        [((3, 256, 128), F32), own2f, own1f, face1, face1], [y2, y2o],
    )
    p2, s0, s1 = call(
        bottom_body, "bottom", [idx, coef],
        [*trade(x1, p1, s0, s1), st1, st1o, own1, owner1, *a1e, *a1o, *zmats[1], xo2, owner2, x21["xs"]],
        [((3, 96, 128), F32), face21, face21], [y1, y1o],
    )
    p2, s0, s1 = call(
        up2_body, "up2", [idx, coef],
        [*trade(x21, p2, s0, s1), b2, st2, st2o, own2, owner2, *a2e, *a2o, *zmats[2], x20["xs"], plane["2e"], pz2],
        [own2f, face20, face20], [y2, y2o],
    )
    x, w, s0, s1 = call(
        rise4_body, "rise4", [idx], [*trade(x20, p2, s0, s1), plane[4], pz4, st4, x4, *mats4], [big, halves, msgx, msgx], [y4],
    )
    r, d, x, w, s0, s1 = call(
        functools.partial(mid4_body, 0), "mid4_0", [idx, coef], [*trade4(w, s0, s1), st4, b, x, x, *mats4],
        [big, big, big, halves, msgx, msgx], [y4, full],
    )
    r, d, x, w, s0, s1 = call(
        functools.partial(mid4_body, 1), "mid4", [idx, coef], [*trade4(w, s0, s1), st4, r, d, x, *mats4],
        [big, big, big, halves, msgx, msgx], [y4, full],
    )
    (out,) = call(
        last4_body, "last4", [idx, coef], [*trade4(w, s0, s1), st4, r, d, x], [((2, 3, NX * NY, NZ), F32)], [full],
    )
    return out.reshape(2, 3, NX, NY, NZ)


def solution(mesh):
    placed = (P(None, None, "gx", "gy", None), P("gx", "gy", None), P("gx", "gy", None), P())
    return jax.shard_map(
        local,
        mesh=mesh,
        in_specs=placed,
        out_specs=P(None, None, "gx", "gy", None),
        check_vma=False,
    )
```

```python
import functools

import jax
import jax.numpy as jnp
import ml_dtypes
import numpy as np
from jax import lax
from jax.experimental import pallas as pl
from jax.experimental.pallas import tpu as pltpu
from jax.sharding import PartitionSpec as P

F32 = jnp.float32
BF16 = jnp.bfloat16
COUPLE = 2.5
NX, NY, NZ = 12, 16, 128
EX, EY = 3, 4
GX, GY = 16, 16

PROLONG = {
    4: np.array([[1.0, 0.0, 0.0], [0.375, 0.75, -0.125], [0.0, 1.0, 0.0], [-0.125, 0.75, 0.375]]),
    2: np.array([[1.0, 0.0], [0.5, 0.5]]),
}


def element_matrices(degree):
    points, weights = np.polynomial.legendre.leggauss(8)
    points, weights = 0.5 * (points + 1.0), 0.5 * weights
    nodes = np.arange(degree + 1) / degree
    values = np.zeros((degree + 1, points.size))
    slopes = np.zeros((degree + 1, points.size))
    for i in range(degree + 1):
        others = [j for j in range(degree + 1) if j != i]
        values[i] = np.prod([(points - nodes[j]) / (nodes[i] - nodes[j]) for j in others], axis=0)
        for k in others:
            rest = [(points - nodes[j]) / (nodes[i] - nodes[j]) for j in others if j != k]
            slopes[i] += np.prod(rest, axis=0) / (nodes[i] - nodes[k]) if rest else 1.0 / (nodes[i] - nodes[k])
    mass = (values * weights) @ values.T
    stiff = (slopes * weights) @ slopes.T
    mixed = (slopes * weights) @ values.T
    return [mass, stiff, mixed, mixed.T]


ELEMENTS = {p: element_matrices(p) for p in (4, 2, 1)}


def line_matrix(element, count):
    degree = element.shape[0] - 1
    full = np.zeros((degree * count + 1, degree * count + 1))
    for e in range(count):
        full[degree * e : degree * e + degree + 1, degree * e : degree * e + degree + 1] += element
    return full


def z_matrices(degree, copies):
    count = NZ // 4
    length = count * degree
    out = np.zeros((4, 128, 128))
    for k, element in enumerate(ELEMENTS[degree]):
        full = line_matrix(element, count)[:length, :length].copy()
        full[0, 0] += element[degree, degree]
        for v in range(copies):
            out[k, v * length : (v + 1) * length, v * length : (v + 1) * length] = full.T
    return out


def hi_lo(array):
    array = array.astype(np.float32)
    hi = array.astype(ml_dtypes.bfloat16)
    lo = (array - hi.astype(np.float32)).astype(ml_dtypes.bfloat16)
    return hi, lo


def prolong_line(degree, count):
    table = PROLONG[degree]
    half = degree // 2
    full = np.zeros((degree * count + 1, half * count + 1))
    for e in range(count):
        for a in range(degree):
            for t in range(table.shape[1]):
                full[degree * e + a, half * e + t] += table[a, t]
    full[-1, -1] = 1.0
    return full


def natural(degree, halo):
    return [
        (i, j)
        for i in range(-degree * halo, degree * (EX + halo) + 1)
        for j in range(-degree * halo, degree * (EY + halo) + 1)
    ]


def pad_to(n, m):
    return -(-n // m) * m


NODES4 = (
    [(i, j) for i in range(NX) for j in range(NY)]
    + [(NX, j) for j in range(NY)]
    + [(i, NY) for i in range(NX)]
    + [(NX, NY)]
)


def in_rings(degree, parts):
    nodes, seen = [], set()
    for halo, rows in enumerate(parts):
        ring = [n for n in natural(degree, halo) if n not in seen]
        seen.update(ring)
        nodes += ring + [None] * (rows - len(ring))
    return nodes


RINGS = {2: (64, 80, 112), 1: (32, 32, 32)}
NODES = {
    "4": NODES4,
    "2o": natural(2, 0),
    "2e": in_rings(2, RINGS[2]),
    "1o": natural(1, 0),
    "1e": in_rings(1, RINGS[1]),
}


def one_hot(rows, cols, pairs):
    out = np.zeros((rows, cols), np.float32)
    for r, c in pairs:
        out[r, c] = 1.0
    return out.astype(ml_dtypes.bfloat16)


def exchange_tables(degree, halo, own, ext, rows_own, rows_ext):
    bx, by = degree * EX, degree * EY
    layers = degree * halo + 1
    own_at = {node: r for r, node in enumerate(own)}
    xlo = [(i, j) for i in range(layers) for j in range(by + 1)]
    xhi = [(bx - layers + 1 + i, j) for i in range(layers) for j in range(by + 1)]
    nx = pad_to(len(xlo), 16)
    sources = [(node, r) for node, r in own_at.items()]
    sources += [((i - bx, j), rows_own + r) for r, (i, j) in enumerate(xhi)]
    sources += [((i + bx, j), rows_own + nx + r) for r, (i, j) in enumerate(xlo)]
    span = range(-degree * halo, bx + degree * halo + 1)
    ylo = [(i, j) for i in span for j in range(layers)]
    yhi = [(i, by - layers + 1 + j) for i in span for j in range(layers)]
    ny = pad_to(len(ylo), 16)
    xs = [one_hot(nx, rows_own, [(r, own_at[n]) for r, n in enumerate(face)]) for face in (xlo, xhi)]
    width = rows_own + 2 * nx
    ys = [
        one_hot(ny, width, [(r, c) for r, n in enumerate(face) for node, c in sources if node == n])
        for face in (ylo, yhi)
    ]
    sources2 = list(sources)
    sources2 += [((i, j - by), width + r) for r, (i, j) in enumerate(yhi)]
    sources2 += [((i, j + by), width + ny + r) for r, (i, j) in enumerate(ylo)]
    ext_at = {node: r for r, node in enumerate(ext) if node is not None}
    total = one_hot(rows_ext, width + 2 * ny, [(ext_at[n], c) for n, c in sources2 if n in ext_at])
    return {
        "nx": nx,
        "ny": ny,
        "xs": np.concatenate(xs, 0),
        "ys": np.concatenate(ys, 0),
        "sum": total,
    }


EXCH = {
    "2": exchange_tables(2, 2, NODES["2o"], NODES["2e"], 64, 256),
    "20": exchange_tables(2, 0, NODES["2o"], NODES["2o"], 64, 64),
    "1": exchange_tables(1, 2, NODES["1o"], NODES["1e"], 32, 96),
}


def side_by_side(a, own_a, b, own_b):
    own, nx, ny = own_a + own_b, a["nx"] + b["nx"], a["ny"] + b["ny"]
    out = {"nx": nx, "ny": ny}
    spread = lambda t, o, first: np.concatenate(
        [
            np.arange(o) + (0 if first else own_a),
            *(own + k * nx + (0 if first else a["nx"]) + np.arange(t["nx"]) for k in range(2)),
            *(own + 2 * nx + k * ny + (0 if first else a["ny"]) + np.arange(t["ny"]) for k in range(2)),
        ]
    )
    for key, width, step in (("xs", own, "nx"), ("ys", own + 2 * nx, "ny")):
        blocks = []
        for k in range(2):
            for t, o, first in ((a, own_a, True), (b, own_b, False)):
                rows = t[key][k * t[step] : (k + 1) * t[step]]
                block = np.zeros((rows.shape[0], width), ml_dtypes.bfloat16)
                block[:, spread(t, o, first)[: rows.shape[1]]] = rows
                blocks.append(block)
        out[key] = np.concatenate(blocks, 0)
    return out


EXCH["21"] = side_by_side(EXCH["2"], 64, EXCH["1"], 32)


def setup_table(degree, nodes, rows, halo):
    out = np.zeros((rows, 128), np.float32)
    for r, node in enumerate(nodes):
        if node is not None:
            out[r, node[0] + degree * halo] = out[r, 32 + node[1] + degree * halo] = 1.0
    parts = [out]
    for wide in (True, False) if halo else (False,):
        grow, start = (halo, 0) if wide else (0, degree * halo)
        for element in ELEMENTS[degree]:
            table = np.zeros((32, 128), np.float32)
            for at, count in ((0, EX + 2 * grow), (32, EY + 2 * grow)):
                n = degree * count + 1
                table[start : start + n, at + start : at + start + n] = line_matrix(element, count)
            parts.append(table)
    return np.concatenate(parts, 0)


def kd_tables(nodes, rows, degree):
    m = lambda a: ELEMENTS[degree][0][a % degree, a % degree] + (ELEMENTS[degree][0][degree, degree] if a % degree == 0 else 0.0)
    k = lambda a: ELEMENTS[degree][1][a % degree, a % degree] + (ELEMENTS[degree][1][degree, degree] if a % degree == 0 else 0.0)
    out = np.zeros((rows, 8), np.float32)
    for r, node in enumerate(nodes):
        if node is None:
            continue
        i, j = node
        for c in range(3):
            co = [1.0 + COUPLE * (c == e) for e in range(3)]
            out[r, c] = co[0] * k(i) * m(j) + co[1] * m(i) * k(j)
            out[r, 3 + c] = co[2] * m(i) * m(j)
    copies = {4: 1, 2: 2, 1: 2}[degree]
    length = NZ // 4 * degree
    lanes = np.zeros((8, 128), np.float32)
    for z in range(length):
        for v in range(copies):
            lanes[0, v * length + z] = m(z)
            lanes[1, v * length + z] = k(z)
    return out, lanes


def dot(a, b):
    return jnp.dot(a, b, preferred_element_type=F32)


def split(v):
    hi = v.astype(BF16)
    return hi, (v - hi.astype(F32)).astype(BF16)


def sel(exact, v):
    hi, lo = split(v)
    return dot(exact, hi) + dot(exact, lo)


def sel3(exact, v):
    hi = v.astype(BF16)
    rest = v - hi.astype(F32)
    mid = rest.astype(BF16)
    lo = (rest - mid.astype(F32)).astype(BF16)
    return dot(exact, hi) + dot(exact, mid) + dot(exact, lo)


def rsel(v, exact):
    hi, lo = split(v)
    return dot(hi, exact) + dot(lo, exact)


def rsel3(v, exact):
    hi = v.astype(BF16)
    rest = v - hi.astype(F32)
    mid = rest.astype(BF16)
    lo = (rest - mid.astype(F32)).astype(BF16)
    return dot(hi, exact) + dot(mid, exact) + dot(lo, exact)


def place(idx_ref, axis):
    at = idx_ref[0]
    at = (at >> 4) if axis == 0 else (at & 15)
    even = (at & 1) == 0
    return even, (at > 0).astype(F32), (at < (GX, GY)[axis] - 1).astype(F32)


def for_pairs(idx_ref, axis, lo, hi):
    even, _, _ = place(idx_ref, axis)
    return jnp.where(even, hi, lo), jnp.where(even, lo, hi)


def from_pairs(idx_ref, axis, r0, r1):
    even, has_lo, has_hi = place(idx_ref, axis)
    return jnp.where(even, r1, r0) * has_lo, jnp.where(even, r0, r1) * has_hi


def stiffness(fields, ahi, alo, bhi, blo, y_ref, rows):
    cols, block = ahi.shape[2], ahi.shape[1] // 4
    for s in range(3):
        u = fields[s]
        if cols != u.shape[0]:
            u = jnp.concatenate([u, jnp.zeros((cols - u.shape[0], u.shape[1]), F32)], 0)
        uh, ul = split(u)
        if rows == block:
            high, low = ahi[s], alo[s]
        else:
            high, low = (jnp.concatenate([m[s, block * k : block * k + rows, :] for k in range(4)], 0) for m in (ahi, alo))
        if u.shape[1] == 128:
            both = dot(high, jnp.concatenate([uh, ul], 1))
            y_ref[s, : 4 * rows] = both[:, :128] + both[:, 128:] + dot(low, uh)
        else:
            y_ref[s, : 4 * rows] = dot(high, uh) + dot(high, ul) + dot(low, uh)
    part = lambda s, k: y_ref[s, k * rows : (k + 1) * rows, :]
    plans = (
        (lambda: part(0, 0) + part(1, 2), lambda: part(0, 1), lambda: part(2, 2), 3),
        (lambda: part(1, 0) + part(0, 2), lambda: part(1, 1), lambda: part(2, 3), 3),
        (lambda: part(2, 0), lambda: part(2, 1), lambda: part(0, 3) + part(1, 3), 2),
    )
    outs = []
    for first, second, third, mixed in plans:
        mats_h = jnp.concatenate([bhi[0], bhi[1], bhi[mixed]], 0)
        mats_l = jnp.concatenate([blo[0], blo[1], blo[mixed]], 0)
        one, two, three = first(), second(), third()
        halves = []
        for v in range(one.shape[1] // 128):
            cut = lambda t: t[:, 128 * v : 128 * v + 128]
            h, l = split(jnp.concatenate([cut(one), cut(two), cut(three)], 1))
            halves.append(dot(h, mats_h) + dot(l, mats_h) + dot(h, mats_l))
        outs.append(halves[0] if len(halves) == 1 else jnp.concatenate(halves, 1))
    return outs


def wide(v):
    return jnp.concatenate([v, v], 1)


VMEM = pl.BlockSpec(memory_space=pltpu.VMEM)
SMEM = pl.BlockSpec(memory_space=pltpu.SMEM)


def call(body, name, smem, args, outs, scratch=(), flops=1000000, limit=40):
    return pl.pallas_call(
        body,
        name=name,
        out_shape=[jax.ShapeDtypeStruct(shape, dtype) for shape, dtype in outs],
        in_specs=[SMEM] * len(smem) + [VMEM] * len(args),
        out_specs=[VMEM] * len(outs),
        scratch_shapes=list(scratch),
        compiler_params=pltpu.CompilerParams(vmem_limit_bytes=limit * 2**20),
        cost_estimate=pl.CostEstimate(flops=flops, bytes_accessed=100000, transcendentals=0),
    )(*smem, *args)


def setup_body(rows_in, plans, idx_ref, c_ref, *refs):
    *outs, xe_ref, ye_ref = refs
    at = idx_ref[0]
    hdot = functools.partial(jnp.dot, preferred_element_type=F32, precision=lax.Precision.HIGHEST)
    tdot = lambda a, b: lax.dot_general(
        a, b, (((1,), (1,)), ((), ())), preferred_element_type=F32, precision=lax.Precision.HIGHEST
    )
    m, k, g, t = range(4)
    strong = 1.0 + COUPLE
    for p, (rows, cols, corner, corr) in enumerate(plans):
        for q in range(4):
            table = c_ref[rows_in + 128 * p + 32 * q : rows_in + 128 * p + 32 * q + 32, :]
            x1, y1 = table[:, 0:32], table[:, 32:64]
            if corner is not None:
                i, j = (lax.broadcasted_iota(jnp.int32, (32, 32), d) for d in (0, 1))
                spot = jnp.where((i == corner) & (j == corner), corr[q], 0.0)
                x1 = x1 + spot * ((at >> 4) == 0).astype(F32)
                y1 = y1 + spot * ((at & 15) == 0).astype(F32)
            ox, oy = c_ref[0:rows_in, 0:32], c_ref[0:rows_in, 32:64]
            xe_ref[q, :rows, :cols] = tdot(hdot(ox[:rows], x1), ox[:cols])
            ye_ref[q, :rows, :cols] = tdot(hdot(oy[:rows], y1), oy[:cols])
        xy = lambda a, b: xe_ref[a, :rows, :cols] * ye_ref[b, :rows, :cols]
        blocks = (
            (lambda: strong * xy(k, m) + xy(m, k), lambda: xy(m, m), lambda: COUPLE * xy(t, g), lambda: COUPLE * xy(t, m)),
            (lambda: xy(k, m) + strong * xy(m, k), lambda: xy(m, m), lambda: COUPLE * xy(g, t), lambda: COUPLE * xy(m, t)),
            (lambda: xy(k, m) + xy(m, k), lambda: strong * xy(m, m), lambda: COUPLE * xy(g, m), lambda: COUPLE * xy(m, g)),
        )
        for s in range(3):
            for b in range(4):
                hi, lo = split(blocks[s][b]())
                outs[2 * p][s, b * rows : (b + 1) * rows, :] = hi
                outs[2 * p + 1][s, b * rows : (b + 1) * rows, :] = lo
    if len(outs) > 2 * len(plans):
        outs[-1][...] = jnp.zeros((8, 128), F32)


def plane_matrices(idx, degree, table, rows_in, halo, sizes, token=False):
    corr = [float(np.float32(e[degree, degree])) for e in ELEMENTS[degree]]
    plans = [(*sizes[-1], degree * halo, corr)]
    if halo:
        plans = [(*sizes[0], None, None)] + plans
    outs = [((3, 4 * r, c), BF16) for r, c, *_ in plans for _ in range(2)]
    return call(
        functools.partial(setup_body, rows_in, plans),
        "setup_" + str(degree),
        [idx],
        [table],
        outs + ([((8, 128), F32)] if token else []),
        [pltpu.VMEM((4, rows_in, rows_in), F32), pltpu.VMEM((4, rows_in, rows_in), F32)],
    )


NX2, NY2 = EXCH["2"]["nx"], EXCH["2"]["ny"]


def pack_x_body(idx_ref, modes_ref, w_ref, pin_ref, c_ref, own_ref, s0_ref, s1_ref, line_ref, m_ref):
    w = w_ref[...]
    m = 1.0 - pin_ref[...].astype(F32)
    m_ref[...] = m
    pick = c_ref[0:64, 0 : NX * NY]
    own = rsel3(sel3(pick, w), c_ref[64:192, 0:128]) + rsel(sel(pick, m), c_ref[64:192, 128:256])
    own_ref[...] = own
    faces = sel3(c_ref[192 : 192 + 2 * NX2, 0:64], own)
    a, b = for_pairs(idx_ref, 0, faces[:NX2], faces[NX2:])
    for ref, face in ((s0_ref, a), (s1_ref, b)):
        for v in range(2):
            for c in range(3):
                ref[16 * (3 * v + c) : 16 * (3 * v + c) + 16, :] = modes_ref[v, c, 0:16, :]
        ref[96:112, :] = w[0:16]
        ref[112:128, :] = m[0:16]
        ref[128 : 128 + NX2, :] = face
    line_ref[...] = jnp.zeros((128, 128), F32)
    for k in range(8):
        if k < 6:
            line = modes_ref[k // 3, k % 3, pl.ds(0, NX, stride=NY), :]
        else:
            line = (w_ref if k == 6 else m_ref)[pl.ds(0, NX, stride=NY), :]
        line_ref[16 * k : 16 * k + NX, :] = line


def pack_y_body(idx_ref, line_ref, own_ref, r0_ref, r1_ref, ys_ref, token_ref, s0_ref, s1_ref):
    lo, hi = from_pairs(idx_ref, 0, r0_ref[...], r1_ref[...])
    stack = jnp.concatenate([own_ref[...], lo[128:], hi[128:]], 0)
    faces = sel3(ys_ref[...], stack)
    a, b = for_pairs(idx_ref, 1, faces[:NY2], faces[NY2:])
    for ref, face in ((s0_ref, a), (s1_ref, b)):
        ref[0:128, :] = line_ref[...]
        for k in range(8):
            ref[16 * k + NX : 16 * k + NX + 1, :] = hi[16 * k : 16 * k + 1]
        ref[128 : 128 + NY2, :] = face


def static_of(w, m, kd, lanes):
    s = w * m
    f = 1.0 - m
    s2 = s * s
    inv = [1.0 / (s2 * (kd[:, c : c + 1] * lanes[0:1] + kd[:, 3 + c : 4 + c] * lanes[1:2]) + f) for c in range(3)]
    return s, f, inv


def statics_body(
    idx_ref, own_ref, rx0_ref, rx1_ref, ry0_ref, ry1_ref, sum_ref, d_ref, pick1_ref, kd2_ref, l2_ref, kd1_ref, l1_ref,
    e2_ref, e1_ref,
):
    xlo, xhi = from_pairs(idx_ref, 0, rx0_ref[128:, :], rx1_ref[128:, :])
    ylo, yhi = from_pairs(idx_ref, 1, ry0_ref[128:, :], ry1_ref[128:, :])
    ext = sel3(sum_ref[...], jnp.concatenate([own_ref[...], xlo, xhi, ylo, yhi], 0))

    def put(ref, w, m, kd, lanes):
        s, f, inv = static_of(w, m, kd, lanes)
        ref[0], ref[1] = s, f
        for c in range(3):
            ref[2 + c] = inv[c]

    put(e2_ref, rsel3(ext, d_ref[0]), rsel(ext, d_ref[1]), kd2_ref[...], l2_ref[...])
    coarse = sel3(pick1_ref[...], ext)
    put(e1_ref, rsel3(coarse, d_ref[2]), rsel(coarse, d_ref[3]), kd1_ref[...], l1_ref[...])


X4, Y4 = 24, 16


def faces_x4(idx_ref, outs, s0_ref, s1_ref):
    even, _, _ = place(idx_ref, 0)
    for c in range(3):
        w = outs[c]
        lo = jnp.concatenate([w[0:16], w[208:216]], 0)
        hi = jnp.concatenate([w[192:208], w[216:224]], 0)
        s0_ref[c] = jnp.where(even, hi, lo)
        s1_ref[c] = jnp.where(even, lo, hi)


LO16, HI16 = 16, 20


def faces_y4_body(idx_ref, w_ref, r0_ref, r1_ref, s0_ref, s1_ref):
    even, _, _ = place(idx_ref, 1)
    for c in range(3):
        xlo, xhi = from_pairs(idx_ref, 0, r0_ref[c], r1_ref[c])
        row = lax.broadcasted_iota(jnp.int32, (Y4, 256), 0)
        lo = jnp.concatenate([w_ref[2 * c + v, pl.ds(0, NX, stride=NY), :] for v in range(2)], 1)
        lo = jnp.concatenate([lo, jnp.concatenate([w_ref[2 * c + v, 192:196, :] for v in range(2)], 1)], 0)
        hi = jnp.concatenate([w_ref[2 * c + v, 208:224, :] for v in range(2)], 1)
        lo = lo + jnp.where(row == 0, xlo[0:1], 0.0) + jnp.where(row == NX, xhi[0:1], 0.0)
        hi = hi + jnp.where(row == 0, xlo[HI16 : HI16 + 1], 0.0) + jnp.where(row == NX, xhi[LO16 : LO16 + 1], 0.0)
        s0_ref[c] = jnp.where(even, hi, lo)
        s1_ref[c] = jnp.where(even, lo, hi)


def summed4(idx_ref, w_ref, rx0, rx1, ry0, ry1, full_ref):
    row = lax.broadcasted_iota(jnp.int32, (Y4, 256), 0)
    for c in range(3):
        xlo, xhi = from_pairs(idx_ref, 0, rx0[c], rx1[c])
        ylo, yhi = from_pairs(idx_ref, 1, ry0[c], ry1[c])
        yhi = jnp.where(row <= NX, yhi, 0.0)
        yhi = yhi + jnp.where(row == 0, xlo[HI16 : HI16 + 1], 0.0) + jnp.where(row == NX, xhi[LO16 : LO16 + 1], 0.0)
        end = xhi[0:16] + jnp.where(row == 0, ylo[NX : NX + 1], 0.0)
        for v in range(2):
            k, cut = 2 * c + v, slice(128 * v, 128 * v + 128)
            full_ref[k] = w_ref[k]
            full_ref[k, 0:16, :] += xlo[0:16, cut]
            full_ref[k, 192:208, :] += end[:, cut]
            full_ref[k, 208:224, :] += yhi[:, cut]
            full_ref[k, pl.ds(0, NX, stride=NY), :] += ylo[:NX, cut]


def put4(ref, outs):
    for c in range(3):
        for v in range(2):
            ref[2 * c + v] = outs[c][:, 128 * v : 128 * v + 128]


def first4_body(
    idx_ref, coef_ref, modes_ref, w_ref, pin_ref, rx0_ref, rx1_ref, ry0_ref, ry1_ref, kd_ref, lanes_ref, ahi, alo, bhi, blo,
    b_ref, st_ref, d_ref, out_ref, s0_ref, s1_ref, y_ref,
):
    _, xhi = from_pairs(idx_ref, 0, rx0_ref[0:128, :], rx1_ref[0:128, :])
    _, yhi = from_pairs(idx_ref, 1, ry0_ref[0:128, :], ry1_ref[0:128, :])

    def gathered(own, k):
        return jnp.concatenate([own, xhi[16 * k : 16 * k + 16], yhi[16 * k : 16 * k + 16]], 0)

    w = gathered(w_ref[...], 6)
    m = gathered(1.0 - pin_ref[...].astype(F32), 7)
    s, f, inv = static_of(w, m, kd_ref[...], lanes_ref[...])
    st_ref[0], st_ref[1] = s, f
    for c in range(3):
        st_ref[2 + c] = inv[c]
    fields = []
    for c in range(3):
        b = jnp.concatenate([gathered(modes_ref[v, c], 3 * v + c) for v in range(2)], 1)
        b_ref[c] = b
        d = wide(inv[c]) * b * coef_ref[0, 0]
        d_ref[c] = d
        fields.append(wide(s) * d)
    outs = stiffness(fields, ahi, alo, bhi, blo, y_ref, 224)
    put4(out_ref, outs)
    faces_x4(idx_ref, outs, s0_ref, s1_ref)


def both4(ref, c):
    return jnp.concatenate([ref[2 * c], ref[2 * c + 1]], 1)


def update4(idx_ref, coef_ref, step, w_ref, recv, st_ref, r_ref, d_ref, full_ref, c):
    s, f, inv = wide(st_ref[0]), wide(st_ref[1]), wide(st_ref[2 + c])
    r = r_ref[c] - (s * both4(full_ref, c) + f * d_ref[c])
    if step == 0:
        d = coef_ref[0, 0] * inv * r
    else:
        d = coef_ref[0, 2 * step - 1] * d_ref[c] + coef_ref[0, 2 * step] * inv * r
    return s, f, r, d


def mid4_body(
    step, idx_ref, coef_ref, w_ref, rx0, rx1, ry0, ry1, st_ref, r_ref, d_ref, x_ref, ahi, alo, bhi, blo,
    r_out, d_out, x_out, out_ref, s0_ref, s1_ref, y_ref, full_ref,
):
    summed4(idx_ref, w_ref, rx0, rx1, ry0, ry1, full_ref)
    fields = []
    for c in range(3):
        s, f, r, d = update4(idx_ref, coef_ref, step, w_ref, None, st_ref, r_ref, d_ref, full_ref, c)
        r_out[c], d_out[c] = r, d
        x_out[c] = x_ref[c] + d
        fields.append(s * d)
    outs = stiffness(fields, ahi, alo, bhi, blo, y_ref, 224)
    put4(out_ref, outs)
    faces_x4(idx_ref, outs, s0_ref, s1_ref)


def resid4_body(
    idx_ref, coef_ref, w_ref, rx0, rx1, ry0, ry1, st_ref, r_ref, d_ref, x_ref, ahi, alo, bhi, blo, rxy_ref, rz_ref, xs_ref,
    x_out, p_ref, s0_ref, s1_ref, y_ref, full_ref, keep_ref,
):
    summed4(idx_ref, w_ref, rx0, rx1, ry0, ry1, full_ref)
    fields = []
    owned = lax.broadcasted_iota(jnp.int32, (224, 256), 0) < NX * NY
    for c in range(3):
        s, f, r, d = update4(idx_ref, coef_ref, 2, w_ref, None, st_ref, r_ref, d_ref, full_ref, c)
        x_out[c] = x_ref[c] + d
        keep_ref[c] = jnp.where(owned, (1.0 - f) * r, 0.0)
        fields.append(s * d)
    outs = stiffness(fields, ahi, alo, bhi, blo, y_ref, 224)
    nx = xs_ref.shape[0] // 2
    for c in range(3):
        left = sel(rxy_ref[...], keep_ref[c] - wide(st_ref[0]) * outs[c])
        part = rsel(left[:, :128], rz_ref[0]) + rsel(left[:, 128:], rz_ref[1])
        p_ref[c] = part
        faces = sel(xs_ref[...], part)
        s0_ref[c], s1_ref[c] = for_pairs(idx_ref, 0, faces[:nx], faces[nx:])


def rise4_body(
    idx_ref, p_ref, rx0, rx1, ry0, ry1, sum_ref, pxy_ref, pz_ref, st_ref, x_ref, ahi, alo, bhi, blo,
    x_out, out_ref, s0_ref, s1_ref, y_ref,
):
    fields = []
    s, m = wide(st_ref[0]), 1.0 - wide(st_ref[1])
    for c in range(3):
        e = gather_sum(idx_ref, sum_ref, p_ref[c], rx0[c], rx1[c], ry0[c], ry1[c])
        e = sel(pxy_ref[...], e)
        x = x_ref[c] + m * jnp.concatenate([rsel(e, pz_ref[0]), rsel(e, pz_ref[1])], 1)
        x_out[c] = x
        fields.append(s * x)
    outs = stiffness(fields, ahi, alo, bhi, blo, y_ref, 224)
    put4(out_ref, outs)
    faces_x4(idx_ref, outs, s0_ref, s1_ref)


def last4_body(idx_ref, coef_ref, w_ref, rx0, rx1, ry0, ry1, st_ref, r_ref, d_ref, x_ref, out_ref, full_ref):
    summed4(idx_ref, w_ref, rx0, rx1, ry0, ry1, full_ref)
    for c in range(3):
        _, _, _, d = update4(idx_ref, coef_ref, 2, w_ref, None, st_ref, r_ref, d_ref, full_ref, c)
        x = x_ref[c] + d
        for v in range(2):
            out_ref[v, c] = x[: NX * NY, 128 * v : 128 * v + 128]


def gather_sum(idx_ref, sum_ref, own, rx0, rx1, ry0, ry1):
    xlo, xhi = from_pairs(idx_ref, 0, rx0, rx1)
    ylo, yhi = from_pairs(idx_ref, 1, ry0, ry1)
    return sel(sum_ref[...], jnp.concatenate([own, xlo, xhi, ylo, yhi], 0))


def faces_y_body(idx_ref, p_ref, r0_ref, r1_ref, ys_ref, s0_ref, s1_ref):
    ny = ys_ref.shape[0] // 2
    for c in range(3):
        lo, hi = from_pairs(idx_ref, 0, r0_ref[c], r1_ref[c])
        faces = sel(ys_ref[...], jnp.concatenate([p_ref[c], lo, hi], 0))
        s0_ref[c], s1_ref[c] = for_pairs(idx_ref, 1, faces[:ny], faces[ny:])


def smooth(level, degree, coef_ref, st_ref, b, x, steps, mats, y_ref):
    sizes = list(np.cumsum(RINGS[degree])[::-1])
    n = int(sizes.pop(0))

    def residual(r, v):
        nonlocal n
        u = [st_ref[0, :n] * t for t in v]
        n = int(sizes.pop(0))
        outs = stiffness(u, *mats, y_ref, n)
        s, f = st_ref[0, :n], st_ref[1, :n]
        return [a[:n] - (s * w + f * t[:n]) for a, w, t in zip(r, outs, v)]

    r = b if x is None else residual(b, x)
    d = [st_ref[2 + c, :n] * r[c] * coef_ref[level, 0] for c in range(3)]
    x = d if x is None else [a[:n] + t for a, t in zip(x, d)]
    for step in range(1, steps):
        r = residual(r, d)
        d = [coef_ref[level, 2 * step - 1] * d[c][:n] + coef_ref[level, 2 * step] * st_ref[2 + c, :n] * r[c] for c in range(3)]
        x = [a[:n] + t for a, t in zip(x, d)]
    return r, d, x


def down2_body(
    idx_ref, coef_ref, p_ref, rx0, rx1, ry0, ry1, sum_ref, st_ref, rxy_ref, rz_ref, xs_ref,
    ahi, alo, ohi, olo, bhi, blo, owner_ref,
    b_out, x_out, p_out, s0_ref, s1_ref, y_ref,
):
    m = 1.0 - st_ref[1]
    b = []
    for c in range(3):
        b.append(m * gather_sum(idx_ref, sum_ref, p_ref[c], rx0[c], rx1[c], ry0[c], ry1[c]))
        b_out[c] = b[c]
    r, d, x = smooth(1, 2, coef_ref, st_ref, b, None, 3, (ahi, alo, bhi, blo), y_ref)
    s = st_ref[0, :64]
    outs = stiffness([s * t for t in d], ohi, olo, bhi, blo, y_ref, 64)
    nx = xs_ref.shape[0] // 2
    for c in range(3):
        x_out[c] = x[c]
        left = owner_ref[...] * m[:64] * r[c] - s * outs[c]
        part = rsel(sel(rxy_ref[...], left), rz_ref[...])
        p_out[c] = part
        faces = sel(xs_ref[...], part)
        s0_ref[c], s1_ref[c] = for_pairs(idx_ref, 0, faces[:nx], faces[nx:])


def tail(level, last, coef_ref, owner_ref, st_ref, r, d, x, outs, c):
    n = x[c].shape[0]
    c1, c2 = coef_ref[level, 2 * last - 1], coef_ref[level, 2 * last]
    s, f, inv = st_ref[0, :n], st_ref[1, :n], st_ref[2 + c, :n]
    return owner_ref[...] * (x[c] + c1 * d[c] + c2 * inv * (r[c] - f * d[c])) - c2 * inv * s * outs[c]


def bottom_body(
    idx_ref, coef_ref, p_ref, rx0, rx1, ry0, ry1, sum_ref, st_ref, owner_ref, ahi, alo, ohi, olo, bhi, blo,
    x2_ref, owner2_ref, xs_ref,
    p_out, s0_ref, s1_ref, y_ref,
):
    m = 1.0 - st_ref[1]
    b = [m * gather_sum(idx_ref, sum_ref, p_ref[c], rx0[c], rx1[c], ry0[c], ry1[c]) for c in range(3)]
    r, d, x = smooth(2, 1, coef_ref, st_ref, b, None, 3, (ahi, alo, bhi, blo), y_ref)
    outs = stiffness([st_ref[0, :32] * t for t in d], ohi, olo, bhi, blo, y_ref, 32)
    nx = xs_ref.shape[0] // 2
    for c in range(3):
        e = tail(2, 3, coef_ref, owner_ref, st_ref, r, d, x, outs, c)
        part = jnp.concatenate([owner2_ref[...] * x2_ref[c], e], 0)
        p_out[c] = part
        faces = sel(xs_ref[...], part)
        s0_ref[c], s1_ref[c] = for_pairs(idx_ref, 0, faces[:nx], faces[nx:])


def up2_body(
    idx_ref, coef_ref, p_ref, rx0, rx1, ry0, ry1, sum_ref, sum1_ref, b_ref, st_ref, owner_ref, ahi, alo, ohi, olo, bhi, blo, xs_ref,
    pxy_ref, pz_ref, p_out, s0_ref, s1_ref, y_ref,
):
    x = []
    for c in range(3):
        fine = gather_sum(idx_ref, sum_ref, p_ref[c, :64], rx0[c, :NX2], rx1[c, :NX2], ry0[c, :NY2], ry1[c, :NY2])
        e = gather_sum(idx_ref, sum1_ref, p_ref[c, 64:], rx0[c, NX2:], rx1[c, NX2:], ry0[c, NY2:], ry1[c, NY2:])
        x.append(fine + (1.0 - st_ref[1]) * rsel(sel(pxy_ref[...], e), pz_ref[...]))
    b = [b_ref[c] for c in range(3)]
    r, d, x = smooth(1, 2, coef_ref, st_ref, b, x, 2, (ahi, alo, bhi, blo), y_ref)
    outs = stiffness([st_ref[0, :64] * t for t in d], ohi, olo, bhi, blo, y_ref, 64)
    nx = xs_ref.shape[0] // 2
    for c in range(3):
        part = tail(1, 2, coef_ref, owner_ref, st_ref, r, d, x, outs, c)
        p_out[c] = part
        faces = sel(xs_ref[...], part)
        s0_ref[c], s1_ref[c] = for_pairs(idx_ref, 0, faces[:nx], faces[nx:])


def swap(axis, s0, s1):
    n = GX if axis == "gx" else GY
    even = [(i, i ^ 1) for i in range(n)]
    odd = [(i, (((i - 1) ^ 1) + 1) % n) for i in range(n)]
    return lax.ppermute(s0, axis, even), lax.ppermute(s1, axis, odd)


def chebyshev_table(spectrum):
    low, top = spectrum[:, 0], spectrum[:, 1]
    center, radius = 0.5 * (top + low), 0.5 * (top - low)
    ratio = center / radius
    rho = 1.0 / ratio
    columns = [1.0 / center]
    for _ in range(3):
        after = 1.0 / (2.0 * ratio - rho)
        columns += [after * rho, 2.0 * after / radius]
        rho = after
    return jnp.stack(columns, 1)


def interp_tables():
    plane = {}
    for key, degree, halo, fine, rows, coarse, rows_c in (
        (4, 4, 0, NODES["4"], 224, NODES["2o"], 64),
        (2, 2, 0, NODES["2o"], 64, NODES["1o"], 32),
        ("2e", 2, 2, NODES["2e"], 256, NODES["1e"], 96),
    ):
        px, py = prolong_line(degree, EX + 2 * halo), prolong_line(degree, EY + 2 * halo)
        f0, c0 = degree * halo, degree * halo // 2
        full = np.zeros((rows, rows_c))
        for r, q in ((r, q) for r in range(len(fine)) for q in range(len(coarse))):
            if fine[r] is not None and coarse[q] is not None:
                (i, j), (a, b) = fine[r], coarse[q]
                full[r, q] = px[i + f0, a + c0] * py[j + f0, b + c0]
        plane[key] = full.astype(ml_dtypes.bfloat16)
    z4 = prolong_line(4, 32)[:128, :64]
    z2 = prolong_line(2, 32)[:64, :32]
    pz4 = np.zeros((2, 128, 128))
    for v in range(2):
        pz4[v, 64 * v : 64 * v + 64, :] = z4.T
    pz2 = np.zeros((128, 128))
    for v in range(2):
        pz2[32 * v : 32 * v + 32, 64 * v : 64 * v + 64] = z2.T
    cast = lambda t: np.ascontiguousarray(t).astype(ml_dtypes.bfloat16)
    return plane, cast(pz4), cast(pz4.transpose(0, 2, 1)), cast(pz2), cast(pz2.T)


def local(modes, moduli, pinned, spectrum):
    idx = (lax.axis_index("gx") * 16 + lax.axis_index("gy")).astype(jnp.int32).reshape(1)
    coef = chebyshev_table(spectrum)
    modes = modes.reshape(2, 3, NX * NY, NZ)
    moduli = moduli.reshape(NX * NY, NZ)
    pinned = pinned.reshape(NX * NY, NZ)

    zmats = {p: hi_lo(z_matrices(p, 1 if p == 4 else 2)) for p in (4, 2, 1)}
    plane, pz4, rz4, pz2, rz2 = interp_tables()
    bf = lambda t: np.ascontiguousarray(t).astype(ml_dtypes.bfloat16)
    x2, x20, x1, x21 = EXCH["2"], EXCH["20"], EXCH["1"], EXCH["21"]

    at4 = {n: r for r, n in enumerate(NODES["4"])}
    at2e = {n: r for r, n in enumerate(NODES["2e"]) if n is not None}
    pick2 = one_hot(64, NX * NY, [(r, at4[(2 * i, 2 * j)]) for r, (i, j) in enumerate(NODES["2o"]) if i < 6 and j < 8])
    zw, zm = np.zeros((128, 128)), np.zeros((128, 128))
    dw, dm, d1w, d1m = (np.zeros((128, 128)) for _ in range(4))
    for k in range(64):
        zw[2 * k, k] = zm[2 * k, 64 + k] = 1.0
        for v in range(2):
            dw[k, 64 * v + k] = dm[64 + k, 64 * v + k] = 1.0
            if k % 2 == 0:
                d1w[k, 32 * v + k // 2] = d1m[64 + k, 32 * v + k // 2] = 1.0
    pick1 = one_hot(96, 256, [(r, at2e[(2 * n[0], 2 * n[1])]) for r, n in enumerate(NODES["1e"]) if n is not None])
    owner2, owner1 = np.zeros((64, 128), np.float32), np.zeros((32, 128), np.float32)
    for r, (i, j) in enumerate(NODES["2o"]):
        owner2[r] = float(i < 6 and j < 8)
    for r, (i, j) in enumerate(NODES["1o"]):
        owner1[r] = float(i < 3 and j < 4)
    kd4, l4 = kd_tables(NODES["4"], 224, 4)
    kd2, l2 = kd_tables(NODES["2e"], 256, 2)
    kd1, l1 = kd_tables(NODES["1e"], 96, 1)
    table4 = setup_table(4, NODES["4"], 256, 0)
    table2 = setup_table(2, NODES["2e"], 256, 2)
    table1 = setup_table(1, NODES["1e"], 96, 2)
    first = np.zeros((192 + 2 * NX2, 256))
    first[0:64, 0 : NX * NY] = pick2
    first[64:192, 0:128], first[64:192, 128:256] = zw, zm
    first[192:, 0:64] = x2["xs"]

    mx = 128 + x2["nx"]
    my = 128 + x2["ny"]
    q2own, sx0, sx1, line = call(
        pack_x_body, "pack_x", [idx], [modes, moduli, pinned, bf(first)],
        [((64, 128), F32), ((mx, 128), F32), ((mx, 128), F32), ((128, 128), F32)], [pltpu.VMEM((NX * NY, NZ), F32)],
    )
    rx0, rx1 = swap("gx", sx0, sx1)
    *a4, token = plane_matrices(idx, 4, table4, 256, 0, [(224, 256)], token=True)
    sy0, sy1 = call(
        pack_y_body, "pack_y", [idx], [line, q2own, rx0, rx1, x2["ys"], token], [((my, 128), F32), ((my, 128), F32)],
    )
    ry0, ry1 = swap("gy", sy0, sy1)
    mats2 = plane_matrices(idx, 2, table2, 256, 2, [(144, 256), (64, 64)])
    mats1 = plane_matrices(idx, 1, table1, 96, 2, [(64, 96), (32, 32)])

    big = ((3, 224, 256), F32)
    msgx, msgy = ((3, X4, 256), F32), ((3, Y4, 256), F32)
    y4 = pltpu.VMEM((3, 4 * 224, 256), F32)
    full = pltpu.VMEM((6, 224, 128), F32)
    keep = pltpu.VMEM((3, 224, 256), F32)
    halves = ((6, 224, 128), F32)
    mats4 = [*a4, *zmats[4]]

    b, st4, d, w, s0, s1 = call(
        first4_body, "first4", [idx, coef], [modes, moduli, pinned, rx0, rx1, ry0, ry1, kd4, l4, *mats4],
        [big, ((5, 224, 128), F32), big, halves, msgx, msgx], [y4],
    )
    st2, st1 = call(
        statics_body, "statics", [idx],
        [q2own, rx0, rx1, ry0, ry1, x2["sum"], bf(np.stack([dw, dm, d1w, d1m])), pick1, kd2, l2, kd1, l1],
        [((5, 256, 128), F32), ((5, 96, 128), F32)],
    )

    def trade4(w, s0, s1):
        r0, r1 = swap("gx", s0, s1)
        t0, t1 = call(faces_y4_body, "faces_y4", [idx], [w, r0, r1], [msgy, msgy])
        return [w, r0, r1, *swap("gy", t0, t1)]

    def trade(table, p, s0, s1, sums=None):
        r0, r1 = swap("gx", s0, s1)
        t0, t1 = call(faces_y_body, "faces_y", [idx], [p, r0, r1, table["ys"]], [((3, table["ny"], 128), F32)] * 2)
        return [p, r0, r1, *swap("gy", t0, t1), *([table["sum"]] if sums is None else sums)]

    got = trade4(w, s0, s1)
    r, d, x, w, s0, s1 = call(
        functools.partial(mid4_body, 1), "mid4", [idx, coef], [*got, st4, b, d, d, *mats4], [big, big, big, halves, msgx, msgx], [y4, full],
    )
    got = trade4(w, s0, s1)
    face2, face20, face1, face21 = (((3, t["nx"], 128), F32) for t in (x2, x20, x1, x21))
    own2f, own1f = ((3, 64, 128), F32), ((3, 32, 128), F32)
    x4, p2, s0, s1 = call(
        resid4_body, "resid4", [idx, coef], [*got, st4, r, d, x, *mats4, bf(plane[4].T), rz4, x2["xs"]],
        [big, own2f, face2, face2], [y4, full, keep],
    )
    y2, y1 = pltpu.VMEM((3, 4 * 144, 128), F32), pltpu.VMEM((3, 4 * 64, 128), F32)
    b2, xo2, p1, s0, s1 = call(
        down2_body, "down2", [idx, coef],
        [*trade(x2, p2, s0, s1), st2, bf(plane[2].T), rz2, x1["xs"], *mats2, *zmats[2], owner2],
        [((3, 256, 128), F32), own2f, own1f, face1, face1], [y2],
    )
    p2, s0, s1 = call(
        bottom_body, "bottom", [idx, coef],
        [*trade(x1, p1, s0, s1), st1, owner1, *mats1, *zmats[1], xo2, owner2, x21["xs"]],
        [((3, 96, 128), F32), face21, face21], [y1],
    )
    p2, s0, s1 = call(
        up2_body, "up2", [idx, coef],
        [*trade(x21, p2, s0, s1, (x2["sum"], x1["sum"])), b2, st2, owner2, *mats2, *zmats[2], x20["xs"], plane["2e"], pz2],
        [own2f, face20, face20], [y2],
    )
    x, w, s0, s1 = call(
        rise4_body, "rise4", [idx], [*trade(x20, p2, s0, s1), plane[4], pz4, st4, x4, *mats4], [big, halves, msgx, msgx], [y4],
    )
    r, d, x, w, s0, s1 = call(
        functools.partial(mid4_body, 0), "mid4_0", [idx, coef], [*trade4(w, s0, s1), st4, b, x, x, *mats4],
        [big, big, big, halves, msgx, msgx], [y4, full],
    )
    r, d, x, w, s0, s1 = call(
        functools.partial(mid4_body, 1), "mid4", [idx, coef], [*trade4(w, s0, s1), st4, r, d, x, *mats4],
        [big, big, big, halves, msgx, msgx], [y4, full],
    )
    (out,) = call(
        last4_body, "last4", [idx, coef], [*trade4(w, s0, s1), st4, r, d, x], [((2, 3, NX * NY, NZ), F32)], [full],
    )
    return out.reshape(2, 3, NX, NY, NZ)


def solution(mesh):
    placed = (P(None, None, "gx", "gy", None), P("gx", "gy", None), P("gx", "gy", None), P())
    return jax.shard_map(
        local,
        mesh=mesh,
        in_specs=placed,
        out_specs=P(None, None, "gx", "gy", None),
        check_vma=False,
    )
```

```python
import functools

import jax
import jax.numpy as jnp
import ml_dtypes
import numpy as np
from jax import lax
from jax.experimental import pallas as pl
from jax.experimental.pallas import tpu as pltpu
from jax.sharding import PartitionSpec as P

F32 = jnp.float32
BF16 = jnp.bfloat16
COUPLE = 2.5
NX, NY, NZ = 12, 16, 128
EX, EY = 3, 4
GX, GY = 16, 16

PROLONG = {
    4: np.array([[1.0, 0.0, 0.0], [0.375, 0.75, -0.125], [0.0, 1.0, 0.0], [-0.125, 0.75, 0.375]]),
    2: np.array([[1.0, 0.0], [0.5, 0.5]]),
}


def element_matrices(degree):
    points, weights = np.polynomial.legendre.leggauss(8)
    points, weights = 0.5 * (points + 1.0), 0.5 * weights
    nodes = np.arange(degree + 1) / degree
    values = np.zeros((degree + 1, points.size))
    slopes = np.zeros((degree + 1, points.size))
    for i in range(degree + 1):
        others = [j for j in range(degree + 1) if j != i]
        values[i] = np.prod([(points - nodes[j]) / (nodes[i] - nodes[j]) for j in others], axis=0)
        for k in others:
            rest = [(points - nodes[j]) / (nodes[i] - nodes[j]) for j in others if j != k]
            slopes[i] += np.prod(rest, axis=0) / (nodes[i] - nodes[k]) if rest else 1.0 / (nodes[i] - nodes[k])
    mass = (values * weights) @ values.T
    stiff = (slopes * weights) @ slopes.T
    mixed = (slopes * weights) @ values.T
    return [mass, stiff, mixed, mixed.T]


ELEMENTS = {p: element_matrices(p) for p in (4, 2, 1)}


def line_matrix(element, count):
    degree = element.shape[0] - 1
    full = np.zeros((degree * count + 1, degree * count + 1))
    for e in range(count):
        full[degree * e : degree * e + degree + 1, degree * e : degree * e + degree + 1] += element
    return full


def z_matrices(degree, copies):
    count = NZ // 4
    length = count * degree
    out = np.zeros((4, 128, 128))
    for k, element in enumerate(ELEMENTS[degree]):
        full = line_matrix(element, count)[:length, :length].copy()
        full[0, 0] += element[degree, degree]
        for v in range(copies):
            out[k, v * length : (v + 1) * length, v * length : (v + 1) * length] = full.T
    return out


def hi_lo(array):
    array = array.astype(np.float32)
    hi = array.astype(ml_dtypes.bfloat16)
    lo = (array - hi.astype(np.float32)).astype(ml_dtypes.bfloat16)
    return hi, lo


def prolong_line(degree, count):
    table = PROLONG[degree]
    half = degree // 2
    full = np.zeros((degree * count + 1, half * count + 1))
    for e in range(count):
        for a in range(degree):
            for t in range(table.shape[1]):
                full[degree * e + a, half * e + t] += table[a, t]
    full[-1, -1] = 1.0
    return full


def natural(degree, halo):
    return [
        (i, j)
        for i in range(-degree * halo, degree * (EX + halo) + 1)
        for j in range(-degree * halo, degree * (EY + halo) + 1)
    ]


def pad_to(n, m):
    return -(-n // m) * m


NODES4 = (
    [(i, j) for i in range(NX) for j in range(NY)]
    + [(NX, j) for j in range(NY)]
    + [(i, NY) for i in range(NX)]
    + [(NX, NY)]
)


def in_rings(degree, parts):
    nodes, seen = [], set()
    for halo, rows in enumerate(parts):
        ring = [n for n in natural(degree, halo) if n not in seen]
        seen.update(ring)
        nodes += ring + [None] * (rows - len(ring))
    return nodes


RINGS = {2: (64, 80, 112), 1: (32, 32, 32)}
NODES = {
    "4": NODES4,
    "2o": natural(2, 0),
    "2e": in_rings(2, RINGS[2]),
    "1o": natural(1, 0),
    "1e": in_rings(1, RINGS[1]),
}


def one_hot(rows, cols, pairs):
    out = np.zeros((rows, cols), np.float32)
    for r, c in pairs:
        out[r, c] = 1.0
    return out.astype(ml_dtypes.bfloat16)


def exchange_tables(degree, halo, own, ext, rows_own, rows_ext):
    bx, by = degree * EX, degree * EY
    layers = degree * halo + 1
    own_at = {node: r for r, node in enumerate(own)}
    xlo = [(i, j) for i in range(layers) for j in range(by + 1)]
    xhi = [(bx - layers + 1 + i, j) for i in range(layers) for j in range(by + 1)]
    nx = pad_to(len(xlo), 16)
    sources = [(node, r) for node, r in own_at.items()]
    sources += [((i - bx, j), rows_own + r) for r, (i, j) in enumerate(xhi)]
    sources += [((i + bx, j), rows_own + nx + r) for r, (i, j) in enumerate(xlo)]
    span = range(-degree * halo, bx + degree * halo + 1)
    ylo = [(i, j) for i in span for j in range(layers)]
    yhi = [(i, by - layers + 1 + j) for i in span for j in range(layers)]
    ny = pad_to(len(ylo), 16)
    xs = [one_hot(nx, rows_own, [(r, own_at[n]) for r, n in enumerate(face)]) for face in (xlo, xhi)]
    width = rows_own + 2 * nx
    ys = [
        one_hot(ny, width, [(r, c) for r, n in enumerate(face) for node, c in sources if node == n])
        for face in (ylo, yhi)
    ]
    sources2 = list(sources)
    sources2 += [((i, j - by), width + r) for r, (i, j) in enumerate(yhi)]
    sources2 += [((i, j + by), width + ny + r) for r, (i, j) in enumerate(ylo)]
    ext_at = {node: r for r, node in enumerate(ext) if node is not None}
    total = one_hot(rows_ext, width + 2 * ny, [(ext_at[n], c) for n, c in sources2 if n in ext_at])
    return {
        "nx": nx,
        "ny": ny,
        "xs": np.concatenate(xs, 0),
        "ys": np.concatenate(ys, 0),
        "sum": total,
    }


EXCH = {
    "2": exchange_tables(2, 2, NODES["2o"], NODES["2e"], 64, 256),
    "20": exchange_tables(2, 0, NODES["2o"], NODES["2o"], 64, 64),
    "1": exchange_tables(1, 2, NODES["1o"], NODES["1e"], 32, 96),
}


def side_by_side(a, own_a, b, own_b):
    own, nx, ny = own_a + own_b, a["nx"] + b["nx"], a["ny"] + b["ny"]
    out = {"nx": nx, "ny": ny}
    spread = lambda t, o, first: np.concatenate(
        [
            np.arange(o) + (0 if first else own_a),
            *(own + k * nx + (0 if first else a["nx"]) + np.arange(t["nx"]) for k in range(2)),
            *(own + 2 * nx + k * ny + (0 if first else a["ny"]) + np.arange(t["ny"]) for k in range(2)),
        ]
    )
    for key, width, step in (("xs", own, "nx"), ("ys", own + 2 * nx, "ny")):
        blocks = []
        for k in range(2):
            for t, o, first in ((a, own_a, True), (b, own_b, False)):
                rows = t[key][k * t[step] : (k + 1) * t[step]]
                block = np.zeros((rows.shape[0], width), ml_dtypes.bfloat16)
                block[:, spread(t, o, first)[: rows.shape[1]]] = rows
                blocks.append(block)
        out[key] = np.concatenate(blocks, 0)
    return out


EXCH["21"] = side_by_side(EXCH["2"], 64, EXCH["1"], 32)


def setup_table(degree, nodes, rows, halo):
    out = np.zeros((rows, 128), np.float32)
    for r, node in enumerate(nodes):
        if node is not None:
            out[r, node[0] + degree * halo] = out[r, 32 + node[1] + degree * halo] = 1.0
    parts = [out]
    for wide in (True, False) if halo else (False,):
        grow, start = (halo, 0) if wide else (0, degree * halo)
        for element in ELEMENTS[degree]:
            table = np.zeros((32, 128), np.float32)
            for at, count in ((0, EX + 2 * grow), (32, EY + 2 * grow)):
                n = degree * count + 1
                table[start : start + n, at + start : at + start + n] = line_matrix(element, count)
            parts.append(table)
    return np.concatenate(parts, 0)


def kd_tables(nodes, rows, degree):
    m = lambda a: ELEMENTS[degree][0][a % degree, a % degree] + (ELEMENTS[degree][0][degree, degree] if a % degree == 0 else 0.0)
    k = lambda a: ELEMENTS[degree][1][a % degree, a % degree] + (ELEMENTS[degree][1][degree, degree] if a % degree == 0 else 0.0)
    out = np.zeros((rows, 8), np.float32)
    for r, node in enumerate(nodes):
        if node is None:
            continue
        i, j = node
        for c in range(3):
            co = [1.0 + COUPLE * (c == e) for e in range(3)]
            out[r, c] = co[0] * k(i) * m(j) + co[1] * m(i) * k(j)
            out[r, 3 + c] = co[2] * m(i) * m(j)
    copies = {4: 1, 2: 2, 1: 2}[degree]
    length = NZ // 4 * degree
    lanes = np.zeros((8, 128), np.float32)
    for z in range(length):
        for v in range(copies):
            lanes[0, v * length + z] = m(z)
            lanes[1, v * length + z] = k(z)
    return out, lanes


def dot(a, b):
    return jnp.dot(a, b, preferred_element_type=F32)


def split(v):
    hi = v.astype(BF16)
    return hi, (v - hi.astype(F32)).astype(BF16)


def sel(exact, v):
    hi, lo = split(v)
    return dot(exact, hi) + dot(exact, lo)


def sel3(exact, v):
    hi = v.astype(BF16)
    rest = v - hi.astype(F32)
    mid = rest.astype(BF16)
    lo = (rest - mid.astype(F32)).astype(BF16)
    return dot(exact, hi) + dot(exact, mid) + dot(exact, lo)


def rsel(v, exact):
    hi, lo = split(v)
    return dot(hi, exact) + dot(lo, exact)


def rsel3(v, exact):
    hi = v.astype(BF16)
    rest = v - hi.astype(F32)
    mid = rest.astype(BF16)
    lo = (rest - mid.astype(F32)).astype(BF16)
    return dot(hi, exact) + dot(mid, exact) + dot(lo, exact)


def place(idx_ref, axis):
    at = idx_ref[0]
    at = (at >> 4) if axis == 0 else (at & 15)
    even = (at & 1) == 0
    return even, (at > 0).astype(F32), (at < (GX, GY)[axis] - 1).astype(F32)


def for_pairs(idx_ref, axis, lo, hi):
    even, _, _ = place(idx_ref, axis)
    return jnp.where(even, hi, lo), jnp.where(even, lo, hi)


def from_pairs(idx_ref, axis, r0, r1):
    even, has_lo, has_hi = place(idx_ref, axis)
    return jnp.where(even, r1, r0) * has_lo, jnp.where(even, r0, r1) * has_hi


def stiffness(fields, ahi, alo, bhi, blo, y_ref, rows, picks=None):
    cols, block = ahi.shape[2], ahi.shape[1] // 4
    for s in range(3):
        u = fields[s]
        if cols != u.shape[0]:
            u = jnp.concatenate([u, jnp.zeros((cols - u.shape[0], u.shape[1]), F32)], 0)
        uh, ul = split(u)
        if rows == block:
            high, low = ahi[s], alo[s]
        else:
            spans = [(block * k + a, block * k + b) for k in range(4) for a, b in picks or ((0, rows),)]
            high, low = (jnp.concatenate([m[s, a:b, :] for a, b in spans], 0) for m in (ahi, alo))
        if u.shape[1] == 128:
            both = dot(high, jnp.concatenate([uh, ul], 1))
            y_ref[s, : 4 * rows] = both[:, :128] + both[:, 128:] + dot(low, uh)
        else:
            y_ref[s, : 4 * rows] = dot(high, uh) + dot(high, ul) + dot(low, uh)
    part = lambda s, k: y_ref[s, k * rows : (k + 1) * rows, :]
    plans = (
        (lambda: part(0, 0) + part(1, 2), lambda: part(0, 1), lambda: part(2, 2), 3),
        (lambda: part(1, 0) + part(0, 2), lambda: part(1, 1), lambda: part(2, 3), 3),
        (lambda: part(2, 0), lambda: part(2, 1), lambda: part(0, 3) + part(1, 3), 2),
    )
    outs = []
    for first, second, third, mixed in plans:
        mats_h = jnp.concatenate([bhi[0], bhi[1], bhi[mixed]], 0)
        mats_l = jnp.concatenate([blo[0], blo[1], blo[mixed]], 0)
        one, two, three = first(), second(), third()
        halves = []
        for v in range(one.shape[1] // 128):
            cut = lambda t: t[:, 128 * v : 128 * v + 128]
            h, l = split(jnp.concatenate([cut(one), cut(two), cut(three)], 1))
            halves.append(dot(h, mats_h) + dot(l, mats_h) + dot(h, mats_l))
        outs.append(halves[0] if len(halves) == 1 else jnp.concatenate(halves, 1))
    return outs


def wide(v):
    return jnp.concatenate([v, v], 1)


VMEM = pl.BlockSpec(memory_space=pltpu.VMEM)
SMEM = pl.BlockSpec(memory_space=pltpu.SMEM)


def call(body, name, smem, args, outs, scratch=(), flops=1000000, limit=40):
    return pl.pallas_call(
        body,
        name=name,
        out_shape=[jax.ShapeDtypeStruct(shape, dtype) for shape, dtype in outs],
        in_specs=[SMEM] * len(smem) + [VMEM] * len(args),
        out_specs=[VMEM] * len(outs),
        scratch_shapes=list(scratch),
        compiler_params=pltpu.CompilerParams(vmem_limit_bytes=limit * 2**20),
        cost_estimate=pl.CostEstimate(flops=flops, bytes_accessed=100000, transcendentals=0),
    )(*smem, *args)


def setup_body(rows_in, plans, idx_ref, c_ref, *refs):
    *outs, xe_ref, ye_ref = refs
    at = idx_ref[0]
    hdot = functools.partial(jnp.dot, preferred_element_type=F32, precision=lax.Precision.HIGHEST)
    tdot = lambda a, b: lax.dot_general(
        a, b, (((1,), (1,)), ((), ())), preferred_element_type=F32, precision=lax.Precision.HIGHEST
    )
    m, k, g, t = range(4)
    strong = 1.0 + COUPLE
    for p, (rows, cols, corner, corr) in enumerate(plans):
        for q in range(4):
            table = c_ref[rows_in + 128 * p + 32 * q : rows_in + 128 * p + 32 * q + 32, :]
            x1, y1 = table[:, 0:32], table[:, 32:64]
            if corner is not None:
                i, j = (lax.broadcasted_iota(jnp.int32, (32, 32), d) for d in (0, 1))
                spot = jnp.where((i == corner) & (j == corner), corr[q], 0.0)
                x1 = x1 + spot * ((at >> 4) == 0).astype(F32)
                y1 = y1 + spot * ((at & 15) == 0).astype(F32)
            ox, oy = c_ref[0:rows_in, 0:32], c_ref[0:rows_in, 32:64]
            xe_ref[q, :rows, :cols] = tdot(hdot(ox[:rows], x1), ox[:cols])
            ye_ref[q, :rows, :cols] = tdot(hdot(oy[:rows], y1), oy[:cols])
        xy = lambda a, b: xe_ref[a, :rows, :cols] * ye_ref[b, :rows, :cols]
        blocks = (
            (lambda: strong * xy(k, m) + xy(m, k), lambda: xy(m, m), lambda: COUPLE * xy(t, g), lambda: COUPLE * xy(t, m)),
            (lambda: xy(k, m) + strong * xy(m, k), lambda: xy(m, m), lambda: COUPLE * xy(g, t), lambda: COUPLE * xy(m, t)),
            (lambda: xy(k, m) + xy(m, k), lambda: strong * xy(m, m), lambda: COUPLE * xy(g, m), lambda: COUPLE * xy(m, g)),
        )
        for s in range(3):
            for b in range(4):
                hi, lo = split(blocks[s][b]())
                outs[2 * p][s, b * rows : (b + 1) * rows, :] = hi
                outs[2 * p + 1][s, b * rows : (b + 1) * rows, :] = lo
    if len(outs) > 2 * len(plans):
        outs[-1][...] = jnp.zeros((8, 128), F32)


def plane_matrices(idx, degree, table, rows_in, halo, sizes, token=False):
    corr = [float(np.float32(e[degree, degree])) for e in ELEMENTS[degree]]
    plans = [(*sizes[-1], degree * halo, corr)]
    if halo:
        plans = [(*sizes[0], None, None)] + plans
    outs = [((3, 4 * r, c), BF16) for r, c, *_ in plans for _ in range(2)]
    return call(
        functools.partial(setup_body, rows_in, plans),
        "setup_" + str(degree),
        [idx],
        [table],
        outs + ([((8, 128), F32)] if token else []),
        [pltpu.VMEM((4, rows_in, rows_in), F32), pltpu.VMEM((4, rows_in, rows_in), F32)],
    )


NX2, NY2 = EXCH["2"]["nx"], EXCH["2"]["ny"]


def pack_x_body(idx_ref, modes_ref, w_ref, pin_ref, c_ref, own_ref, s0_ref, s1_ref, line_ref, m_ref):
    w = w_ref[...]
    m = 1.0 - pin_ref[...].astype(F32)
    m_ref[...] = m
    pick = c_ref[0:64, 0 : NX * NY]
    own = rsel3(sel3(pick, w), c_ref[64:192, 0:128]) + rsel(sel(pick, m), c_ref[64:192, 128:256])
    own_ref[...] = own
    faces = sel3(c_ref[192 : 192 + 2 * NX2, 0:64], own)
    a, b = for_pairs(idx_ref, 0, faces[:NX2], faces[NX2:])
    for ref, face in ((s0_ref, a), (s1_ref, b)):
        for v in range(2):
            for c in range(3):
                ref[16 * (3 * v + c) : 16 * (3 * v + c) + 16, :] = modes_ref[v, c, 0:16, :]
        ref[96:112, :] = w[0:16]
        ref[112:128, :] = m[0:16]
        ref[128 : 128 + NX2, :] = face
    line_ref[...] = jnp.zeros((128, 128), F32)
    for k in range(8):
        if k < 6:
            line = modes_ref[k // 3, k % 3, pl.ds(0, NX, stride=NY), :]
        else:
            line = (w_ref if k == 6 else m_ref)[pl.ds(0, NX, stride=NY), :]
        line_ref[16 * k : 16 * k + NX, :] = line


def pack_y_body(idx_ref, line_ref, own_ref, r0_ref, r1_ref, ys_ref, s0_ref, s1_ref):
    lo, hi = from_pairs(idx_ref, 0, r0_ref[...], r1_ref[...])
    stack = jnp.concatenate([own_ref[...], lo[128:], hi[128:]], 0)
    faces = sel3(ys_ref[...], stack)
    a, b = for_pairs(idx_ref, 1, faces[:NY2], faces[NY2:])
    for ref, face in ((s0_ref, a), (s1_ref, b)):
        ref[0:128, :] = line_ref[...]
        for k in range(8):
            ref[16 * k + NX : 16 * k + NX + 1, :] = hi[16 * k : 16 * k + 1]
        ref[128 : 128 + NY2, :] = face


def static_of(w, m, kd, lanes):
    s = w * m
    f = 1.0 - m
    s2 = s * s
    inv = [1.0 / (s2 * (kd[:, c : c + 1] * lanes[0:1] + kd[:, 3 + c : 4 + c] * lanes[1:2]) + f) for c in range(3)]
    return s, f, inv


def statics_body(
    idx_ref, own_ref, rx0_ref, rx1_ref, ry0_ref, ry1_ref, sum_ref, d_ref, pick1_ref, kd2_ref, l2_ref, kd1_ref, l1_ref,
    e2_ref, e1_ref,
):
    xlo, xhi = from_pairs(idx_ref, 0, rx0_ref[128:, :], rx1_ref[128:, :])
    ylo, yhi = from_pairs(idx_ref, 1, ry0_ref[128:, :], ry1_ref[128:, :])
    ext = sel3(sum_ref[...], jnp.concatenate([own_ref[...], xlo, xhi, ylo, yhi], 0))

    def put(ref, w, m, kd, lanes):
        s, f, inv = static_of(w, m, kd, lanes)
        ref[0], ref[1] = s, f
        for c in range(3):
            ref[2 + c] = inv[c]

    put(e2_ref, rsel3(ext, d_ref[0]), rsel(ext, d_ref[1]), kd2_ref[...], l2_ref[...])
    coarse = sel3(pick1_ref[...], ext)
    put(e1_ref, rsel3(coarse, d_ref[2]), rsel(coarse, d_ref[3]), kd1_ref[...], l1_ref[...])


X4, Y4 = 24, 16


FACES4 = ((0, 16), (192, 224))


def faces_x4(idx_ref, fields, mats, y_ref, u_ref, s0_ref, s1_ref):
    even, _, _ = place(idx_ref, 0)
    outs = stiffness(fields, *mats, y_ref, 48, FACES4)
    for c in range(3):
        u_ref[c] = fields[c]
        w = outs[c]
        lo = jnp.concatenate([w[0:16], w[32:40]], 0)
        hi = jnp.concatenate([w[16:32], w[40:48]], 0)
        s0_ref[c] = jnp.where(even, hi, lo)
        s1_ref[c] = jnp.where(even, lo, hi)


def block4_body(u_ref, ahi, alo, bhi, blo, out_ref, y_ref):
    put4(out_ref, stiffness([u_ref[c] for c in range(3)], ahi, alo, bhi, blo, y_ref, 224))


LO16, HI16 = 16, 20


def faces_y4_body(idx_ref, w_ref, r0_ref, r1_ref, s0_ref, s1_ref):
    even, _, _ = place(idx_ref, 1)
    for c in range(3):
        xlo, xhi = from_pairs(idx_ref, 0, r0_ref[c], r1_ref[c])
        row = lax.broadcasted_iota(jnp.int32, (Y4, 256), 0)
        lo = jnp.concatenate([w_ref[2 * c + v, pl.ds(0, NX, stride=NY), :] for v in range(2)], 1)
        lo = jnp.concatenate([lo, jnp.concatenate([w_ref[2 * c + v, 192:196, :] for v in range(2)], 1)], 0)
        hi = jnp.concatenate([w_ref[2 * c + v, 208:224, :] for v in range(2)], 1)
        lo = lo + jnp.where(row == 0, xlo[0:1], 0.0) + jnp.where(row == NX, xhi[0:1], 0.0)
        hi = hi + jnp.where(row == 0, xlo[HI16 : HI16 + 1], 0.0) + jnp.where(row == NX, xhi[LO16 : LO16 + 1], 0.0)
        s0_ref[c] = jnp.where(even, hi, lo)
        s1_ref[c] = jnp.where(even, lo, hi)


def summed4(idx_ref, w_ref, rx0, rx1, ry0, ry1, full_ref):
    row = lax.broadcasted_iota(jnp.int32, (Y4, 256), 0)
    for c in range(3):
        xlo, xhi = from_pairs(idx_ref, 0, rx0[c], rx1[c])
        ylo, yhi = from_pairs(idx_ref, 1, ry0[c], ry1[c])
        yhi = jnp.where(row <= NX, yhi, 0.0)
        yhi = yhi + jnp.where(row == 0, xlo[HI16 : HI16 + 1], 0.0) + jnp.where(row == NX, xhi[LO16 : LO16 + 1], 0.0)
        end = xhi[0:16] + jnp.where(row == 0, ylo[NX : NX + 1], 0.0)
        for v in range(2):
            k, cut = 2 * c + v, slice(128 * v, 128 * v + 128)
            full_ref[k] = w_ref[k]
            full_ref[k, 0:16, :] += xlo[0:16, cut]
            full_ref[k, 192:208, :] += end[:, cut]
            full_ref[k, 208:224, :] += yhi[:, cut]
            full_ref[k, pl.ds(0, NX, stride=NY), :] += ylo[:NX, cut]


def put4(ref, outs):
    for c in range(3):
        for v in range(2):
            ref[2 * c + v] = outs[c][:, 128 * v : 128 * v + 128]


def first4_body(
    idx_ref, coef_ref, modes_ref, w_ref, pin_ref, rx0_ref, rx1_ref, ry0_ref, ry1_ref, kd_ref, lanes_ref, ahi, alo, bhi, blo,
    b_ref, st_ref, d_ref, u_ref, s0_ref, s1_ref, y_ref,
):
    _, xhi = from_pairs(idx_ref, 0, rx0_ref[0:128, :], rx1_ref[0:128, :])
    _, yhi = from_pairs(idx_ref, 1, ry0_ref[0:128, :], ry1_ref[0:128, :])

    def gathered(own, k):
        return jnp.concatenate([own, xhi[16 * k : 16 * k + 16], yhi[16 * k : 16 * k + 16]], 0)

    w = gathered(w_ref[...], 6)
    m = gathered(1.0 - pin_ref[...].astype(F32), 7)
    s, f, inv = static_of(w, m, kd_ref[...], lanes_ref[...])
    st_ref[0], st_ref[1] = s, f
    for c in range(3):
        st_ref[2 + c] = inv[c]
    fields = []
    for c in range(3):
        b = jnp.concatenate([gathered(modes_ref[v, c], 3 * v + c) for v in range(2)], 1)
        b_ref[c] = b
        d = wide(inv[c]) * b * coef_ref[0, 0]
        d_ref[c] = d
        fields.append(wide(s) * d)
    faces_x4(idx_ref, fields, (ahi, alo, bhi, blo), y_ref, u_ref, s0_ref, s1_ref)


def both4(ref, c):
    return jnp.concatenate([ref[2 * c], ref[2 * c + 1]], 1)


def update4(idx_ref, coef_ref, step, w_ref, recv, st_ref, r_ref, d_ref, full_ref, c):
    s, f, inv = wide(st_ref[0]), wide(st_ref[1]), wide(st_ref[2 + c])
    r = r_ref[c] - (s * both4(full_ref, c) + f * d_ref[c])
    if step == 0:
        d = coef_ref[0, 0] * inv * r
    else:
        d = coef_ref[0, 2 * step - 1] * d_ref[c] + coef_ref[0, 2 * step] * inv * r
    return s, f, r, d


def mid4_body(
    step, idx_ref, coef_ref, w_ref, rx0, rx1, ry0, ry1, st_ref, r_ref, d_ref, x_ref, ahi, alo, bhi, blo,
    r_out, d_out, x_out, u_ref, s0_ref, s1_ref, y_ref, full_ref,
):
    summed4(idx_ref, w_ref, rx0, rx1, ry0, ry1, full_ref)
    fields = []
    for c in range(3):
        s, f, r, d = update4(idx_ref, coef_ref, step, w_ref, None, st_ref, r_ref, d_ref, full_ref, c)
        r_out[c], d_out[c] = r, d
        x_out[c] = x_ref[c] + d
        fields.append(s * d)
    faces_x4(idx_ref, fields, (ahi, alo, bhi, blo), y_ref, u_ref, s0_ref, s1_ref)


def resid4_body(
    idx_ref, coef_ref, w_ref, rx0, rx1, ry0, ry1, st_ref, r_ref, d_ref, x_ref, ahi, alo, bhi, blo, rxy_ref, rz_ref, xs_ref,
    x_out, p_ref, s0_ref, s1_ref, y_ref, full_ref, keep_ref,
):
    summed4(idx_ref, w_ref, rx0, rx1, ry0, ry1, full_ref)
    fields = []
    owned = lax.broadcasted_iota(jnp.int32, (224, 256), 0) < NX * NY
    for c in range(3):
        s, f, r, d = update4(idx_ref, coef_ref, 2, w_ref, None, st_ref, r_ref, d_ref, full_ref, c)
        x_out[c] = x_ref[c] + d
        keep_ref[c] = jnp.where(owned, (1.0 - f) * r, 0.0)
        fields.append(s * d)
    outs = stiffness(fields, ahi, alo, bhi, blo, y_ref, 224)
    nx = xs_ref.shape[0] // 2
    for c in range(3):
        left = sel(rxy_ref[...], keep_ref[c] - wide(st_ref[0]) * outs[c])
        part = rsel(left[:, :128], rz_ref[0]) + rsel(left[:, 128:], rz_ref[1])
        p_ref[c] = part
        faces = sel(xs_ref[...], part)
        s0_ref[c], s1_ref[c] = for_pairs(idx_ref, 0, faces[:nx], faces[nx:])


def rise4_body(
    idx_ref, p_ref, rx0, rx1, ry0, ry1, sum_ref, pxy_ref, pz_ref, st_ref, x_ref, ahi, alo, bhi, blo,
    x_out, u_ref, s0_ref, s1_ref, y_ref,
):
    fields = []
    s, m = wide(st_ref[0]), 1.0 - wide(st_ref[1])
    for c in range(3):
        e = gather_sum(idx_ref, sum_ref, p_ref[c], rx0[c], rx1[c], ry0[c], ry1[c])
        e = sel(pxy_ref[...], e)
        x = x_ref[c] + m * jnp.concatenate([rsel(e, pz_ref[0]), rsel(e, pz_ref[1])], 1)
        x_out[c] = x
        fields.append(s * x)
    faces_x4(idx_ref, fields, (ahi, alo, bhi, blo), y_ref, u_ref, s0_ref, s1_ref)


def last4_body(idx_ref, coef_ref, w_ref, rx0, rx1, ry0, ry1, st_ref, r_ref, d_ref, x_ref, out_ref, full_ref):
    summed4(idx_ref, w_ref, rx0, rx1, ry0, ry1, full_ref)
    for c in range(3):
        _, _, _, d = update4(idx_ref, coef_ref, 2, w_ref, None, st_ref, r_ref, d_ref, full_ref, c)
        x = x_ref[c] + d
        for v in range(2):
            out_ref[v, c] = x[: NX * NY, 128 * v : 128 * v + 128]


def gather_sum(idx_ref, sum_ref, own, rx0, rx1, ry0, ry1):
    xlo, xhi = from_pairs(idx_ref, 0, rx0, rx1)
    ylo, yhi = from_pairs(idx_ref, 1, ry0, ry1)
    return sel(sum_ref[...], jnp.concatenate([own, xlo, xhi, ylo, yhi], 0))


def faces_y_body(idx_ref, p_ref, r0_ref, r1_ref, ys_ref, s0_ref, s1_ref):
    ny = ys_ref.shape[0] // 2
    for c in range(3):
        lo, hi = from_pairs(idx_ref, 0, r0_ref[c], r1_ref[c])
        faces = sel(ys_ref[...], jnp.concatenate([p_ref[c], lo, hi], 0))
        s0_ref[c], s1_ref[c] = for_pairs(idx_ref, 1, faces[:ny], faces[ny:])


def smooth(level, degree, coef_ref, st_ref, b, x, steps, mats, y_ref):
    sizes = list(np.cumsum(RINGS[degree])[::-1])
    n = int(sizes.pop(0))

    def residual(r, v):
        nonlocal n
        u = [st_ref[0, :n] * t for t in v]
        n = int(sizes.pop(0))
        outs = stiffness(u, *mats, y_ref, n)
        s, f = st_ref[0, :n], st_ref[1, :n]
        return [a[:n] - (s * w + f * t[:n]) for a, w, t in zip(r, outs, v)]

    r = b if x is None else residual(b, x)
    d = [st_ref[2 + c, :n] * r[c] * coef_ref[level, 0] for c in range(3)]
    x = d if x is None else [a[:n] + t for a, t in zip(x, d)]
    for step in range(1, steps):
        r = residual(r, d)
        d = [coef_ref[level, 2 * step - 1] * d[c][:n] + coef_ref[level, 2 * step] * st_ref[2 + c, :n] * r[c] for c in range(3)]
        x = [a[:n] + t for a, t in zip(x, d)]
    return r, d, x


def down2_body(
    idx_ref, coef_ref, p_ref, rx0, rx1, ry0, ry1, sum_ref, st_ref, rxy_ref, rz_ref, xs_ref,
    ahi, alo, ohi, olo, bhi, blo, owner_ref,
    b_out, x_out, p_out, s0_ref, s1_ref, y_ref,
):
    m = 1.0 - st_ref[1]
    b = []
    for c in range(3):
        b.append(m * gather_sum(idx_ref, sum_ref, p_ref[c], rx0[c], rx1[c], ry0[c], ry1[c]))
        b_out[c] = b[c]
    r, d, x = smooth(1, 2, coef_ref, st_ref, b, None, 3, (ahi, alo, bhi, blo), y_ref)
    s = st_ref[0, :64]
    outs = stiffness([s * t for t in d], ohi, olo, bhi, blo, y_ref, 64)
    nx = xs_ref.shape[0] // 2
    for c in range(3):
        x_out[c] = x[c]
        left = owner_ref[...] * m[:64] * r[c] - s * outs[c]
        part = rsel(sel(rxy_ref[...], left), rz_ref[...])
        p_out[c] = part
        faces = sel(xs_ref[...], part)
        s0_ref[c], s1_ref[c] = for_pairs(idx_ref, 0, faces[:nx], faces[nx:])


def tail(level, last, coef_ref, owner_ref, st_ref, r, d, x, outs, c):
    n = x[c].shape[0]
    c1, c2 = coef_ref[level, 2 * last - 1], coef_ref[level, 2 * last]
    s, f, inv = st_ref[0, :n], st_ref[1, :n], st_ref[2 + c, :n]
    return owner_ref[...] * (x[c] + c1 * d[c] + c2 * inv * (r[c] - f * d[c])) - c2 * inv * s * outs[c]


def bottom_body(
    idx_ref, coef_ref, p_ref, rx0, rx1, ry0, ry1, sum_ref, st_ref, owner_ref, ahi, alo, ohi, olo, bhi, blo,
    x2_ref, owner2_ref, xs_ref,
    p_out, s0_ref, s1_ref, y_ref,
):
    m = 1.0 - st_ref[1]
    b = [m * gather_sum(idx_ref, sum_ref, p_ref[c], rx0[c], rx1[c], ry0[c], ry1[c]) for c in range(3)]
    r, d, x = smooth(2, 1, coef_ref, st_ref, b, None, 3, (ahi, alo, bhi, blo), y_ref)
    outs = stiffness([st_ref[0, :32] * t for t in d], ohi, olo, bhi, blo, y_ref, 32)
    nx = xs_ref.shape[0] // 2
    for c in range(3):
        e = tail(2, 3, coef_ref, owner_ref, st_ref, r, d, x, outs, c)
        part = jnp.concatenate([owner2_ref[...] * x2_ref[c], e], 0)
        p_out[c] = part
        faces = sel(xs_ref[...], part)
        s0_ref[c], s1_ref[c] = for_pairs(idx_ref, 0, faces[:nx], faces[nx:])


def up2_body(
    idx_ref, coef_ref, p_ref, rx0, rx1, ry0, ry1, sum_ref, sum1_ref, b_ref, st_ref, owner_ref, ahi, alo, ohi, olo, bhi, blo, xs_ref,
    pxy_ref, pz_ref, p_out, s0_ref, s1_ref, y_ref,
):
    x = []
    for c in range(3):
        fine = gather_sum(idx_ref, sum_ref, p_ref[c, :64], rx0[c, :NX2], rx1[c, :NX2], ry0[c, :NY2], ry1[c, :NY2])
        e = gather_sum(idx_ref, sum1_ref, p_ref[c, 64:], rx0[c, NX2:], rx1[c, NX2:], ry0[c, NY2:], ry1[c, NY2:])
        x.append(fine + (1.0 - st_ref[1]) * rsel(sel(pxy_ref[...], e), pz_ref[...]))
    b = [b_ref[c] for c in range(3)]
    r, d, x = smooth(1, 2, coef_ref, st_ref, b, x, 2, (ahi, alo, bhi, blo), y_ref)
    outs = stiffness([st_ref[0, :64] * t for t in d], ohi, olo, bhi, blo, y_ref, 64)
    nx = xs_ref.shape[0] // 2
    for c in range(3):
        part = tail(1, 2, coef_ref, owner_ref, st_ref, r, d, x, outs, c)
        p_out[c] = part
        faces = sel(xs_ref[...], part)
        s0_ref[c], s1_ref[c] = for_pairs(idx_ref, 0, faces[:nx], faces[nx:])


def swap(axis, s0, s1):
    n = GX if axis == "gx" else GY
    even = [(i, i ^ 1) for i in range(n)]
    odd = [(i, (((i - 1) ^ 1) + 1) % n) for i in range(n)]
    return lax.ppermute(s0, axis, even), lax.ppermute(s1, axis, odd)


def chebyshev_table(spectrum):
    low, top = spectrum[:, 0], spectrum[:, 1]
    center, radius = 0.5 * (top + low), 0.5 * (top - low)
    ratio = center / radius
    rho = 1.0 / ratio
    columns = [1.0 / center]
    for _ in range(3):
        after = 1.0 / (2.0 * ratio - rho)
        columns += [after * rho, 2.0 * after / radius]
        rho = after
    return jnp.stack(columns, 1)


def interp_tables():
    plane = {}
    for key, degree, halo, fine, rows, coarse, rows_c in (
        (4, 4, 0, NODES["4"], 224, NODES["2o"], 64),
        (2, 2, 0, NODES["2o"], 64, NODES["1o"], 32),
        ("2e", 2, 2, NODES["2e"], 256, NODES["1e"], 96),
    ):
        px, py = prolong_line(degree, EX + 2 * halo), prolong_line(degree, EY + 2 * halo)
        f0, c0 = degree * halo, degree * halo // 2
        full = np.zeros((rows, rows_c))
        for r, q in ((r, q) for r in range(len(fine)) for q in range(len(coarse))):
            if fine[r] is not None and coarse[q] is not None:
                (i, j), (a, b) = fine[r], coarse[q]
                full[r, q] = px[i + f0, a + c0] * py[j + f0, b + c0]
        plane[key] = full.astype(ml_dtypes.bfloat16)
    z4 = prolong_line(4, 32)[:128, :64]
    z2 = prolong_line(2, 32)[:64, :32]
    pz4 = np.zeros((2, 128, 128))
    for v in range(2):
        pz4[v, 64 * v : 64 * v + 64, :] = z4.T
    pz2 = np.zeros((128, 128))
    for v in range(2):
        pz2[32 * v : 32 * v + 32, 64 * v : 64 * v + 64] = z2.T
    cast = lambda t: np.ascontiguousarray(t).astype(ml_dtypes.bfloat16)
    return plane, cast(pz4), cast(pz4.transpose(0, 2, 1)), cast(pz2), cast(pz2.T)


def local(modes, moduli, pinned, spectrum):
    idx = (lax.axis_index("gx") * 16 + lax.axis_index("gy")).astype(jnp.int32).reshape(1)
    coef = chebyshev_table(spectrum)
    modes = modes.reshape(2, 3, NX * NY, NZ)
    moduli = moduli.reshape(NX * NY, NZ)
    pinned = pinned.reshape(NX * NY, NZ)

    zmats = {p: hi_lo(z_matrices(p, 1 if p == 4 else 2)) for p in (4, 2, 1)}
    plane, pz4, rz4, pz2, rz2 = interp_tables()
    bf = lambda t: np.ascontiguousarray(t).astype(ml_dtypes.bfloat16)
    x2, x20, x1, x21 = EXCH["2"], EXCH["20"], EXCH["1"], EXCH["21"]

    at4 = {n: r for r, n in enumerate(NODES["4"])}
    at2e = {n: r for r, n in enumerate(NODES["2e"]) if n is not None}
    pick2 = one_hot(64, NX * NY, [(r, at4[(2 * i, 2 * j)]) for r, (i, j) in enumerate(NODES["2o"]) if i < 6 and j < 8])
    zw, zm = np.zeros((128, 128)), np.zeros((128, 128))
    dw, dm, d1w, d1m = (np.zeros((128, 128)) for _ in range(4))
    for k in range(64):
        zw[2 * k, k] = zm[2 * k, 64 + k] = 1.0
        for v in range(2):
            dw[k, 64 * v + k] = dm[64 + k, 64 * v + k] = 1.0
            if k % 2 == 0:
                d1w[k, 32 * v + k // 2] = d1m[64 + k, 32 * v + k // 2] = 1.0
    pick1 = one_hot(96, 256, [(r, at2e[(2 * n[0], 2 * n[1])]) for r, n in enumerate(NODES["1e"]) if n is not None])
    owner2, owner1 = np.zeros((64, 128), np.float32), np.zeros((32, 128), np.float32)
    for r, (i, j) in enumerate(NODES["2o"]):
        owner2[r] = float(i < 6 and j < 8)
    for r, (i, j) in enumerate(NODES["1o"]):
        owner1[r] = float(i < 3 and j < 4)
    kd4, l4 = kd_tables(NODES["4"], 224, 4)
    kd2, l2 = kd_tables(NODES["2e"], 256, 2)
    kd1, l1 = kd_tables(NODES["1e"], 96, 1)
    table4 = setup_table(4, NODES["4"], 256, 0)
    table2 = setup_table(2, NODES["2e"], 256, 2)
    table1 = setup_table(1, NODES["1e"], 96, 2)
    first = np.zeros((192 + 2 * NX2, 256))
    first[0:64, 0 : NX * NY] = pick2
    first[64:192, 0:128], first[64:192, 128:256] = zw, zm
    first[192:, 0:64] = x2["xs"]

    mx = 128 + x2["nx"]
    my = 128 + x2["ny"]
    q2own, sx0, sx1, line = call(
        pack_x_body, "pack_x", [idx], [modes, moduli, pinned, bf(first)],
        [((64, 128), F32), ((mx, 128), F32), ((mx, 128), F32), ((128, 128), F32)], [pltpu.VMEM((NX * NY, NZ), F32)],
    )
    rx0, rx1 = swap("gx", sx0, sx1)
    a4 = plane_matrices(idx, 4, table4, 256, 0, [(224, 256)])
    sy0, sy1 = call(
        pack_y_body, "pack_y", [idx], [line, q2own, rx0, rx1, x2["ys"]], [((my, 128), F32), ((my, 128), F32)],
    )
    ry0, ry1 = swap("gy", sy0, sy1)
    mats2 = plane_matrices(idx, 2, table2, 256, 2, [(144, 256), (64, 64)])
    mats1 = plane_matrices(idx, 1, table1, 96, 2, [(64, 96), (32, 32)])

    big = ((3, 224, 256), F32)
    msgx, msgy = ((3, X4, 256), F32), ((3, Y4, 256), F32)
    y4 = pltpu.VMEM((3, 4 * 224, 256), F32)
    y4f = pltpu.VMEM((3, 4 * 48, 256), F32)
    full = pltpu.VMEM((6, 224, 128), F32)
    keep = pltpu.VMEM((3, 224, 256), F32)
    halves = ((6, 224, 128), F32)
    mats4 = [*a4, *zmats[4]]

    b, st4, d, w, s0, s1 = call(
        first4_body, "first4", [idx, coef], [modes, moduli, pinned, rx0, rx1, ry0, ry1, kd4, l4, *mats4],
        [big, ((5, 224, 128), F32), big, big, msgx, msgx], [y4f],
    )
    st2, st1 = call(
        statics_body, "statics", [idx],
        [q2own, rx0, rx1, ry0, ry1, x2["sum"], bf(np.stack([dw, dm, d1w, d1m])), pick1, kd2, l2, kd1, l1],
        [((5, 256, 128), F32), ((5, 96, 128), F32)],
    )

    def trade4(u, s0, s1):
        r0, r1 = swap("gx", s0, s1)
        (w,) = call(block4_body, "block4", [], [u, *mats4], [halves], [y4], flops=10**10)
        t0, t1 = call(faces_y4_body, "faces_y4", [idx], [w, r0, r1], [msgy, msgy])
        return [w, r0, r1, *swap("gy", t0, t1)]

    def trade(table, p, s0, s1, sums=None):
        r0, r1 = swap("gx", s0, s1)
        t0, t1 = call(faces_y_body, "faces_y", [idx], [p, r0, r1, table["ys"]], [((3, table["ny"], 128), F32)] * 2)
        return [p, r0, r1, *swap("gy", t0, t1), *([table["sum"]] if sums is None else sums)]

    got = trade4(w, s0, s1)
    r, d, x, w, s0, s1 = call(
        functools.partial(mid4_body, 1), "mid4", [idx, coef], [*got, st4, b, d, d, *mats4], [big, big, big, big, msgx, msgx], [y4f, full],
    )
    got = trade4(w, s0, s1)
    face2, face20, face1, face21 = (((3, t["nx"], 128), F32) for t in (x2, x20, x1, x21))
    own2f, own1f = ((3, 64, 128), F32), ((3, 32, 128), F32)
    x4, p2, s0, s1 = call(
        resid4_body, "resid4", [idx, coef], [*got, st4, r, d, x, *mats4, bf(plane[4].T), rz4, x2["xs"]],
        [big, own2f, face2, face2], [y4, full, keep],
    )
    y2, y1 = pltpu.VMEM((3, 4 * 144, 128), F32), pltpu.VMEM((3, 4 * 64, 128), F32)
    b2, xo2, p1, s0, s1 = call(
        down2_body, "down2", [idx, coef],
        [*trade(x2, p2, s0, s1), st2, bf(plane[2].T), rz2, x1["xs"], *mats2, *zmats[2], owner2],
        [((3, 256, 128), F32), own2f, own1f, face1, face1], [y2],
    )
    p2, s0, s1 = call(
        bottom_body, "bottom", [idx, coef],
        [*trade(x1, p1, s0, s1), st1, owner1, *mats1, *zmats[1], xo2, owner2, x21["xs"]],
        [((3, 96, 128), F32), face21, face21], [y1],
    )
    p2, s0, s1 = call(
        up2_body, "up2", [idx, coef],
        [*trade(x21, p2, s0, s1, (x2["sum"], x1["sum"])), b2, st2, owner2, *mats2, *zmats[2], x20["xs"], plane["2e"], pz2],
        [own2f, face20, face20], [y2],
    )
    x, w, s0, s1 = call(
        rise4_body, "rise4", [idx], [*trade(x20, p2, s0, s1), plane[4], pz4, st4, x4, *mats4], [big, big, msgx, msgx], [y4f],
    )
    r, d, x, w, s0, s1 = call(
        functools.partial(mid4_body, 0), "mid4_0", [idx, coef], [*trade4(w, s0, s1), st4, b, x, x, *mats4],
        [big, big, big, big, msgx, msgx], [y4f, full],
    )
    r, d, x, w, s0, s1 = call(
        functools.partial(mid4_body, 1), "mid4", [idx, coef], [*trade4(w, s0, s1), st4, r, d, x, *mats4],
        [big, big, big, big, msgx, msgx], [y4f, full],
    )
    (out,) = call(
        last4_body, "last4", [idx, coef], [*trade4(w, s0, s1), st4, r, d, x], [((2, 3, NX * NY, NZ), F32)], [full],
    )
    return out.reshape(2, 3, NX, NY, NZ)


def solution(mesh):
    placed = (P(None, None, "gx", "gy", None), P("gx", "gy", None), P("gx", "gy", None), P())
    return jax.shard_map(
        local,
        mesh=mesh,
        in_specs=placed,
        out_specs=P(None, None, "gx", "gy", None),
        check_vma=False,
    )
```

```python
import functools

import jax
import jax.numpy as jnp
import ml_dtypes
import numpy as np
from jax import lax
from jax.experimental import pallas as pl
from jax.experimental.pallas import tpu as pltpu
from jax.sharding import PartitionSpec as P

F32 = jnp.float32
BF16 = jnp.bfloat16
COUPLE = 2.5
NX, NY, NZ = 12, 16, 128
EX, EY = 3, 4
GX, GY = 16, 16

PROLONG = {
    4: np.array([[1.0, 0.0, 0.0], [0.375, 0.75, -0.125], [0.0, 1.0, 0.0], [-0.125, 0.75, 0.375]]),
    2: np.array([[1.0, 0.0], [0.5, 0.5]]),
}


def element_matrices(degree):
    points, weights = np.polynomial.legendre.leggauss(8)
    points, weights = 0.5 * (points + 1.0), 0.5 * weights
    nodes = np.arange(degree + 1) / degree
    values = np.zeros((degree + 1, points.size))
    slopes = np.zeros((degree + 1, points.size))
    for i in range(degree + 1):
        others = [j for j in range(degree + 1) if j != i]
        values[i] = np.prod([(points - nodes[j]) / (nodes[i] - nodes[j]) for j in others], axis=0)
        for k in others:
            rest = [(points - nodes[j]) / (nodes[i] - nodes[j]) for j in others if j != k]
            slopes[i] += np.prod(rest, axis=0) / (nodes[i] - nodes[k]) if rest else 1.0 / (nodes[i] - nodes[k])
    mass = (values * weights) @ values.T
    stiff = (slopes * weights) @ slopes.T
    mixed = (slopes * weights) @ values.T
    return [mass, stiff, mixed, mixed.T]


ELEMENTS = {p: element_matrices(p) for p in (4, 2, 1)}


def line_matrix(element, count):
    degree = element.shape[0] - 1
    full = np.zeros((degree * count + 1, degree * count + 1))
    for e in range(count):
        full[degree * e : degree * e + degree + 1, degree * e : degree * e + degree + 1] += element
    return full


def z_matrices(degree, copies):
    count = NZ // 4
    length = count * degree
    out = np.zeros((4, 128, 128))
    for k, element in enumerate(ELEMENTS[degree]):
        full = line_matrix(element, count)[:length, :length].copy()
        full[0, 0] += element[degree, degree]
        for v in range(copies):
            out[k, v * length : (v + 1) * length, v * length : (v + 1) * length] = full.T
    return out


def hi_lo(array):
    array = array.astype(np.float32)
    hi = array.astype(ml_dtypes.bfloat16)
    lo = (array - hi.astype(np.float32)).astype(ml_dtypes.bfloat16)
    return hi, lo


def prolong_line(degree, count):
    table = PROLONG[degree]
    half = degree // 2
    full = np.zeros((degree * count + 1, half * count + 1))
    for e in range(count):
        for a in range(degree):
            for t in range(table.shape[1]):
                full[degree * e + a, half * e + t] += table[a, t]
    full[-1, -1] = 1.0
    return full


def natural(degree, halo):
    return [
        (i, j)
        for i in range(-degree * halo, degree * (EX + halo) + 1)
        for j in range(-degree * halo, degree * (EY + halo) + 1)
    ]


def pad_to(n, m):
    return -(-n // m) * m


NODES4 = (
    [(i, j) for i in range(NX) for j in range(NY)]
    + [(NX, j) for j in range(NY)]
    + [(i, NY) for i in range(NX)]
    + [(NX, NY)]
)


def in_rings(degree, parts):
    nodes, seen = [], set()
    for halo, rows in enumerate(parts):
        ring = [n for n in natural(degree, halo) if n not in seen]
        seen.update(ring)
        nodes += ring + [None] * (rows - len(ring))
    return nodes


RINGS = {2: (64, 80, 112), 1: (32, 32, 32)}
NODES = {
    "4": NODES4,
    "2o": natural(2, 0),
    "2e": in_rings(2, RINGS[2]),
    "1o": natural(1, 0),
    "1e": in_rings(1, RINGS[1]),
}


def one_hot(rows, cols, pairs):
    out = np.zeros((rows, cols), np.float32)
    for r, c in pairs:
        out[r, c] = 1.0
    return out.astype(ml_dtypes.bfloat16)


def exchange_tables(degree, halo, own, ext, rows_own, rows_ext):
    bx, by = degree * EX, degree * EY
    layers = degree * halo + 1
    own_at = {node: r for r, node in enumerate(own)}
    xlo = [(i, j) for i in range(layers) for j in range(by + 1)]
    xhi = [(bx - layers + 1 + i, j) for i in range(layers) for j in range(by + 1)]
    nx = pad_to(len(xlo), 16)
    sources = [(node, r) for node, r in own_at.items()]
    sources += [((i - bx, j), rows_own + r) for r, (i, j) in enumerate(xhi)]
    sources += [((i + bx, j), rows_own + nx + r) for r, (i, j) in enumerate(xlo)]
    span = range(-degree * halo, bx + degree * halo + 1)
    ylo = [(i, j) for i in span for j in range(layers)]
    yhi = [(i, by - layers + 1 + j) for i in span for j in range(layers)]
    ny = pad_to(len(ylo), 16)
    xs = [one_hot(nx, rows_own, [(r, own_at[n]) for r, n in enumerate(face)]) for face in (xlo, xhi)]
    width = rows_own + 2 * nx
    ys = [
        one_hot(ny, width, [(r, c) for r, n in enumerate(face) for node, c in sources if node == n])
        for face in (ylo, yhi)
    ]
    sources2 = list(sources)
    sources2 += [((i, j - by), width + r) for r, (i, j) in enumerate(yhi)]
    sources2 += [((i, j + by), width + ny + r) for r, (i, j) in enumerate(ylo)]
    ext_at = {node: r for r, node in enumerate(ext) if node is not None}
    total = one_hot(rows_ext, width + 2 * ny, [(ext_at[n], c) for n, c in sources2 if n in ext_at])
    return {
        "nx": nx,
        "ny": ny,
        "xs": np.concatenate(xs, 0),
        "ys": np.concatenate(ys, 0),
        "sum": total,
    }


EXCH = {
    "2": exchange_tables(2, 2, NODES["2o"], NODES["2e"], 64, 256),
    "20": exchange_tables(2, 0, NODES["2o"], NODES["2o"], 64, 64),
    "1": exchange_tables(1, 2, NODES["1o"], NODES["1e"], 32, 96),
}


def side_by_side(a, own_a, b, own_b):
    own, nx, ny = own_a + own_b, a["nx"] + b["nx"], a["ny"] + b["ny"]
    out = {"nx": nx, "ny": ny}
    spread = lambda t, o, first: np.concatenate(
        [
            np.arange(o) + (0 if first else own_a),
            *(own + k * nx + (0 if first else a["nx"]) + np.arange(t["nx"]) for k in range(2)),
            *(own + 2 * nx + k * ny + (0 if first else a["ny"]) + np.arange(t["ny"]) for k in range(2)),
        ]
    )
    for key, width, step in (("xs", own, "nx"), ("ys", own + 2 * nx, "ny")):
        blocks = []
        for k in range(2):
            for t, o, first in ((a, own_a, True), (b, own_b, False)):
                rows = t[key][k * t[step] : (k + 1) * t[step]]
                block = np.zeros((rows.shape[0], width), ml_dtypes.bfloat16)
                block[:, spread(t, o, first)[: rows.shape[1]]] = rows
                blocks.append(block)
        out[key] = np.concatenate(blocks, 0)
    return out


EXCH["21"] = side_by_side(EXCH["2"], 64, EXCH["1"], 32)


def setup_table(degree, nodes, rows, halo):
    out = np.zeros((rows, 128), np.float32)
    for r, node in enumerate(nodes):
        if node is not None:
            out[r, node[0] + degree * halo] = out[r, 32 + node[1] + degree * halo] = 1.0
    parts = [out]
    for wide in (True, False) if halo else (False,):
        grow, start = (halo, 0) if wide else (0, degree * halo)
        for element in ELEMENTS[degree]:
            table = np.zeros((32, 128), np.float32)
            for at, count in ((0, EX + 2 * grow), (32, EY + 2 * grow)):
                n = degree * count + 1
                table[start : start + n, at + start : at + start + n] = line_matrix(element, count)
            parts.append(table)
    return np.concatenate(parts, 0)


def kd_tables(nodes, rows, degree):
    m = lambda a: ELEMENTS[degree][0][a % degree, a % degree] + (ELEMENTS[degree][0][degree, degree] if a % degree == 0 else 0.0)
    k = lambda a: ELEMENTS[degree][1][a % degree, a % degree] + (ELEMENTS[degree][1][degree, degree] if a % degree == 0 else 0.0)
    out = np.zeros((rows, 8), np.float32)
    for r, node in enumerate(nodes):
        if node is None:
            continue
        i, j = node
        for c in range(3):
            co = [1.0 + COUPLE * (c == e) for e in range(3)]
            out[r, c] = co[0] * k(i) * m(j) + co[1] * m(i) * k(j)
            out[r, 3 + c] = co[2] * m(i) * m(j)
    copies = {4: 1, 2: 2, 1: 2}[degree]
    length = NZ // 4 * degree
    lanes = np.zeros((8, 128), np.float32)
    for z in range(length):
        for v in range(copies):
            lanes[0, v * length + z] = m(z)
            lanes[1, v * length + z] = k(z)
    return out, lanes


def dot(a, b):
    return jnp.dot(a, b, preferred_element_type=F32)


def split(v):
    hi = v.astype(BF16)
    return hi, (v - hi.astype(F32)).astype(BF16)


def sel(exact, v):
    hi, lo = split(v)
    return dot(exact, hi) + dot(exact, lo)


def sel3(exact, v):
    hi = v.astype(BF16)
    rest = v - hi.astype(F32)
    mid = rest.astype(BF16)
    lo = (rest - mid.astype(F32)).astype(BF16)
    return dot(exact, hi) + dot(exact, mid) + dot(exact, lo)


def rsel(v, exact):
    hi, lo = split(v)
    return dot(hi, exact) + dot(lo, exact)


def rsel3(v, exact):
    hi = v.astype(BF16)
    rest = v - hi.astype(F32)
    mid = rest.astype(BF16)
    lo = (rest - mid.astype(F32)).astype(BF16)
    return dot(hi, exact) + dot(mid, exact) + dot(lo, exact)


def place(idx_ref, axis):
    at = idx_ref[0]
    at = (at >> 4) if axis == 0 else (at & 15)
    even = (at & 1) == 0
    return even, (at > 0).astype(F32), (at < (GX, GY)[axis] - 1).astype(F32)


def for_pairs(idx_ref, axis, lo, hi):
    even, _, _ = place(idx_ref, axis)
    return jnp.where(even, hi, lo), jnp.where(even, lo, hi)


def from_pairs(idx_ref, axis, r0, r1):
    even, has_lo, has_hi = place(idx_ref, axis)
    return jnp.where(even, r1, r0) * has_lo, jnp.where(even, r0, r1) * has_hi


def stiffness(fields, ahi, alo, bhi, blo, y_ref, rows, picks=None):
    cols, block = ahi.shape[2], ahi.shape[1] // 4
    for s in range(3):
        u = fields[s]
        if cols != u.shape[0]:
            u = jnp.concatenate([u, jnp.zeros((cols - u.shape[0], u.shape[1]), F32)], 0)
        uh, ul = split(u)
        if rows == block:
            high, low = ahi[s], alo[s]
        else:
            spans = [(block * k + a, block * k + b) for k in range(4) for a, b in picks or ((0, rows),)]
            high, low = (jnp.concatenate([m[s, a:b, :] for a, b in spans], 0) for m in (ahi, alo))
        if u.shape[1] == 128:
            both = dot(high, jnp.concatenate([uh, ul], 1))
            y_ref[s, : 4 * rows] = both[:, :128] + both[:, 128:] + dot(low, uh)
        else:
            y_ref[s, : 4 * rows] = dot(high, uh) + dot(high, ul) + dot(low, uh)
    part = lambda s, k: y_ref[s, k * rows : (k + 1) * rows, :]
    plans = (
        (lambda: part(0, 0) + part(1, 2), lambda: part(0, 1), lambda: part(2, 2), 3),
        (lambda: part(1, 0) + part(0, 2), lambda: part(1, 1), lambda: part(2, 3), 3),
        (lambda: part(2, 0), lambda: part(2, 1), lambda: part(0, 3) + part(1, 3), 2),
    )
    outs = []
    for first, second, third, mixed in plans:
        mats_h = jnp.concatenate([bhi[0], bhi[1], bhi[mixed]], 0)
        mats_l = jnp.concatenate([blo[0], blo[1], blo[mixed]], 0)
        one, two, three = first(), second(), third()
        halves = []
        for v in range(one.shape[1] // 128):
            cut = lambda t: t[:, 128 * v : 128 * v + 128]
            h, l = split(jnp.concatenate([cut(one), cut(two), cut(three)], 1))
            halves.append(dot(h, mats_h) + dot(l, mats_h) + dot(h, mats_l))
        outs.append(halves[0] if len(halves) == 1 else jnp.concatenate(halves, 1))
    return outs


def wide(v):
    return jnp.concatenate([v, v], 1)


VMEM = pl.BlockSpec(memory_space=pltpu.VMEM)
SMEM = pl.BlockSpec(memory_space=pltpu.SMEM)


def call(body, name, smem, args, outs, scratch=(), flops=1000000, limit=40):
    return pl.pallas_call(
        body,
        name=name,
        out_shape=[jax.ShapeDtypeStruct(shape, dtype) for shape, dtype in outs],
        in_specs=[SMEM] * len(smem) + [VMEM] * len(args),
        out_specs=[VMEM] * len(outs),
        scratch_shapes=list(scratch),
        compiler_params=pltpu.CompilerParams(vmem_limit_bytes=limit * 2**20),
        cost_estimate=pl.CostEstimate(flops=flops, bytes_accessed=100000, transcendentals=0),
    )(*smem, *args)


def setup_body(rows_in, plans, idx_ref, c_ref, *refs):
    *outs, xe_ref, ye_ref = refs
    at = idx_ref[0]
    hdot = functools.partial(jnp.dot, preferred_element_type=F32, precision=lax.Precision.HIGHEST)
    tdot = lambda a, b: lax.dot_general(
        a, b, (((1,), (1,)), ((), ())), preferred_element_type=F32, precision=lax.Precision.HIGHEST
    )
    m, k, g, t = range(4)
    strong = 1.0 + COUPLE
    for p, (rows, cols, corner, corr) in enumerate(plans):
        for q in range(4):
            table = c_ref[rows_in + 128 * p + 32 * q : rows_in + 128 * p + 32 * q + 32, :]
            x1, y1 = table[:, 0:32], table[:, 32:64]
            if corner is not None:
                i, j = (lax.broadcasted_iota(jnp.int32, (32, 32), d) for d in (0, 1))
                spot = jnp.where((i == corner) & (j == corner), corr[q], 0.0)
                x1 = x1 + spot * ((at >> 4) == 0).astype(F32)
                y1 = y1 + spot * ((at & 15) == 0).astype(F32)
            ox, oy = c_ref[0:rows_in, 0:32], c_ref[0:rows_in, 32:64]
            xe_ref[q, :rows, :cols] = tdot(hdot(ox[:rows], x1), ox[:cols])
            ye_ref[q, :rows, :cols] = tdot(hdot(oy[:rows], y1), oy[:cols])
        xy = lambda a, b: xe_ref[a, :rows, :cols] * ye_ref[b, :rows, :cols]
        blocks = (
            (lambda: strong * xy(k, m) + xy(m, k), lambda: xy(m, m), lambda: COUPLE * xy(t, g), lambda: COUPLE * xy(t, m)),
            (lambda: xy(k, m) + strong * xy(m, k), lambda: xy(m, m), lambda: COUPLE * xy(g, t), lambda: COUPLE * xy(m, t)),
            (lambda: xy(k, m) + xy(m, k), lambda: strong * xy(m, m), lambda: COUPLE * xy(g, m), lambda: COUPLE * xy(m, g)),
        )
        for s in range(3):
            for b in range(4):
                hi, lo = split(blocks[s][b]())
                outs[2 * p][s, b * rows : (b + 1) * rows, :] = hi
                outs[2 * p + 1][s, b * rows : (b + 1) * rows, :] = lo
    if len(outs) > 2 * len(plans):
        outs[-1][...] = jnp.zeros((8, 128), F32)


def plane_matrices(idx, degree, table, rows_in, halo, sizes, token=False):
    corr = [float(np.float32(e[degree, degree])) for e in ELEMENTS[degree]]
    plans = [(*sizes[-1], degree * halo, corr)]
    if halo:
        plans = [(*sizes[0], None, None)] + plans
    outs = [((3, 4 * r, c), BF16) for r, c, *_ in plans for _ in range(2)]
    return call(
        functools.partial(setup_body, rows_in, plans),
        "setup_" + str(degree),
        [idx],
        [table],
        outs + ([((8, 128), F32)] if token else []),
        [pltpu.VMEM((4, rows_in, rows_in), F32), pltpu.VMEM((4, rows_in, rows_in), F32)],
    )


NX2, NY2 = EXCH["2"]["nx"], EXCH["2"]["ny"]


def pack_x_body(idx_ref, modes_ref, w_ref, pin_ref, c_ref, own_ref, s0_ref, s1_ref, line_ref, ys_ref, m_ref):
    ys_ref[...] = c_ref[192 + 2 * NX2 :, :]
    w = w_ref[...]
    m = 1.0 - pin_ref[...].astype(F32)
    m_ref[...] = m
    pick = c_ref[0:64, 0 : NX * NY]
    own = rsel3(sel3(pick, w), c_ref[64:192, 0:128]) + rsel(sel(pick, m), c_ref[64:192, 128:256])
    own_ref[...] = own
    faces = sel3(c_ref[192 : 192 + 2 * NX2, 0:64], own)
    a, b = for_pairs(idx_ref, 0, faces[:NX2], faces[NX2:])
    for ref, face in ((s0_ref, a), (s1_ref, b)):
        for v in range(2):
            for c in range(3):
                ref[16 * (3 * v + c) : 16 * (3 * v + c) + 16, :] = modes_ref[v, c, 0:16, :]
        ref[96:112, :] = w[0:16]
        ref[112:128, :] = m[0:16]
        ref[128 : 128 + NX2, :] = face
    line_ref[...] = jnp.zeros((128, 128), F32)
    for k in range(8):
        if k < 6:
            line = modes_ref[k // 3, k % 3, pl.ds(0, NX, stride=NY), :]
        else:
            line = (w_ref if k == 6 else m_ref)[pl.ds(0, NX, stride=NY), :]
        line_ref[16 * k : 16 * k + NX, :] = line


def pack_y_body(idx_ref, line_ref, own_ref, r0_ref, r1_ref, ys_ref, s0_ref, s1_ref):
    lo, hi = from_pairs(idx_ref, 0, r0_ref[...], r1_ref[...])
    stack = jnp.concatenate([own_ref[...], lo[128:], hi[128:]], 0)
    faces = sel3(ys_ref[:, 0 : 64 + 2 * NX2], stack)
    a, b = for_pairs(idx_ref, 1, faces[:NY2], faces[NY2:])
    for ref, face in ((s0_ref, a), (s1_ref, b)):
        ref[0:128, :] = line_ref[...]
        for k in range(8):
            ref[16 * k + NX : 16 * k + NX + 1, :] = hi[16 * k : 16 * k + 1]
        ref[128 : 128 + NY2, :] = face


def static_of(w, m, kd, lanes):
    s = w * m
    f = 1.0 - m
    s2 = s * s
    inv = [1.0 / (s2 * (kd[:, c : c + 1] * lanes[0:1] + kd[:, 3 + c : 4 + c] * lanes[1:2]) + f) for c in range(3)]
    return s, f, inv


def statics_body(
    idx_ref, own_ref, rx0_ref, rx1_ref, ry0_ref, ry1_ref, sum_ref, d_ref, pick1_ref, kd2_ref, l2_ref, kd1_ref, l1_ref,
    e2_ref, e1_ref,
):
    xlo, xhi = from_pairs(idx_ref, 0, rx0_ref[128:, :], rx1_ref[128:, :])
    ylo, yhi = from_pairs(idx_ref, 1, ry0_ref[128:, :], ry1_ref[128:, :])
    ext = sel3(sum_ref[...], jnp.concatenate([own_ref[...], xlo, xhi, ylo, yhi], 0))

    def put(ref, w, m, kd, lanes):
        s, f, inv = static_of(w, m, kd, lanes)
        ref[0], ref[1] = s, f
        for c in range(3):
            ref[2 + c] = inv[c]

    put(e2_ref, rsel3(ext, d_ref[0]), rsel(ext, d_ref[1]), kd2_ref[...], l2_ref[...])
    coarse = sel3(pick1_ref[...], ext)
    put(e1_ref, rsel3(coarse, d_ref[2]), rsel(coarse, d_ref[3]), kd1_ref[...], l1_ref[...])


X4, Y4 = 24, 16


FACES4 = ((0, 16), (192, 224))


def faces_x4(idx_ref, fields, mats, y_ref, u_ref, s0_ref, s1_ref):
    even, _, _ = place(idx_ref, 0)
    outs = stiffness(fields, *mats, y_ref, 48, FACES4)
    for c in range(3):
        u_ref[c] = fields[c]
        w = outs[c]
        lo = jnp.concatenate([w[0:16], w[32:40]], 0)
        hi = jnp.concatenate([w[16:32], w[40:48]], 0)
        s0_ref[c] = jnp.where(even, hi, lo)
        s1_ref[c] = jnp.where(even, lo, hi)


def block4_body(u_ref, ahi, alo, bhi, blo, out_ref, y_ref):
    put4(out_ref, stiffness([u_ref[c] for c in range(3)], ahi, alo, bhi, blo, y_ref, 224))


LO16, HI16 = 16, 20


def faces_y4_body(idx_ref, w_ref, r0_ref, r1_ref, s0_ref, s1_ref):
    even, _, _ = place(idx_ref, 1)
    for c in range(3):
        xlo, xhi = from_pairs(idx_ref, 0, r0_ref[c], r1_ref[c])
        row = lax.broadcasted_iota(jnp.int32, (Y4, 256), 0)
        lo = jnp.concatenate([w_ref[2 * c + v, pl.ds(0, NX, stride=NY), :] for v in range(2)], 1)
        lo = jnp.concatenate([lo, jnp.concatenate([w_ref[2 * c + v, 192:196, :] for v in range(2)], 1)], 0)
        hi = jnp.concatenate([w_ref[2 * c + v, 208:224, :] for v in range(2)], 1)
        lo = lo + jnp.where(row == 0, xlo[0:1], 0.0) + jnp.where(row == NX, xhi[0:1], 0.0)
        hi = hi + jnp.where(row == 0, xlo[HI16 : HI16 + 1], 0.0) + jnp.where(row == NX, xhi[LO16 : LO16 + 1], 0.0)
        s0_ref[c] = jnp.where(even, hi, lo)
        s1_ref[c] = jnp.where(even, lo, hi)


def summed4(idx_ref, w_ref, rx0, rx1, ry0, ry1, full_ref):
    row = lax.broadcasted_iota(jnp.int32, (Y4, 256), 0)
    for c in range(3):
        xlo, xhi = from_pairs(idx_ref, 0, rx0[c], rx1[c])
        ylo, yhi = from_pairs(idx_ref, 1, ry0[c], ry1[c])
        yhi = jnp.where(row <= NX, yhi, 0.0)
        yhi = yhi + jnp.where(row == 0, xlo[HI16 : HI16 + 1], 0.0) + jnp.where(row == NX, xhi[LO16 : LO16 + 1], 0.0)
        end = xhi[0:16] + jnp.where(row == 0, ylo[NX : NX + 1], 0.0)
        for v in range(2):
            k, cut = 2 * c + v, slice(128 * v, 128 * v + 128)
            full_ref[k] = w_ref[k]
            full_ref[k, 0:16, :] += xlo[0:16, cut]
            full_ref[k, 192:208, :] += end[:, cut]
            full_ref[k, 208:224, :] += yhi[:, cut]
            full_ref[k, pl.ds(0, NX, stride=NY), :] += ylo[:NX, cut]


def put4(ref, outs):
    for c in range(3):
        for v in range(2):
            ref[2 * c + v] = outs[c][:, 128 * v : 128 * v + 128]


def first4_body(
    idx_ref, coef_ref, modes_ref, w_ref, pin_ref, rx0_ref, rx1_ref, ry0_ref, ry1_ref, table_ref, ahi, alo, bhi, blo,
    b_ref, st_ref, d_ref, u_ref, s0_ref, s1_ref, y_ref,
):
    _, xhi = from_pairs(idx_ref, 0, rx0_ref[0:128, :], rx1_ref[0:128, :])
    _, yhi = from_pairs(idx_ref, 1, ry0_ref[0:128, :], ry1_ref[0:128, :])

    def gathered(own, k):
        return jnp.concatenate([own, xhi[16 * k : 16 * k + 16], yhi[16 * k : 16 * k + 16]], 0)

    w = gathered(w_ref[...], 6)
    m = gathered(1.0 - pin_ref[...].astype(F32), 7)
    s, f, inv = static_of(w, m, table_ref[0:224, 64:72], table_ref[384:392, :])
    st_ref[0], st_ref[1] = s, f
    for c in range(3):
        st_ref[2 + c] = inv[c]
    fields = []
    for c in range(3):
        b = jnp.concatenate([gathered(modes_ref[v, c], 3 * v + c) for v in range(2)], 1)
        b_ref[c] = b
        d = wide(inv[c]) * b * coef_ref[0, 0]
        d_ref[c] = d
        fields.append(wide(s) * d)
    faces_x4(idx_ref, fields, (ahi, alo, bhi, blo), y_ref, u_ref, s0_ref, s1_ref)


def both4(ref, c):
    return jnp.concatenate([ref[2 * c], ref[2 * c + 1]], 1)


def update4(idx_ref, coef_ref, step, w_ref, recv, st_ref, r_ref, d_ref, full_ref, c):
    s, f, inv = wide(st_ref[0]), wide(st_ref[1]), wide(st_ref[2 + c])
    r = r_ref[c] - (s * both4(full_ref, c) + f * d_ref[c])
    if step == 0:
        d = coef_ref[0, 0] * inv * r
    else:
        d = coef_ref[0, 2 * step - 1] * d_ref[c] + coef_ref[0, 2 * step] * inv * r
    return s, f, r, d


def mid4_body(
    step, idx_ref, coef_ref, w_ref, rx0, rx1, ry0, ry1, st_ref, r_ref, d_ref, x_ref, ahi, alo, bhi, blo,
    r_out, d_out, x_out, u_ref, s0_ref, s1_ref, y_ref, full_ref,
):
    summed4(idx_ref, w_ref, rx0, rx1, ry0, ry1, full_ref)
    fields = []
    for c in range(3):
        s, f, r, d = update4(idx_ref, coef_ref, step, w_ref, None, st_ref, r_ref, d_ref, full_ref, c)
        r_out[c], d_out[c] = r, d
        x_out[c] = x_ref[c] + d
        fields.append(s * d)
    faces_x4(idx_ref, fields, (ahi, alo, bhi, blo), y_ref, u_ref, s0_ref, s1_ref)


def resid4_body(
    idx_ref, coef_ref, w_ref, rx0, rx1, ry0, ry1, st_ref, r_ref, d_ref, x_ref, ahi, alo, bhi, blo, rxy_ref, rz_ref, xs_ref,
    x_out, p_ref, s0_ref, s1_ref, y_ref, full_ref, keep_ref,
):
    summed4(idx_ref, w_ref, rx0, rx1, ry0, ry1, full_ref)
    fields = []
    owned = lax.broadcasted_iota(jnp.int32, (224, 256), 0) < NX * NY
    for c in range(3):
        s, f, r, d = update4(idx_ref, coef_ref, 2, w_ref, None, st_ref, r_ref, d_ref, full_ref, c)
        x_out[c] = x_ref[c] + d
        keep_ref[c] = jnp.where(owned, (1.0 - f) * r, 0.0)
        fields.append(s * d)
    outs = stiffness(fields, ahi, alo, bhi, blo, y_ref, 224)
    nx = xs_ref.shape[0] // 2
    for c in range(3):
        left = sel(rxy_ref[...], keep_ref[c] - wide(st_ref[0]) * outs[c])
        part = rsel(left[:, :128], rz_ref[0]) + rsel(left[:, 128:], rz_ref[1])
        p_ref[c] = part
        faces = sel(xs_ref[...], part)
        s0_ref[c], s1_ref[c] = for_pairs(idx_ref, 0, faces[:nx], faces[nx:])


def rise4_body(
    idx_ref, p_ref, rx0, rx1, ry0, ry1, sum_ref, pxy_ref, pz_ref, st_ref, x_ref, ahi, alo, bhi, blo,
    x_out, u_ref, s0_ref, s1_ref, y_ref,
):
    fields = []
    s, m = wide(st_ref[0]), 1.0 - wide(st_ref[1])
    for c in range(3):
        e = gather_sum(idx_ref, sum_ref, p_ref[c], rx0[c], rx1[c], ry0[c], ry1[c])
        e = sel(pxy_ref[...], e)
        x = x_ref[c] + m * jnp.concatenate([rsel(e, pz_ref[0]), rsel(e, pz_ref[1])], 1)
        x_out[c] = x
        fields.append(s * x)
    faces_x4(idx_ref, fields, (ahi, alo, bhi, blo), y_ref, u_ref, s0_ref, s1_ref)


def last4_body(idx_ref, coef_ref, w_ref, rx0, rx1, ry0, ry1, st_ref, r_ref, d_ref, x_ref, out_ref, full_ref):
    summed4(idx_ref, w_ref, rx0, rx1, ry0, ry1, full_ref)
    for c in range(3):
        _, _, _, d = update4(idx_ref, coef_ref, 2, w_ref, None, st_ref, r_ref, d_ref, full_ref, c)
        x = x_ref[c] + d
        for v in range(2):
            out_ref[v, c] = x[: NX * NY, 128 * v : 128 * v + 128]


def gather_sum(idx_ref, sum_ref, own, rx0, rx1, ry0, ry1):
    xlo, xhi = from_pairs(idx_ref, 0, rx0, rx1)
    ylo, yhi = from_pairs(idx_ref, 1, ry0, ry1)
    return sel(sum_ref[...], jnp.concatenate([own, xlo, xhi, ylo, yhi], 0))


def faces_y_body(idx_ref, p_ref, r0_ref, r1_ref, ys_ref, s0_ref, s1_ref):
    ny = ys_ref.shape[0] // 2
    for c in range(3):
        lo, hi = from_pairs(idx_ref, 0, r0_ref[c], r1_ref[c])
        faces = sel(ys_ref[...], jnp.concatenate([p_ref[c], lo, hi], 0))
        s0_ref[c], s1_ref[c] = for_pairs(idx_ref, 1, faces[:ny], faces[ny:])


def smooth(level, degree, coef_ref, st_ref, b, x, steps, mats, y_ref):
    sizes = list(np.cumsum(RINGS[degree])[::-1])
    n = int(sizes.pop(0))

    def residual(r, v):
        nonlocal n
        u = [st_ref[0, :n] * t for t in v]
        n = int(sizes.pop(0))
        outs = stiffness(u, *mats, y_ref, n)
        s, f = st_ref[0, :n], st_ref[1, :n]
        return [a[:n] - (s * w + f * t[:n]) for a, w, t in zip(r, outs, v)]

    r = b if x is None else residual(b, x)
    d = [st_ref[2 + c, :n] * r[c] * coef_ref[level, 0] for c in range(3)]
    x = d if x is None else [a[:n] + t for a, t in zip(x, d)]
    for step in range(1, steps):
        r = residual(r, d)
        d = [coef_ref[level, 2 * step - 1] * d[c][:n] + coef_ref[level, 2 * step] * st_ref[2 + c, :n] * r[c] for c in range(3)]
        x = [a[:n] + t for a, t in zip(x, d)]
    return r, d, x


def down2_body(
    idx_ref, coef_ref, p_ref, rx0, rx1, ry0, ry1, sum_ref, st_ref, rxy_ref, rz_ref, xs_ref,
    ahi, alo, ohi, olo, bhi, blo, owner_ref,
    b_out, x_out, p_out, s0_ref, s1_ref, y_ref,
):
    m = 1.0 - st_ref[1]
    b = []
    for c in range(3):
        b.append(m * gather_sum(idx_ref, sum_ref, p_ref[c], rx0[c], rx1[c], ry0[c], ry1[c]))
        b_out[c] = b[c]
    r, d, x = smooth(1, 2, coef_ref, st_ref, b, None, 3, (ahi, alo, bhi, blo), y_ref)
    s = st_ref[0, :64]
    outs = stiffness([s * t for t in d], ohi, olo, bhi, blo, y_ref, 64)
    nx = xs_ref.shape[0] // 2
    for c in range(3):
        x_out[c] = x[c]
        left = owner_ref[...] * m[:64] * r[c] - s * outs[c]
        part = rsel(sel(rxy_ref[...], left), rz_ref[...])
        p_out[c] = part
        faces = sel(xs_ref[...], part)
        s0_ref[c], s1_ref[c] = for_pairs(idx_ref, 0, faces[:nx], faces[nx:])


def tail(level, last, coef_ref, owner_ref, st_ref, r, d, x, outs, c):
    n = x[c].shape[0]
    c1, c2 = coef_ref[level, 2 * last - 1], coef_ref[level, 2 * last]
    s, f, inv = st_ref[0, :n], st_ref[1, :n], st_ref[2 + c, :n]
    return owner_ref[...] * (x[c] + c1 * d[c] + c2 * inv * (r[c] - f * d[c])) - c2 * inv * s * outs[c]


def bottom_body(
    idx_ref, coef_ref, p_ref, rx0, rx1, ry0, ry1, sum_ref, st_ref, owner_ref, ahi, alo, ohi, olo, bhi, blo,
    x2_ref, owner2_ref, xs_ref,
    p_out, s0_ref, s1_ref, y_ref,
):
    m = 1.0 - st_ref[1]
    b = [m * gather_sum(idx_ref, sum_ref, p_ref[c], rx0[c], rx1[c], ry0[c], ry1[c]) for c in range(3)]
    r, d, x = smooth(2, 1, coef_ref, st_ref, b, None, 3, (ahi, alo, bhi, blo), y_ref)
    outs = stiffness([st_ref[0, :32] * t for t in d], ohi, olo, bhi, blo, y_ref, 32)
    nx = xs_ref.shape[0] // 2
    for c in range(3):
        e = tail(2, 3, coef_ref, owner_ref, st_ref, r, d, x, outs, c)
        part = jnp.concatenate([owner2_ref[...] * x2_ref[c], e], 0)
        p_out[c] = part
        faces = sel(xs_ref[...], part)
        s0_ref[c], s1_ref[c] = for_pairs(idx_ref, 0, faces[:nx], faces[nx:])


def up2_body(
    idx_ref, coef_ref, p_ref, rx0, rx1, ry0, ry1, sum_ref, sum1_ref, b_ref, st_ref, owner_ref, ahi, alo, ohi, olo, bhi, blo, xs_ref,
    pxy_ref, pz_ref, p_out, s0_ref, s1_ref, y_ref,
):
    x = []
    for c in range(3):
        fine = gather_sum(idx_ref, sum_ref, p_ref[c, :64], rx0[c, :NX2], rx1[c, :NX2], ry0[c, :NY2], ry1[c, :NY2])
        e = gather_sum(idx_ref, sum1_ref, p_ref[c, 64:], rx0[c, NX2:], rx1[c, NX2:], ry0[c, NY2:], ry1[c, NY2:])
        x.append(fine + (1.0 - st_ref[1]) * rsel(sel(pxy_ref[...], e), pz_ref[...]))
    b = [b_ref[c] for c in range(3)]
    r, d, x = smooth(1, 2, coef_ref, st_ref, b, x, 2, (ahi, alo, bhi, blo), y_ref)
    outs = stiffness([st_ref[0, :64] * t for t in d], ohi, olo, bhi, blo, y_ref, 64)
    nx = xs_ref.shape[0] // 2
    for c in range(3):
        part = tail(1, 2, coef_ref, owner_ref, st_ref, r, d, x, outs, c)
        p_out[c] = part
        faces = sel(xs_ref[...], part)
        s0_ref[c], s1_ref[c] = for_pairs(idx_ref, 0, faces[:nx], faces[nx:])


def swap(axis, s0, s1):
    n = GX if axis == "gx" else GY
    even = [(i, i ^ 1) for i in range(n)]
    odd = [(i, (((i - 1) ^ 1) + 1) % n) for i in range(n)]
    return lax.ppermute(s0, axis, even), lax.ppermute(s1, axis, odd)


def chebyshev_table(spectrum):
    low, top = spectrum[:, 0], spectrum[:, 1]
    center, radius = 0.5 * (top + low), 0.5 * (top - low)
    ratio = center / radius
    rho = 1.0 / ratio
    columns = [1.0 / center]
    for _ in range(3):
        after = 1.0 / (2.0 * ratio - rho)
        columns += [after * rho, 2.0 * after / radius]
        rho = after
    return jnp.stack(columns, 1)


def interp_tables():
    plane = {}
    for key, degree, halo, fine, rows, coarse, rows_c in (
        (4, 4, 0, NODES["4"], 224, NODES["2o"], 64),
        (2, 2, 0, NODES["2o"], 64, NODES["1o"], 32),
        ("2e", 2, 2, NODES["2e"], 256, NODES["1e"], 96),
    ):
        px, py = prolong_line(degree, EX + 2 * halo), prolong_line(degree, EY + 2 * halo)
        f0, c0 = degree * halo, degree * halo // 2
        full = np.zeros((rows, rows_c))
        for r, q in ((r, q) for r in range(len(fine)) for q in range(len(coarse))):
            if fine[r] is not None and coarse[q] is not None:
                (i, j), (a, b) = fine[r], coarse[q]
                full[r, q] = px[i + f0, a + c0] * py[j + f0, b + c0]
        plane[key] = full.astype(ml_dtypes.bfloat16)
    z4 = prolong_line(4, 32)[:128, :64]
    z2 = prolong_line(2, 32)[:64, :32]
    pz4 = np.zeros((2, 128, 128))
    for v in range(2):
        pz4[v, 64 * v : 64 * v + 64, :] = z4.T
    pz2 = np.zeros((128, 128))
    for v in range(2):
        pz2[32 * v : 32 * v + 32, 64 * v : 64 * v + 64] = z2.T
    cast = lambda t: np.ascontiguousarray(t).astype(ml_dtypes.bfloat16)
    return plane, cast(pz4), cast(pz4.transpose(0, 2, 1)), cast(pz2), cast(pz2.T)


def local(modes, moduli, pinned, spectrum):
    idx = (lax.axis_index("gx") * 16 + lax.axis_index("gy")).astype(jnp.int32).reshape(1)
    coef = chebyshev_table(spectrum)
    modes = modes.reshape(2, 3, NX * NY, NZ)
    moduli = moduli.reshape(NX * NY, NZ)
    pinned = pinned.reshape(NX * NY, NZ)

    zmats = {p: hi_lo(z_matrices(p, 1 if p == 4 else 2)) for p in (4, 2, 1)}
    plane, pz4, rz4, pz2, rz2 = interp_tables()
    bf = lambda t: np.ascontiguousarray(t).astype(ml_dtypes.bfloat16)
    x2, x20, x1, x21 = EXCH["2"], EXCH["20"], EXCH["1"], EXCH["21"]

    at4 = {n: r for r, n in enumerate(NODES["4"])}
    at2e = {n: r for r, n in enumerate(NODES["2e"]) if n is not None}
    pick2 = one_hot(64, NX * NY, [(r, at4[(2 * i, 2 * j)]) for r, (i, j) in enumerate(NODES["2o"]) if i < 6 and j < 8])
    zw, zm = np.zeros((128, 128)), np.zeros((128, 128))
    dw, dm, d1w, d1m = (np.zeros((128, 128)) for _ in range(4))
    for k in range(64):
        zw[2 * k, k] = zm[2 * k, 64 + k] = 1.0
        for v in range(2):
            dw[k, 64 * v + k] = dm[64 + k, 64 * v + k] = 1.0
            if k % 2 == 0:
                d1w[k, 32 * v + k // 2] = d1m[64 + k, 32 * v + k // 2] = 1.0
    pick1 = one_hot(96, 256, [(r, at2e[(2 * n[0], 2 * n[1])]) for r, n in enumerate(NODES["1e"]) if n is not None])
    owner2, owner1 = np.zeros((64, 128), np.float32), np.zeros((32, 128), np.float32)
    for r, (i, j) in enumerate(NODES["2o"]):
        owner2[r] = float(i < 6 and j < 8)
    for r, (i, j) in enumerate(NODES["1o"]):
        owner1[r] = float(i < 3 and j < 4)
    kd4, l4 = kd_tables(NODES["4"], 224, 4)
    kd2, l2 = kd_tables(NODES["2e"], 256, 2)
    kd1, l1 = kd_tables(NODES["1e"], 96, 1)
    table4 = np.concatenate([setup_table(4, NODES["4"], 256, 0), l4], 0)
    table4[0:224, 64:72] = kd4
    table2 = setup_table(2, NODES["2e"], 256, 2)
    table1 = setup_table(1, NODES["1e"], 96, 2)
    first = np.zeros((192 + 2 * NX2 + 2 * NY2, 256))
    first[0:64, 0 : NX * NY] = pick2
    first[64:192, 0:128], first[64:192, 128:256] = zw, zm
    first[192 : 192 + 2 * NX2, 0:64] = x2["xs"]
    first[192 + 2 * NX2 :, 0 : 64 + 2 * NX2] = x2["ys"]
    first = bf(first)

    mx = 128 + x2["nx"]
    my = 128 + x2["ny"]
    q2own, sx0, sx1, line, ys = call(
        pack_x_body, "pack_x", [idx], [modes, moduli, pinned, first],
        [((64, 128), F32), ((mx, 128), F32), ((mx, 128), F32), ((128, 128), F32), ((2 * NY2, 256), BF16)], [pltpu.VMEM((NX * NY, NZ), F32)],
    )
    rx0, rx1 = swap("gx", sx0, sx1)
    a4 = plane_matrices(idx, 4, table4, 256, 0, [(224, 256)])
    sy0, sy1 = call(
        pack_y_body, "pack_y", [idx], [line, q2own, rx0, rx1, ys], [((my, 128), F32), ((my, 128), F32)],
    )
    ry0, ry1 = swap("gy", sy0, sy1)
    mats2 = plane_matrices(idx, 2, table2, 256, 2, [(144, 256), (64, 64)])
    mats1 = plane_matrices(idx, 1, table1, 96, 2, [(64, 96), (32, 32)])

    big = ((3, 224, 256), F32)
    msgx, msgy = ((3, X4, 256), F32), ((3, Y4, 256), F32)
    y4 = pltpu.VMEM((3, 4 * 224, 256), F32)
    y4f = pltpu.VMEM((3, 4 * 48, 256), F32)
    full = pltpu.VMEM((6, 224, 128), F32)
    keep = pltpu.VMEM((3, 224, 256), F32)
    halves = ((6, 224, 128), F32)
    mats4 = [*a4, *zmats[4]]

    b, st4, d, w, s0, s1 = call(
        first4_body, "first4", [idx, coef], [modes, moduli, pinned, rx0, rx1, ry0, ry1, table4, *mats4],
        [big, ((5, 224, 128), F32), big, big, msgx, msgx], [y4f],
    )
    st2, st1 = call(
        statics_body, "statics", [idx],
        [q2own, rx0, rx1, ry0, ry1, x2["sum"], bf(np.stack([dw, dm, d1w, d1m])), pick1, kd2, l2, kd1, l1],
        [((5, 256, 128), F32), ((5, 96, 128), F32)],
    )

    def trade4(u, s0, s1):
        r0, r1 = swap("gx", s0, s1)
        (w,) = call(block4_body, "block4", [], [u, *mats4], [halves], [y4], flops=10**10)
        t0, t1 = call(faces_y4_body, "faces_y4", [idx], [w, r0, r1], [msgy, msgy])
        return [w, r0, r1, *swap("gy", t0, t1)]

    def trade(table, p, s0, s1, sums=None):
        r0, r1 = swap("gx", s0, s1)
        t0, t1 = call(faces_y_body, "faces_y", [idx], [p, r0, r1, table["ys"]], [((3, table["ny"], 128), F32)] * 2)
        return [p, r0, r1, *swap("gy", t0, t1), *([table["sum"]] if sums is None else sums)]

    got = trade4(w, s0, s1)
    r, d, x, w, s0, s1 = call(
        functools.partial(mid4_body, 1), "mid4", [idx, coef], [*got, st4, b, d, d, *mats4], [big, big, big, big, msgx, msgx], [y4f, full],
    )
    got = trade4(w, s0, s1)
    face2, face20, face1, face21 = (((3, t["nx"], 128), F32) for t in (x2, x20, x1, x21))
    own2f, own1f = ((3, 64, 128), F32), ((3, 32, 128), F32)
    x4, p2, s0, s1 = call(
        resid4_body, "resid4", [idx, coef], [*got, st4, r, d, x, *mats4, bf(plane[4].T), rz4, x2["xs"]],
        [big, own2f, face2, face2], [y4, full, keep],
    )
    y2, y1 = pltpu.VMEM((3, 4 * 144, 128), F32), pltpu.VMEM((3, 4 * 64, 128), F32)
    b2, xo2, p1, s0, s1 = call(
        down2_body, "down2", [idx, coef],
        [*trade(x2, p2, s0, s1), st2, bf(plane[2].T), rz2, x1["xs"], *mats2, *zmats[2], owner2],
        [((3, 256, 128), F32), own2f, own1f, face1, face1], [y2],
    )
    p2, s0, s1 = call(
        bottom_body, "bottom", [idx, coef],
        [*trade(x1, p1, s0, s1), st1, owner1, *mats1, *zmats[1], xo2, owner2, x21["xs"]],
        [((3, 96, 128), F32), face21, face21], [y1],
    )
    p2, s0, s1 = call(
        up2_body, "up2", [idx, coef],
        [*trade(x21, p2, s0, s1, (x2["sum"], x1["sum"])), b2, st2, owner2, *mats2, *zmats[2], x20["xs"], plane["2e"], pz2],
        [own2f, face20, face20], [y2],
    )
    x, w, s0, s1 = call(
        rise4_body, "rise4", [idx], [*trade(x20, p2, s0, s1), plane[4], pz4, st4, x4, *mats4], [big, big, msgx, msgx], [y4f],
    )
    r, d, x, w, s0, s1 = call(
        functools.partial(mid4_body, 0), "mid4_0", [idx, coef], [*trade4(w, s0, s1), st4, b, x, x, *mats4],
        [big, big, big, big, msgx, msgx], [y4f, full],
    )
    r, d, x, w, s0, s1 = call(
        functools.partial(mid4_body, 1), "mid4", [idx, coef], [*trade4(w, s0, s1), st4, r, d, x, *mats4],
        [big, big, big, big, msgx, msgx], [y4f, full],
    )
    (out,) = call(
        last4_body, "last4", [idx, coef], [*trade4(w, s0, s1), st4, r, d, x], [((2, 3, NX * NY, NZ), F32)], [full],
    )
    return out.reshape(2, 3, NX, NY, NZ)


def solution(mesh):
    placed = (P(None, None, "gx", "gy", None), P("gx", "gy", None), P("gx", "gy", None), P())
    return jax.shard_map(
        local,
        mesh=mesh,
        in_specs=placed,
        out_specs=P(None, None, "gx", "gy", None),
        check_vma=False,
    )
```

```python
import functools

import jax
import jax.numpy as jnp
import ml_dtypes
import numpy as np
from jax import lax
from jax.experimental import pallas as pl
from jax.experimental.pallas import tpu as pltpu
from jax.sharding import PartitionSpec as P

F32 = jnp.float32
BF16 = jnp.bfloat16
COUPLE = 2.5
NX, NY, NZ = 12, 16, 128
EX, EY = 3, 4
GX, GY = 16, 16

PROLONG = {
    4: np.array([[1.0, 0.0, 0.0], [0.375, 0.75, -0.125], [0.0, 1.0, 0.0], [-0.125, 0.75, 0.375]]),
    2: np.array([[1.0, 0.0], [0.5, 0.5]]),
}


def element_matrices(degree):
    points, weights = np.polynomial.legendre.leggauss(8)
    points, weights = 0.5 * (points + 1.0), 0.5 * weights
    nodes = np.arange(degree + 1) / degree
    values = np.zeros((degree + 1, points.size))
    slopes = np.zeros((degree + 1, points.size))
    for i in range(degree + 1):
        others = [j for j in range(degree + 1) if j != i]
        values[i] = np.prod([(points - nodes[j]) / (nodes[i] - nodes[j]) for j in others], axis=0)
        for k in others:
            rest = [(points - nodes[j]) / (nodes[i] - nodes[j]) for j in others if j != k]
            slopes[i] += np.prod(rest, axis=0) / (nodes[i] - nodes[k]) if rest else 1.0 / (nodes[i] - nodes[k])
    mass = (values * weights) @ values.T
    stiff = (slopes * weights) @ slopes.T
    mixed = (slopes * weights) @ values.T
    return [mass, stiff, mixed, mixed.T]


ELEMENTS = {p: element_matrices(p) for p in (4, 2, 1)}


def line_matrix(element, count):
    degree = element.shape[0] - 1
    full = np.zeros((degree * count + 1, degree * count + 1))
    for e in range(count):
        full[degree * e : degree * e + degree + 1, degree * e : degree * e + degree + 1] += element
    return full


def z_matrices(degree, copies):
    count = NZ // 4
    length = count * degree
    out = np.zeros((4, 128, 128))
    for k, element in enumerate(ELEMENTS[degree]):
        full = line_matrix(element, count)[:length, :length].copy()
        full[0, 0] += element[degree, degree]
        for v in range(copies):
            out[k, v * length : (v + 1) * length, v * length : (v + 1) * length] = full.T
    return out


def hi_lo(array):
    array = array.astype(np.float32)
    hi = array.astype(ml_dtypes.bfloat16)
    lo = (array - hi.astype(np.float32)).astype(ml_dtypes.bfloat16)
    return hi, lo


def prolong_line(degree, count):
    table = PROLONG[degree]
    half = degree // 2
    full = np.zeros((degree * count + 1, half * count + 1))
    for e in range(count):
        for a in range(degree):
            for t in range(table.shape[1]):
                full[degree * e + a, half * e + t] += table[a, t]
    full[-1, -1] = 1.0
    return full


def natural(degree, halo):
    return [
        (i, j)
        for i in range(-degree * halo, degree * (EX + halo) + 1)
        for j in range(-degree * halo, degree * (EY + halo) + 1)
    ]


def pad_to(n, m):
    return -(-n // m) * m


NODES4 = (
    [(i, j) for i in range(NX) for j in range(NY)]
    + [(NX, j) for j in range(NY)]
    + [(i, NY) for i in range(NX)]
    + [(NX, NY)]
)


def in_rings(degree, parts):
    nodes, seen = [], set()
    for halo, rows in enumerate(parts):
        ring = [n for n in natural(degree, halo) if n not in seen]
        seen.update(ring)
        nodes += ring + [None] * (rows - len(ring))
    return nodes


RINGS = {2: (64, 80, 112), 1: (32, 32, 32)}
NODES = {
    "4": NODES4,
    "2o": natural(2, 0),
    "2e": in_rings(2, RINGS[2]),
    "1o": natural(1, 0),
    "1e": in_rings(1, RINGS[1]),
}


def one_hot(rows, cols, pairs):
    out = np.zeros((rows, cols), np.float32)
    for r, c in pairs:
        out[r, c] = 1.0
    return out.astype(ml_dtypes.bfloat16)


def exchange_tables(degree, halo, own, ext, rows_own, rows_ext):
    bx, by = degree * EX, degree * EY
    layers = degree * halo + 1
    own_at = {node: r for r, node in enumerate(own)}
    xlo = [(i, j) for i in range(layers) for j in range(by + 1)]
    xhi = [(bx - layers + 1 + i, j) for i in range(layers) for j in range(by + 1)]
    nx = pad_to(len(xlo), 16)
    sources = [(node, r) for node, r in own_at.items()]
    sources += [((i - bx, j), rows_own + r) for r, (i, j) in enumerate(xhi)]
    sources += [((i + bx, j), rows_own + nx + r) for r, (i, j) in enumerate(xlo)]
    span = range(-degree * halo, bx + degree * halo + 1)
    ylo = [(i, j) for i in span for j in range(layers)]
    yhi = [(i, by - layers + 1 + j) for i in span for j in range(layers)]
    ny = pad_to(len(ylo), 16)
    xs = [one_hot(nx, rows_own, [(r, own_at[n]) for r, n in enumerate(face)]) for face in (xlo, xhi)]
    width = rows_own + 2 * nx
    ys = [
        one_hot(ny, width, [(r, c) for r, n in enumerate(face) for node, c in sources if node == n])
        for face in (ylo, yhi)
    ]
    sources2 = list(sources)
    sources2 += [((i, j - by), width + r) for r, (i, j) in enumerate(yhi)]
    sources2 += [((i, j + by), width + ny + r) for r, (i, j) in enumerate(ylo)]
    ext_at = {node: r for r, node in enumerate(ext) if node is not None}
    total = one_hot(rows_ext, width + 2 * ny, [(ext_at[n], c) for n, c in sources2 if n in ext_at])
    return {
        "nx": nx,
        "ny": ny,
        "xs": np.concatenate(xs, 0),
        "ys": np.concatenate(ys, 0),
        "sum": total,
    }


EXCH = {
    "2": exchange_tables(2, 2, NODES["2o"], NODES["2e"], 64, 256),
    "20": exchange_tables(2, 0, NODES["2o"], NODES["2o"], 64, 64),
    "1": exchange_tables(1, 2, NODES["1o"], NODES["1e"], 32, 96),
}


def side_by_side(a, own_a, b, own_b):
    own, nx, ny = own_a + own_b, a["nx"] + b["nx"], a["ny"] + b["ny"]
    out = {"nx": nx, "ny": ny}
    spread = lambda t, o, first: np.concatenate(
        [
            np.arange(o) + (0 if first else own_a),
            *(own + k * nx + (0 if first else a["nx"]) + np.arange(t["nx"]) for k in range(2)),
            *(own + 2 * nx + k * ny + (0 if first else a["ny"]) + np.arange(t["ny"]) for k in range(2)),
        ]
    )
    for key, width, step in (("xs", own, "nx"), ("ys", own + 2 * nx, "ny")):
        blocks = []
        for k in range(2):
            for t, o, first in ((a, own_a, True), (b, own_b, False)):
                rows = t[key][k * t[step] : (k + 1) * t[step]]
                block = np.zeros((rows.shape[0], width), ml_dtypes.bfloat16)
                block[:, spread(t, o, first)[: rows.shape[1]]] = rows
                blocks.append(block)
        out[key] = np.concatenate(blocks, 0)
    return out


EXCH["21"] = side_by_side(EXCH["2"], 64, EXCH["1"], 32)


def setup_table(degree, nodes, rows, halo):
    out = np.zeros((rows, 128), np.float32)
    for r, node in enumerate(nodes):
        if node is not None:
            out[r, node[0] + degree * halo] = out[r, 32 + node[1] + degree * halo] = 1.0
    parts = [out]
    for wide in (True, False) if halo else (False,):
        grow, start = (halo, 0) if wide else (0, degree * halo)
        for element in ELEMENTS[degree]:
            table = np.zeros((32, 128), np.float32)
            for at, count in ((0, EX + 2 * grow), (32, EY + 2 * grow)):
                n = degree * count + 1
                table[start : start + n, at + start : at + start + n] = line_matrix(element, count)
            parts.append(table)
    return np.concatenate(parts, 0)


def kd_tables(nodes, rows, degree):
    m = lambda a: ELEMENTS[degree][0][a % degree, a % degree] + (ELEMENTS[degree][0][degree, degree] if a % degree == 0 else 0.0)
    k = lambda a: ELEMENTS[degree][1][a % degree, a % degree] + (ELEMENTS[degree][1][degree, degree] if a % degree == 0 else 0.0)
    out = np.zeros((rows, 8), np.float32)
    for r, node in enumerate(nodes):
        if node is None:
            continue
        i, j = node
        for c in range(3):
            co = [1.0 + COUPLE * (c == e) for e in range(3)]
            out[r, c] = co[0] * k(i) * m(j) + co[1] * m(i) * k(j)
            out[r, 3 + c] = co[2] * m(i) * m(j)
    copies = {4: 1, 2: 2, 1: 2}[degree]
    length = NZ // 4 * degree
    lanes = np.zeros((8, 128), np.float32)
    for z in range(length):
        for v in range(copies):
            lanes[0, v * length + z] = m(z)
            lanes[1, v * length + z] = k(z)
    return out, lanes


def dot(a, b):
    return jnp.dot(a, b, preferred_element_type=F32)


def split(v):
    hi = v.astype(BF16)
    return hi, (v - hi.astype(F32)).astype(BF16)


def sel(exact, v):
    hi, lo = split(v)
    return dot(exact, hi) + dot(exact, lo)


def sel3(exact, v):
    hi = v.astype(BF16)
    rest = v - hi.astype(F32)
    mid = rest.astype(BF16)
    lo = (rest - mid.astype(F32)).astype(BF16)
    return dot(exact, hi) + dot(exact, mid) + dot(exact, lo)


def rsel(v, exact):
    hi, lo = split(v)
    return dot(hi, exact) + dot(lo, exact)


def rsel3(v, exact):
    hi = v.astype(BF16)
    rest = v - hi.astype(F32)
    mid = rest.astype(BF16)
    lo = (rest - mid.astype(F32)).astype(BF16)
    return dot(hi, exact) + dot(mid, exact) + dot(lo, exact)


def place(idx_ref, axis):
    at = idx_ref[0]
    at = (at >> 4) if axis == 0 else (at & 15)
    even = (at & 1) == 0
    return even, (at > 0).astype(F32), (at < (GX, GY)[axis] - 1).astype(F32)


def for_pairs(idx_ref, axis, lo, hi):
    even, _, _ = place(idx_ref, axis)
    return jnp.where(even, hi, lo), jnp.where(even, lo, hi)


def from_pairs(idx_ref, axis, r0, r1):
    even, has_lo, has_hi = place(idx_ref, axis)
    return jnp.where(even, r1, r0) * has_lo, jnp.where(even, r0, r1) * has_hi


def stiffness(fields, ahi, alo, bhi, blo, y_ref, rows, picks=None):
    cols, block = ahi.shape[2], ahi.shape[1] // 4
    for s in range(3):
        u = fields[s]
        if cols != u.shape[0]:
            u = jnp.concatenate([u, jnp.zeros((cols - u.shape[0], u.shape[1]), F32)], 0)
        uh, ul = split(u)
        if rows == block:
            high, low = ahi[s], alo[s]
        else:
            spans = [(block * k + a, block * k + b) for k in range(4) for a, b in picks or ((0, rows),)]
            high, low = (jnp.concatenate([m[s, a:b, :] for a, b in spans], 0) for m in (ahi, alo))
        if u.shape[1] == 128:
            both = dot(high, jnp.concatenate([uh, ul], 1))
            y_ref[s, : 4 * rows] = both[:, :128] + both[:, 128:] + dot(low, uh)
        else:
            y_ref[s, : 4 * rows] = dot(high, uh) + dot(high, ul) + dot(low, uh)
    part = lambda s, k: y_ref[s, k * rows : (k + 1) * rows, :]
    plans = (
        (lambda: part(0, 0) + part(1, 2), lambda: part(0, 1), lambda: part(2, 2), 3),
        (lambda: part(1, 0) + part(0, 2), lambda: part(1, 1), lambda: part(2, 3), 3),
        (lambda: part(2, 0), lambda: part(2, 1), lambda: part(0, 3) + part(1, 3), 2),
    )
    outs = []
    for first, second, third, mixed in plans:
        mats_h = jnp.concatenate([bhi[0], bhi[1], bhi[mixed]], 0)
        mats_l = jnp.concatenate([blo[0], blo[1], blo[mixed]], 0)
        one, two, three = first(), second(), third()
        halves = []
        for v in range(one.shape[1] // 128):
            cut = lambda t: t[:, 128 * v : 128 * v + 128]
            h, l = split(jnp.concatenate([cut(one), cut(two), cut(three)], 1))
            halves.append(dot(h, mats_h) + dot(l, mats_h) + dot(h, mats_l))
        outs.append(halves[0] if len(halves) == 1 else jnp.concatenate(halves, 1))
    return outs


def wide(v):
    return jnp.concatenate([v, v], 1)


VMEM = pl.BlockSpec(memory_space=pltpu.VMEM)
SMEM = pl.BlockSpec(memory_space=pltpu.SMEM)


def call(body, name, smem, args, outs, scratch=(), flops=1000000, limit=40):
    return pl.pallas_call(
        body,
        name=name,
        out_shape=[jax.ShapeDtypeStruct(shape, dtype) for shape, dtype in outs],
        in_specs=[SMEM] * len(smem) + [VMEM] * len(args),
        out_specs=[VMEM] * len(outs),
        scratch_shapes=list(scratch),
        compiler_params=pltpu.CompilerParams(vmem_limit_bytes=limit * 2**20),
        cost_estimate=pl.CostEstimate(flops=flops, bytes_accessed=100000, transcendentals=0),
    )(*smem, *args)


def setup_body(rows_in, plans, idx_ref, c_ref, *refs):
    *outs, xe_ref, ye_ref = refs
    at = idx_ref[0]
    hdot = lambda a, b: sel3(a.astype(BF16), b)

    def tdot(a, b):
        hi = a.astype(BF16)
        rest = a - hi.astype(F32)
        mid = rest.astype(BF16)
        b = b.astype(BF16)
        turn = lambda x: lax.dot_general(x, b, (((1,), (1,)), ((), ())), preferred_element_type=F32)
        return turn(hi) + turn(mid) + turn((rest - mid.astype(F32)).astype(BF16))

    m, k, g, t = range(4)
    strong = 1.0 + COUPLE
    for p, (rows, cols, corner, corr) in enumerate(plans):
        for q in range(4):
            table = c_ref[rows_in + 128 * p + 32 * q : rows_in + 128 * p + 32 * q + 32, :]
            x1, y1 = table[:, 0:32], table[:, 32:64]
            if corner is not None:
                i, j = (lax.broadcasted_iota(jnp.int32, (32, 32), d) for d in (0, 1))
                spot = jnp.where((i == corner) & (j == corner), corr[q], 0.0)
                x1 = x1 + spot * ((at >> 4) == 0).astype(F32)
                y1 = y1 + spot * ((at & 15) == 0).astype(F32)
            ox, oy = c_ref[0:rows_in, 0:32], c_ref[0:rows_in, 32:64]
            xe_ref[q, :rows, :cols] = tdot(hdot(ox[:rows], x1), ox[:cols])
            ye_ref[q, :rows, :cols] = tdot(hdot(oy[:rows], y1), oy[:cols])
        xy = lambda a, b: xe_ref[a, :rows, :cols] * ye_ref[b, :rows, :cols]
        blocks = (
            (lambda: strong * xy(k, m) + xy(m, k), lambda: xy(m, m), lambda: COUPLE * xy(t, g), lambda: COUPLE * xy(t, m)),
            (lambda: xy(k, m) + strong * xy(m, k), lambda: xy(m, m), lambda: COUPLE * xy(g, t), lambda: COUPLE * xy(m, t)),
            (lambda: xy(k, m) + xy(m, k), lambda: strong * xy(m, m), lambda: COUPLE * xy(g, m), lambda: COUPLE * xy(m, g)),
        )
        for s in range(3):
            for b in range(4):
                hi, lo = split(blocks[s][b]())
                outs[2 * p][s, b * rows : (b + 1) * rows, :] = hi
                outs[2 * p + 1][s, b * rows : (b + 1) * rows, :] = lo
    if len(outs) > 2 * len(plans):
        outs[-1][...] = jnp.zeros((8, 128), F32)


def plane_matrices(idx, degree, table, rows_in, halo, sizes, token=False):
    corr = [float(np.float32(e[degree, degree])) for e in ELEMENTS[degree]]
    plans = [(*sizes[-1], degree * halo, corr)]
    if halo:
        plans = [(*sizes[0], None, None)] + plans
    outs = [((3, 4 * r, c), BF16) for r, c, *_ in plans for _ in range(2)]
    return call(
        functools.partial(setup_body, rows_in, plans),
        "setup_" + str(degree),
        [idx],
        [table],
        outs + ([((8, 128), F32)] if token else []),
        [pltpu.VMEM((4, rows_in, rows_in), F32), pltpu.VMEM((4, rows_in, rows_in), F32)],
    )


NX2, NY2 = EXCH["2"]["nx"], EXCH["2"]["ny"]


def pack_x_body(idx_ref, modes_ref, w_ref, pin_ref, c_ref, own_ref, s0_ref, s1_ref, line_ref, ys_ref, m_ref):
    ys_ref[...] = c_ref[192 + 2 * NX2 :, :]
    w = w_ref[...]
    m = 1.0 - pin_ref[...].astype(F32)
    m_ref[...] = m
    pick = c_ref[0:64, 0 : NX * NY]
    own = rsel3(sel3(pick, w), c_ref[64:192, 0:128]) + rsel(sel(pick, m), c_ref[64:192, 128:256])
    own_ref[...] = own
    faces = sel3(c_ref[192 : 192 + 2 * NX2, 0:64], own)
    a, b = for_pairs(idx_ref, 0, faces[:NX2], faces[NX2:])
    for ref, face in ((s0_ref, a), (s1_ref, b)):
        for v in range(2):
            for c in range(3):
                ref[16 * (3 * v + c) : 16 * (3 * v + c) + 16, :] = modes_ref[v, c, 0:16, :]
        ref[96:112, :] = w[0:16]
        ref[112:128, :] = m[0:16]
        ref[128 : 128 + NX2, :] = face
    line_ref[...] = jnp.zeros((128, 128), F32)
    for k in range(8):
        if k < 6:
            line = modes_ref[k // 3, k % 3, pl.ds(0, NX, stride=NY), :]
        else:
            line = (w_ref if k == 6 else m_ref)[pl.ds(0, NX, stride=NY), :]
        line_ref[16 * k : 16 * k + NX, :] = line


def pack_y_body(idx_ref, line_ref, own_ref, r0_ref, r1_ref, ys_ref, s0_ref, s1_ref):
    lo, hi = from_pairs(idx_ref, 0, r0_ref[...], r1_ref[...])
    stack = jnp.concatenate([own_ref[...], lo[128:], hi[128:]], 0)
    faces = sel3(ys_ref[:, 0 : 64 + 2 * NX2], stack)
    a, b = for_pairs(idx_ref, 1, faces[:NY2], faces[NY2:])
    for ref, face in ((s0_ref, a), (s1_ref, b)):
        ref[0:128, :] = line_ref[...]
        for k in range(8):
            ref[16 * k + NX : 16 * k + NX + 1, :] = hi[16 * k : 16 * k + 1]
        ref[128 : 128 + NY2, :] = face


def static_of(w, m, kd, lanes):
    s = w * m
    f = 1.0 - m
    s2 = s * s
    inv = [1.0 / (s2 * (kd[:, c : c + 1] * lanes[0:1] + kd[:, 3 + c : 4 + c] * lanes[1:2]) + f) for c in range(3)]
    return s, f, inv


def statics_body(
    idx_ref, own_ref, rx0_ref, rx1_ref, ry0_ref, ry1_ref, sum_ref, d_ref, pick1_ref, kd2_ref, l2_ref, kd1_ref, l1_ref,
    e2_ref, e1_ref,
):
    xlo, xhi = from_pairs(idx_ref, 0, rx0_ref[128:, :], rx1_ref[128:, :])
    ylo, yhi = from_pairs(idx_ref, 1, ry0_ref[128:, :], ry1_ref[128:, :])
    ext = sel3(sum_ref[...], jnp.concatenate([own_ref[...], xlo, xhi, ylo, yhi], 0))

    def put(ref, w, m, kd, lanes):
        s, f, inv = static_of(w, m, kd, lanes)
        ref[0], ref[1] = s, f
        for c in range(3):
            ref[2 + c] = inv[c]

    put(e2_ref, rsel3(ext, d_ref[0]), rsel(ext, d_ref[1]), kd2_ref[...], l2_ref[...])
    coarse = sel3(pick1_ref[...], ext)
    put(e1_ref, rsel3(coarse, d_ref[2]), rsel(coarse, d_ref[3]), kd1_ref[...], l1_ref[...])


X4, Y4 = 24, 16


FACES4 = ((0, 16), (192, 224))


def faces_x4(idx_ref, fields, mats, y_ref, u_ref, s0_ref, s1_ref):
    even, _, _ = place(idx_ref, 0)
    outs = stiffness(fields, *mats, y_ref, 48, FACES4)
    for c in range(3):
        u_ref[c] = fields[c]
        w = outs[c]
        lo = jnp.concatenate([w[0:16], w[32:40]], 0)
        hi = jnp.concatenate([w[16:32], w[40:48]], 0)
        s0_ref[c] = jnp.where(even, hi, lo)
        s1_ref[c] = jnp.where(even, lo, hi)


def block4_body(u_ref, ahi, alo, bhi, blo, out_ref, y_ref):
    put4(out_ref, stiffness([u_ref[c] for c in range(3)], ahi, alo, bhi, blo, y_ref, 224))


LO16, HI16 = 16, 20


def faces_y4_body(idx_ref, w_ref, r0_ref, r1_ref, s0_ref, s1_ref):
    even, _, _ = place(idx_ref, 1)
    for c in range(3):
        xlo, xhi = from_pairs(idx_ref, 0, r0_ref[c], r1_ref[c])
        row = lax.broadcasted_iota(jnp.int32, (Y4, 256), 0)
        lo = jnp.concatenate([w_ref[2 * c + v, pl.ds(0, NX, stride=NY), :] for v in range(2)], 1)
        lo = jnp.concatenate([lo, jnp.concatenate([w_ref[2 * c + v, 192:196, :] for v in range(2)], 1)], 0)
        hi = jnp.concatenate([w_ref[2 * c + v, 208:224, :] for v in range(2)], 1)
        lo = lo + jnp.where(row == 0, xlo[0:1], 0.0) + jnp.where(row == NX, xhi[0:1], 0.0)
        hi = hi + jnp.where(row == 0, xlo[HI16 : HI16 + 1], 0.0) + jnp.where(row == NX, xhi[LO16 : LO16 + 1], 0.0)
        s0_ref[c] = jnp.where(even, hi, lo)
        s1_ref[c] = jnp.where(even, lo, hi)


def summed4(idx_ref, w_ref, rx0, rx1, ry0, ry1, full_ref):
    row = lax.broadcasted_iota(jnp.int32, (Y4, 256), 0)
    for c in range(3):
        xlo, xhi = from_pairs(idx_ref, 0, rx0[c], rx1[c])
        ylo, yhi = from_pairs(idx_ref, 1, ry0[c], ry1[c])
        yhi = jnp.where(row <= NX, yhi, 0.0)
        yhi = yhi + jnp.where(row == 0, xlo[HI16 : HI16 + 1], 0.0) + jnp.where(row == NX, xhi[LO16 : LO16 + 1], 0.0)
        end = xhi[0:16] + jnp.where(row == 0, ylo[NX : NX + 1], 0.0)
        for v in range(2):
            k, cut = 2 * c + v, slice(128 * v, 128 * v + 128)
            full_ref[k] = w_ref[k]
            full_ref[k, 0:16, :] += xlo[0:16, cut]
            full_ref[k, 192:208, :] += end[:, cut]
            full_ref[k, 208:224, :] += yhi[:, cut]
            full_ref[k, pl.ds(0, NX, stride=NY), :] += ylo[:NX, cut]


def put4(ref, outs):
    for c in range(3):
        for v in range(2):
            ref[2 * c + v] = outs[c][:, 128 * v : 128 * v + 128]


def first4_body(
    idx_ref, coef_ref, modes_ref, w_ref, pin_ref, rx0_ref, rx1_ref, ry0_ref, ry1_ref, table_ref, ahi, alo, bhi, blo,
    b_ref, st_ref, d_ref, u_ref, s0_ref, s1_ref, y_ref,
):
    _, xhi = from_pairs(idx_ref, 0, rx0_ref[0:128, :], rx1_ref[0:128, :])
    _, yhi = from_pairs(idx_ref, 1, ry0_ref[0:128, :], ry1_ref[0:128, :])

    def gathered(own, k):
        return jnp.concatenate([own, xhi[16 * k : 16 * k + 16], yhi[16 * k : 16 * k + 16]], 0)

    w = gathered(w_ref[...], 6)
    m = gathered(1.0 - pin_ref[...].astype(F32), 7)
    s, f, inv = static_of(w, m, table_ref[0:224, 64:72], table_ref[384:392, :])
    st_ref[0], st_ref[1] = s, f
    for c in range(3):
        st_ref[2 + c] = inv[c]
    fields = []
    for c in range(3):
        b = jnp.concatenate([gathered(modes_ref[v, c], 3 * v + c) for v in range(2)], 1)
        b_ref[c] = b
        d = wide(inv[c]) * b * coef_ref[0, 0]
        d_ref[c] = d
        fields.append(wide(s) * d)
    faces_x4(idx_ref, fields, (ahi, alo, bhi, blo), y_ref, u_ref, s0_ref, s1_ref)


def both4(ref, c):
    return jnp.concatenate([ref[2 * c], ref[2 * c + 1]], 1)


def update4(idx_ref, coef_ref, step, w_ref, recv, st_ref, r_ref, d_ref, full_ref, c):
    s, f, inv = wide(st_ref[0]), wide(st_ref[1]), wide(st_ref[2 + c])
    r = r_ref[c] - (s * both4(full_ref, c) + f * d_ref[c])
    if step == 0:
        d = coef_ref[0, 0] * inv * r
    else:
        d = coef_ref[0, 2 * step - 1] * d_ref[c] + coef_ref[0, 2 * step] * inv * r
    return s, f, r, d


def mid4_body(
    step, idx_ref, coef_ref, w_ref, rx0, rx1, ry0, ry1, st_ref, r_ref, d_ref, x_ref, ahi, alo, bhi, blo,
    r_out, d_out, x_out, u_ref, s0_ref, s1_ref, y_ref, full_ref,
):
    summed4(idx_ref, w_ref, rx0, rx1, ry0, ry1, full_ref)
    fields = []
    for c in range(3):
        s, f, r, d = update4(idx_ref, coef_ref, step, w_ref, None, st_ref, r_ref, d_ref, full_ref, c)
        r_out[c], d_out[c] = r, d
        x_out[c] = x_ref[c] + d
        fields.append(s * d)
    faces_x4(idx_ref, fields, (ahi, alo, bhi, blo), y_ref, u_ref, s0_ref, s1_ref)


def resid4_body(
    idx_ref, coef_ref, w_ref, rx0, rx1, ry0, ry1, st_ref, r_ref, d_ref, x_ref, ahi, alo, bhi, blo, rxy_ref, rz_ref, xs_ref,
    x_out, p_ref, s0_ref, s1_ref, y_ref, full_ref, keep_ref,
):
    summed4(idx_ref, w_ref, rx0, rx1, ry0, ry1, full_ref)
    fields = []
    owned = lax.broadcasted_iota(jnp.int32, (224, 256), 0) < NX * NY
    for c in range(3):
        s, f, r, d = update4(idx_ref, coef_ref, 2, w_ref, None, st_ref, r_ref, d_ref, full_ref, c)
        x_out[c] = x_ref[c] + d
        keep_ref[c] = jnp.where(owned, (1.0 - f) * r, 0.0)
        fields.append(s * d)
    outs = stiffness(fields, ahi, alo, bhi, blo, y_ref, 224)
    nx = xs_ref.shape[0] // 2
    for c in range(3):
        left = sel(rxy_ref[...], keep_ref[c] - wide(st_ref[0]) * outs[c])
        part = rsel(left[:, :128], rz_ref[0]) + rsel(left[:, 128:], rz_ref[1])
        p_ref[c] = part
        faces = sel(xs_ref[...], part)
        s0_ref[c], s1_ref[c] = for_pairs(idx_ref, 0, faces[:nx], faces[nx:])


def rise4_body(
    idx_ref, p_ref, rx0, rx1, ry0, ry1, sum_ref, pxy_ref, pz_ref, st_ref, x_ref, ahi, alo, bhi, blo,
    x_out, u_ref, s0_ref, s1_ref, y_ref,
):
    fields = []
    s, m = wide(st_ref[0]), 1.0 - wide(st_ref[1])
    for c in range(3):
        e = gather_sum(idx_ref, sum_ref, p_ref[c], rx0[c], rx1[c], ry0[c], ry1[c])
        e = sel(pxy_ref[...], e)
        x = x_ref[c] + m * jnp.concatenate([rsel(e, pz_ref[0]), rsel(e, pz_ref[1])], 1)
        x_out[c] = x
        fields.append(s * x)
    faces_x4(idx_ref, fields, (ahi, alo, bhi, blo), y_ref, u_ref, s0_ref, s1_ref)


def last4_body(idx_ref, coef_ref, w_ref, rx0, rx1, ry0, ry1, st_ref, r_ref, d_ref, x_ref, out_ref, full_ref):
    summed4(idx_ref, w_ref, rx0, rx1, ry0, ry1, full_ref)
    for c in range(3):
        _, _, _, d = update4(idx_ref, coef_ref, 2, w_ref, None, st_ref, r_ref, d_ref, full_ref, c)
        x = x_ref[c] + d
        for v in range(2):
            out_ref[v, c] = x[: NX * NY, 128 * v : 128 * v + 128]


def gather_sum(idx_ref, sum_ref, own, rx0, rx1, ry0, ry1):
    xlo, xhi = from_pairs(idx_ref, 0, rx0, rx1)
    ylo, yhi = from_pairs(idx_ref, 1, ry0, ry1)
    return sel(sum_ref[...], jnp.concatenate([own, xlo, xhi, ylo, yhi], 0))


def faces_y_body(idx_ref, p_ref, r0_ref, r1_ref, ys_ref, s0_ref, s1_ref):
    ny = ys_ref.shape[0] // 2
    for c in range(3):
        lo, hi = from_pairs(idx_ref, 0, r0_ref[c], r1_ref[c])
        faces = sel(ys_ref[...], jnp.concatenate([p_ref[c], lo, hi], 0))
        s0_ref[c], s1_ref[c] = for_pairs(idx_ref, 1, faces[:ny], faces[ny:])


def smooth(level, degree, coef_ref, st_ref, b, x, steps, mats, y_ref):
    sizes = list(np.cumsum(RINGS[degree])[::-1])
    n = int(sizes.pop(0))

    def residual(r, v):
        nonlocal n
        u = [st_ref[0, :n] * t for t in v]
        n = int(sizes.pop(0))
        outs = stiffness(u, *mats, y_ref, n)
        s, f = st_ref[0, :n], st_ref[1, :n]
        return [a[:n] - (s * w + f * t[:n]) for a, w, t in zip(r, outs, v)]

    r = b if x is None else residual(b, x)
    d = [st_ref[2 + c, :n] * r[c] * coef_ref[level, 0] for c in range(3)]
    x = d if x is None else [a[:n] + t for a, t in zip(x, d)]
    for step in range(1, steps):
        r = residual(r, d)
        d = [coef_ref[level, 2 * step - 1] * d[c][:n] + coef_ref[level, 2 * step] * st_ref[2 + c, :n] * r[c] for c in range(3)]
        x = [a[:n] + t for a, t in zip(x, d)]
    return r, d, x


def down2_body(
    idx_ref, coef_ref, p_ref, rx0, rx1, ry0, ry1, sum_ref, st_ref, rxy_ref, rz_ref, xs_ref,
    ahi, alo, ohi, olo, bhi, blo, owner_ref,
    b_out, x_out, p_out, s0_ref, s1_ref, y_ref,
):
    m = 1.0 - st_ref[1]
    b = []
    for c in range(3):
        b.append(m * gather_sum(idx_ref, sum_ref, p_ref[c], rx0[c], rx1[c], ry0[c], ry1[c]))
        b_out[c] = b[c]
    r, d, x = smooth(1, 2, coef_ref, st_ref, b, None, 3, (ahi, alo, bhi, blo), y_ref)
    s = st_ref[0, :64]
    outs = stiffness([s * t for t in d], ohi, olo, bhi, blo, y_ref, 64)
    nx = xs_ref.shape[0] // 2
    for c in range(3):
        x_out[c] = x[c]
        left = owner_ref[...] * m[:64] * r[c] - s * outs[c]
        part = rsel(sel(rxy_ref[...], left), rz_ref[...])
        p_out[c] = part
        faces = sel(xs_ref[...], part)
        s0_ref[c], s1_ref[c] = for_pairs(idx_ref, 0, faces[:nx], faces[nx:])


def tail(level, last, coef_ref, owner_ref, st_ref, r, d, x, outs, c):
    n = x[c].shape[0]
    c1, c2 = coef_ref[level, 2 * last - 1], coef_ref[level, 2 * last]
    s, f, inv = st_ref[0, :n], st_ref[1, :n], st_ref[2 + c, :n]
    return owner_ref[...] * (x[c] + c1 * d[c] + c2 * inv * (r[c] - f * d[c])) - c2 * inv * s * outs[c]


def bottom_body(
    idx_ref, coef_ref, p_ref, rx0, rx1, ry0, ry1, sum_ref, st_ref, owner_ref, ahi, alo, ohi, olo, bhi, blo,
    x2_ref, owner2_ref, xs_ref,
    p_out, s0_ref, s1_ref, y_ref,
):
    m = 1.0 - st_ref[1]
    b = [m * gather_sum(idx_ref, sum_ref, p_ref[c], rx0[c], rx1[c], ry0[c], ry1[c]) for c in range(3)]
    r, d, x = smooth(2, 1, coef_ref, st_ref, b, None, 3, (ahi, alo, bhi, blo), y_ref)
    outs = stiffness([st_ref[0, :32] * t for t in d], ohi, olo, bhi, blo, y_ref, 32)
    nx = xs_ref.shape[0] // 2
    for c in range(3):
        e = tail(2, 3, coef_ref, owner_ref, st_ref, r, d, x, outs, c)
        part = jnp.concatenate([owner2_ref[...] * x2_ref[c], e], 0)
        p_out[c] = part
        faces = sel(xs_ref[...], part)
        s0_ref[c], s1_ref[c] = for_pairs(idx_ref, 0, faces[:nx], faces[nx:])


def up2_body(
    idx_ref, coef_ref, p_ref, rx0, rx1, ry0, ry1, sum_ref, sum1_ref, b_ref, st_ref, owner_ref, ahi, alo, ohi, olo, bhi, blo, xs_ref,
    pxy_ref, pz_ref, p_out, s0_ref, s1_ref, y_ref,
):
    x = []
    for c in range(3):
        fine = gather_sum(idx_ref, sum_ref, p_ref[c, :64], rx0[c, :NX2], rx1[c, :NX2], ry0[c, :NY2], ry1[c, :NY2])
        e = gather_sum(idx_ref, sum1_ref, p_ref[c, 64:], rx0[c, NX2:], rx1[c, NX2:], ry0[c, NY2:], ry1[c, NY2:])
        x.append(fine + (1.0 - st_ref[1]) * rsel(sel(pxy_ref[...], e), pz_ref[...]))
    b = [b_ref[c] for c in range(3)]
    r, d, x = smooth(1, 2, coef_ref, st_ref, b, x, 2, (ahi, alo, bhi, blo), y_ref)
    outs = stiffness([st_ref[0, :64] * t for t in d], ohi, olo, bhi, blo, y_ref, 64)
    nx = xs_ref.shape[0] // 2
    for c in range(3):
        part = tail(1, 2, coef_ref, owner_ref, st_ref, r, d, x, outs, c)
        p_out[c] = part
        faces = sel(xs_ref[...], part)
        s0_ref[c], s1_ref[c] = for_pairs(idx_ref, 0, faces[:nx], faces[nx:])


def swap(axis, s0, s1):
    n = GX if axis == "gx" else GY
    even = [(i, i ^ 1) for i in range(n)]
    odd = [(i, (((i - 1) ^ 1) + 1) % n) for i in range(n)]
    return lax.ppermute(s0, axis, even), lax.ppermute(s1, axis, odd)


def chebyshev_table(spectrum):
    low, top = spectrum[:, 0], spectrum[:, 1]
    center, radius = 0.5 * (top + low), 0.5 * (top - low)
    ratio = center / radius
    rho = 1.0 / ratio
    columns = [1.0 / center]
    for _ in range(3):
        after = 1.0 / (2.0 * ratio - rho)
        columns += [after * rho, 2.0 * after / radius]
        rho = after
    return jnp.stack(columns, 1)


def interp_tables():
    plane = {}
    for key, degree, halo, fine, rows, coarse, rows_c in (
        (4, 4, 0, NODES["4"], 224, NODES["2o"], 64),
        (2, 2, 0, NODES["2o"], 64, NODES["1o"], 32),
        ("2e", 2, 2, NODES["2e"], 256, NODES["1e"], 96),
    ):
        px, py = prolong_line(degree, EX + 2 * halo), prolong_line(degree, EY + 2 * halo)
        f0, c0 = degree * halo, degree * halo // 2
        full = np.zeros((rows, rows_c))
        for r, q in ((r, q) for r in range(len(fine)) for q in range(len(coarse))):
            if fine[r] is not None and coarse[q] is not None:
                (i, j), (a, b) = fine[r], coarse[q]
                full[r, q] = px[i + f0, a + c0] * py[j + f0, b + c0]
        plane[key] = full.astype(ml_dtypes.bfloat16)
    z4 = prolong_line(4, 32)[:128, :64]
    z2 = prolong_line(2, 32)[:64, :32]
    pz4 = np.zeros((2, 128, 128))
    for v in range(2):
        pz4[v, 64 * v : 64 * v + 64, :] = z4.T
    pz2 = np.zeros((128, 128))
    for v in range(2):
        pz2[32 * v : 32 * v + 32, 64 * v : 64 * v + 64] = z2.T
    cast = lambda t: np.ascontiguousarray(t).astype(ml_dtypes.bfloat16)
    return plane, cast(pz4), cast(pz4.transpose(0, 2, 1)), cast(pz2), cast(pz2.T)


def local(modes, moduli, pinned, spectrum):
    idx = (lax.axis_index("gx") * 16 + lax.axis_index("gy")).astype(jnp.int32).reshape(1)
    coef = chebyshev_table(spectrum)
    modes = modes.reshape(2, 3, NX * NY, NZ)
    moduli = moduli.reshape(NX * NY, NZ)
    pinned = pinned.reshape(NX * NY, NZ)

    zmats = {p: hi_lo(z_matrices(p, 1 if p == 4 else 2)) for p in (4, 2, 1)}
    plane, pz4, rz4, pz2, rz2 = interp_tables()
    bf = lambda t: np.ascontiguousarray(t).astype(ml_dtypes.bfloat16)
    x2, x20, x1, x21 = EXCH["2"], EXCH["20"], EXCH["1"], EXCH["21"]

    at4 = {n: r for r, n in enumerate(NODES["4"])}
    at2e = {n: r for r, n in enumerate(NODES["2e"]) if n is not None}
    pick2 = one_hot(64, NX * NY, [(r, at4[(2 * i, 2 * j)]) for r, (i, j) in enumerate(NODES["2o"]) if i < 6 and j < 8])
    zw, zm = np.zeros((128, 128)), np.zeros((128, 128))
    dw, dm, d1w, d1m = (np.zeros((128, 128)) for _ in range(4))
    for k in range(64):
        zw[2 * k, k] = zm[2 * k, 64 + k] = 1.0
        for v in range(2):
            dw[k, 64 * v + k] = dm[64 + k, 64 * v + k] = 1.0
            if k % 2 == 0:
                d1w[k, 32 * v + k // 2] = d1m[64 + k, 32 * v + k // 2] = 1.0
    pick1 = one_hot(96, 256, [(r, at2e[(2 * n[0], 2 * n[1])]) for r, n in enumerate(NODES["1e"]) if n is not None])
    owner2, owner1 = np.zeros((64, 128), np.float32), np.zeros((32, 128), np.float32)
    for r, (i, j) in enumerate(NODES["2o"]):
        owner2[r] = float(i < 6 and j < 8)
    for r, (i, j) in enumerate(NODES["1o"]):
        owner1[r] = float(i < 3 and j < 4)
    kd4, l4 = kd_tables(NODES["4"], 224, 4)
    kd2, l2 = kd_tables(NODES["2e"], 256, 2)
    kd1, l1 = kd_tables(NODES["1e"], 96, 1)
    table4 = np.concatenate([setup_table(4, NODES["4"], 256, 0), l4], 0)
    table4[0:224, 64:72] = kd4
    table2 = setup_table(2, NODES["2e"], 256, 2)
    table1 = setup_table(1, NODES["1e"], 96, 2)
    first = np.zeros((192 + 2 * NX2 + 2 * NY2, 256))
    first[0:64, 0 : NX * NY] = pick2
    first[64:192, 0:128], first[64:192, 128:256] = zw, zm
    first[192 : 192 + 2 * NX2, 0:64] = x2["xs"]
    first[192 + 2 * NX2 :, 0 : 64 + 2 * NX2] = x2["ys"]
    first = bf(first)

    mx = 128 + x2["nx"]
    my = 128 + x2["ny"]
    q2own, sx0, sx1, line, ys = call(
        pack_x_body, "pack_x", [idx], [modes, moduli, pinned, first],
        [((64, 128), F32), ((mx, 128), F32), ((mx, 128), F32), ((128, 128), F32), ((2 * NY2, 256), BF16)], [pltpu.VMEM((NX * NY, NZ), F32)],
    )
    rx0, rx1 = swap("gx", sx0, sx1)
    a4 = plane_matrices(idx, 4, table4, 256, 0, [(224, 256)])
    sy0, sy1 = call(
        pack_y_body, "pack_y", [idx], [line, q2own, rx0, rx1, ys], [((my, 128), F32), ((my, 128), F32)],
    )
    ry0, ry1 = swap("gy", sy0, sy1)
    mats2 = plane_matrices(idx, 2, table2, 256, 2, [(144, 256), (64, 64)])
    mats1 = plane_matrices(idx, 1, table1, 96, 2, [(64, 96), (32, 32)])

    big = ((3, 224, 256), F32)
    msgx, msgy = ((3, X4, 256), F32), ((3, Y4, 256), F32)
    y4 = pltpu.VMEM((3, 4 * 224, 256), F32)
    y4f = pltpu.VMEM((3, 4 * 48, 256), F32)
    full = pltpu.VMEM((6, 224, 128), F32)
    keep = pltpu.VMEM((3, 224, 256), F32)
    halves = ((6, 224, 128), F32)
    mats4 = [*a4, *zmats[4]]

    b, st4, d, w, s0, s1 = call(
        first4_body, "first4", [idx, coef], [modes, moduli, pinned, rx0, rx1, ry0, ry1, table4, *mats4],
        [big, ((5, 224, 128), F32), big, big, msgx, msgx], [y4f],
    )
    st2, st1 = call(
        statics_body, "statics", [idx],
        [q2own, rx0, rx1, ry0, ry1, x2["sum"], bf(np.stack([dw, dm, d1w, d1m])), pick1, kd2, l2, kd1, l1],
        [((5, 256, 128), F32), ((5, 96, 128), F32)],
    )

    def trade4(u, s0, s1):
        r0, r1 = swap("gx", s0, s1)
        (w,) = call(block4_body, "block4", [], [u, *mats4], [halves], [y4], flops=10**10)
        t0, t1 = call(faces_y4_body, "faces_y4", [idx], [w, r0, r1], [msgy, msgy])
        return [w, r0, r1, *swap("gy", t0, t1)]

    def trade(table, p, s0, s1, sums=None):
        r0, r1 = swap("gx", s0, s1)
        t0, t1 = call(faces_y_body, "faces_y", [idx], [p, r0, r1, table["ys"]], [((3, table["ny"], 128), F32)] * 2)
        return [p, r0, r1, *swap("gy", t0, t1), *([table["sum"]] if sums is None else sums)]

    got = trade4(w, s0, s1)
    r, d, x, w, s0, s1 = call(
        functools.partial(mid4_body, 1), "mid4", [idx, coef], [*got, st4, b, d, d, *mats4], [big, big, big, big, msgx, msgx], [y4f, full],
    )
    got = trade4(w, s0, s1)
    face2, face20, face1, face21 = (((3, t["nx"], 128), F32) for t in (x2, x20, x1, x21))
    own2f, own1f = ((3, 64, 128), F32), ((3, 32, 128), F32)
    x4, p2, s0, s1 = call(
        resid4_body, "resid4", [idx, coef], [*got, st4, r, d, x, *mats4, bf(plane[4].T), rz4, x2["xs"]],
        [big, own2f, face2, face2], [y4, full, keep],
    )
    y2, y1 = pltpu.VMEM((3, 4 * 144, 128), F32), pltpu.VMEM((3, 4 * 64, 128), F32)
    b2, xo2, p1, s0, s1 = call(
        down2_body, "down2", [idx, coef],
        [*trade(x2, p2, s0, s1), st2, bf(plane[2].T), rz2, x1["xs"], *mats2, *zmats[2], owner2],
        [((3, 256, 128), F32), own2f, own1f, face1, face1], [y2],
    )
    p2, s0, s1 = call(
        bottom_body, "bottom", [idx, coef],
        [*trade(x1, p1, s0, s1), st1, owner1, *mats1, *zmats[1], xo2, owner2, x21["xs"]],
        [((3, 96, 128), F32), face21, face21], [y1],
    )
    p2, s0, s1 = call(
        up2_body, "up2", [idx, coef],
        [*trade(x21, p2, s0, s1, (x2["sum"], x1["sum"])), b2, st2, owner2, *mats2, *zmats[2], x20["xs"], plane["2e"], pz2],
        [own2f, face20, face20], [y2],
    )
    x, w, s0, s1 = call(
        rise4_body, "rise4", [idx], [*trade(x20, p2, s0, s1), plane[4], pz4, st4, x4, *mats4], [big, big, msgx, msgx], [y4f],
    )
    r, d, x, w, s0, s1 = call(
        functools.partial(mid4_body, 0), "mid4_0", [idx, coef], [*trade4(w, s0, s1), st4, b, x, x, *mats4],
        [big, big, big, big, msgx, msgx], [y4f, full],
    )
    r, d, x, w, s0, s1 = call(
        functools.partial(mid4_body, 1), "mid4", [idx, coef], [*trade4(w, s0, s1), st4, r, d, x, *mats4],
        [big, big, big, big, msgx, msgx], [y4f, full],
    )
    (out,) = call(
        last4_body, "last4", [idx, coef], [*trade4(w, s0, s1), st4, r, d, x], [((2, 3, NX * NY, NZ), F32)], [full],
    )
    return out.reshape(2, 3, NX, NY, NZ)


def solution(mesh):
    placed = (P(None, None, "gx", "gy", None), P("gx", "gy", None), P("gx", "gy", None), P())
    return jax.shard_map(
        local,
        mesh=mesh,
        in_specs=placed,
        out_specs=P(None, None, "gx", "gy", None),
        check_vma=False,
    )
```
